256 devices in a mesh: groups: 2 (over y), chan: 64 (over x, z), sub: 2 (over core).
Axes of the slice: x: 4, y: 2, z: 16, core: 2. Of those that a mesh axis runs over, the one named last changes fastest.
The devices are a block of a 4x16x16 slice.
Arguments:
- predicted_sky_response: bfloat16 [131072, 8, 2, 128], P(('groups', 'chan', 'sub')), parts along dimension 0, may hold values from -0.4375 to 0.4375
- measured_correlation: bfloat16 [131072, 2, 128], P(('groups', 'chan', 'sub')), parts along dimension 0, may hold values from -6 to 6
- keep_indicator: int32 [131072, 128], P(('groups', 'chan', 'sub')), parts along dimension 0, may hold values 0 or 1
- tile_owner: int32 [131072, 1], P(('groups', 'chan', 'sub')), parts along dimension 0, may hold values from 0 to 63; in each aligned block of 512 rows (0 to 511, 512 to 1023, ...) at most 24 rows name the same one
- tile_channel: int32 [131072], P(('groups', 'chan', 'sub')), parts along dimension 0, may hold values from 0 to 3
- tile_base: int32 [131072], P(('groups', 'chan', 'sub')), parts along dimension 0, may hold values from 0 to 14
- pairs: int32 [15, 2, 128], replicated, may hold values from 0 to 61, as said below
- gains: float32 [512, 2, 62, 8], P(('groups', 'chan')), parts along dimension 0, may hold values from -5 to 5
- duals: float32 [512, 2, 62, 8], P(('groups', 'chan', 'sub')), parts along dimension 0, may hold values from -4 to 4
- consensus: float32 [8, 2, 62, 8], P('groups'), parts along dimension 0, may hold values from -5 to 5
- rho: float32 [8], replicated, may hold values from 0.3 to 3
Outputs:
- gains_new: float32 [512, 2, 62, 8], P(('groups', 'chan', 'sub')), parts along dimension 0
- consensus_new: float32 [8, 2, 62, 8], P('groups'), parts along dimension 0
- duals_new: float32 [512, 2, 62, 8], P(('groups', 'chan', 'sub')), parts along dimension 0
The draws below stay inside these ranges and needn't reach their ends.
There are 2 independent parts, one for each index of `groups`. The reference program is written for one: setup_inputs(seed, part) draws one part's arguments, and reference() takes and returns one part's arrays. A program takes and returns all parts, laid end to end along the dimension named above; an argument that names none is the same for every part. Nothing has to cross between parts.
Inputs may be any that keep to these rules, and one draw needn't show every extreme that they name: `tile_owner`: on the tiles of one device at most 24 name the same owner, a bound that some block reaches. `pairs`: the two stations of a row differ.
All inputs are finite; a program needn't handle non-finite values. No bound on the sum of `keep_indicator` on one device may be relied on, other than what follows from the above.
Results may differ from the reference program's by a relative error of at most 0.0027.
Values may be sent and summed in bfloat16 or wider, within the bound.
A program may use at most 128 MiB of HBM per device.

```python
import math
import jax
import jax.numpy as jnp
import numpy as np
from jax import lax

NS = 62
K = 8
DEG = 4
TR = 128
BT = 15
CH_DEV = 4
TILES_DEV = 512
F = 256
TILES = 65536
CAP = 24
ROWS_CH = 32768
N_CHAN = 64


def draw_pairs(key, part):
    key_first, key_offset = jax.random.split(jax.random.fold_in(key, 17))
    first_station = jax.random.randint(key_first, (BT, TR), 0, NS)
    offset = jax.random.randint(key_offset, (BT, TR), 1, NS)
    station_second = (first_station + offset) % NS
    return jnp.stack([first_station, station_second], axis=1).astype(jnp.int32)


def touch_ends(result, own_key, smallest, top_value):
    longest = result.shape.index(max(result.shape))
    spots = []
    for shift in (0, 1):
        where = [jax.random.randint(jax.random.fold_in(own_key, axis), (), 0, length) for axis, length in enumerate(result.shape)]
        where[longest] = (where[longest] + shift) % result.shape[longest]
        spots.append(tuple(where))
    return result.at[spots[0]].set(smallest).at[spots[1]].set(top_value)


def block_scale(rng, extent, pieces, low, top_value):
    factor_of, own = 1.0, jax.random.fold_in(rng, 6)
    for position, blocks in pieces:
        steps = jnp.exp(jax.random.uniform(jax.random.fold_in(own, position), (blocks,), jnp.float32, low / len(pieces), top_value / len(pieces)))
        factor_of = factor_of * jnp.repeat(steps, extent[position] // blocks).reshape([-1 if axis == position else 1 for axis in range(len(extent))])
    return factor_of


def assign_block(own_key, own, number, rows, number_of, top, bound, skew):
    order = jax.random.permutation(own_key, number_of)
    heavy_load, common = load_shares(number_of, rows * top, bound, skew, True), load_shares(number_of, rows * top, bound, skew, False)
    places = jnp.arange(number_of)

    def named(tallies, rotation):
        used = int((tallies > 0).sum())
        fixed = max(1, used // 4)
        passed = fixed + (places - fixed + rotation * (used - fixed)) % max(1, number_of - fixed)
        return jnp.zeros((number_of,), jnp.int32).at[order[jnp.where(places < fixed, places, passed)]].set(jnp.asarray(tallies, jnp.int32))

    tallies = jnp.where(number % 4 == 0, named(heavy_load, number // 4), named(common, number - number // 4 - 1))
    mixed = jax.random.permutation(jax.random.fold_in(own, 3), number_of)
    giver, taker = mixed[0:number_of // 2 * 2:2], mixed[1:number_of // 2 * 2:2]
    room = jnp.minimum(tallies[giver] - 1, bound - tallies[taker]) // 2
    room = jnp.where((giver == order[0]) | (taker == order[0]) | (tallies[taker] == 0), 0, jnp.maximum(room, 0))
    passed = jax.random.randint(jax.random.fold_in(own, 4), (number_of // 2,), 0, 1 << 20) % (room + 1)
    tallies = tallies.at[giver].add(-passed).at[taker].add(passed)
    members = jnp.searchsorted(jnp.cumsum(tallies), jnp.arange(rows * top), side="right").astype(jnp.int32)
    table = members.reshape(top, rows).T
    table = table[jax.random.permutation(jax.random.fold_in(own, 1), rows)]
    rotation = jax.random.randint(jax.random.fold_in(own, 2), (rows, 1), 0, top)
    return jnp.take_along_axis(table, (jnp.arange(top)[None, :] + rotation) % top, axis=1)


def load_shares(count, total, most, skew, full):
    loads = [(1 << 20) // math.isqrt(grade ** skew) + 1 for grade in range(1, count + 1)]
    largest = most if full else min(most, max(-(-total // count), total * loads[0] // sum(loads)))
    least = 1 if total - largest >= count - 1 else 0
    given, rest = [largest] + [least] * (count - 1), total - largest - least * (count - 1)
    while rest > 0:
        movable = [i for i in range(1, count) if given[i] < largest] or [i for i in range(1, count) if given[i] < most]
        mass, remaining = sum([loads[i] for i in movable]), rest
        for i in movable:
            more = min(most - given[i], max(1, remaining * loads[i] // mass), rest)
            given[i] = given[i] + more
            rest = rest - more
    return np.array(given)


def scatter_about(key, shape, width, most, shards=(), kind=jnp.bfloat16):
    result = jax.random.normal(key, shape, jnp.float32) * width
    if len(shards) > 0:
        result = block_scale(key, shape, shards, -0.22, 0.18) * result
    return jnp.clip(result, min=-most, max=most).astype(kind)


def setup_inputs(seed: int = 0, part: int = 0) -> dict:
    arg_keys = jax.random.split(jax.random.key(seed), 12)
    own_keys = jax.random.split(jax.random.fold_in(arg_keys[11], part), 12)
    predicted_sky_response = scatter_about(own_keys[0], (TILES, K, 2, TR), ((2 * ROWS_CH // NS) ** -0.5), 0.4375, ((0, 128),))
    measured_correlation = scatter_about(own_keys[1], (TILES, 2, TR), 1.0, 6.0, ((0, 128),))
    keep_indicator = touch_ends((jax.random.randint(own_keys[2], (TILES, TR), 0, 4) < 3).astype(jnp.int32), jax.random.fold_in(own_keys[2], 1), 0, 1)
    tile_owner_keys = jax.random.split(jax.random.fold_in(own_keys[3], 1), TILES // TILES_DEV)
    tile_owner_turns = jax.random.permutation(jax.random.fold_in(own_keys[3], 3), TILES // TILES_DEV)
    tile_owner = jax.vmap(lambda own, number: assign_block(jax.random.fold_in(own_keys[3], 2), own, number, TILES_DEV, N_CHAN, 1, CAP, 2))(tile_owner_keys, tile_owner_turns).reshape((TILES, 1))
    tile_channel = touch_ends(jax.random.randint(own_keys[4], (TILES,), 0, CH_DEV), jax.random.fold_in(own_keys[4], 1), 0, CH_DEV - 1).astype(jnp.int32)
    tile_base = touch_ends(jax.random.randint(own_keys[5], (TILES,), 0, BT), jax.random.fold_in(own_keys[5], 1), 0, BT - 1).astype(jnp.int32)
    pairs = draw_pairs(jax.random.fold_in(arg_keys[11], 71), part)
    gains = scatter_about(own_keys[7], (F, 2, NS, K), 0.8, 5.0, ((0, 64),), jnp.float32)
    duals = scatter_about(own_keys[8], (F, 2, NS, K), 0.3, 4.0, ((0, 128),), jnp.float32)
    consensus = scatter_about(own_keys[9], (DEG, 2, NS, K), 0.5, 5.0, (), jnp.float32)
    rho = jnp.clip(jnp.exp(jax.random.uniform(arg_keys[10], (K,), jnp.float32, math.log(0.3), math.log(3.0))), 0.3, 3.0)
    return dict(predicted_sky_response=predicted_sky_response, measured_correlation=measured_correlation, keep_indicator=keep_indicator, tile_owner=tile_owner, tile_channel=tile_channel, tile_base=tile_base, pairs=pairs, gains=gains, duals=duals, consensus=consensus, rho=rho)


def legendre_rows(channels):
    positions = jnp.arange(channels, dtype=jnp.float32)
    abscissa = (2.0 * positions - (channels - 1)) / max(channels - 1, 1)
    return jnp.stack([jnp.ones_like(abscissa), abscissa, 0.5 * (3.0 * abscissa * abscissa - 1.0), 0.5 * (5.0 * abscissa * abscissa * abscissa - 3.0 * abscissa)])

def outer_terms(vector_real, vector_imag, weight_real, weight_imag):
    tiles_count, row_total_count, directions = vector_real.shape
    outer_real = vector_real[..., :, None] * vector_real[..., None, :] + vector_imag[..., :, None] * vector_imag[..., None, :]
    outer_imag = vector_real[..., :, None] * vector_imag[..., None, :] - vector_imag[..., :, None] * vector_real[..., None, :]
    normal = jnp.stack([outer_real, outer_imag], axis=2).reshape(tiles_count, row_total_count, 2 * directions * directions)
    side_real = vector_real * weight_real[..., None] + vector_imag * weight_imag[..., None]
    side_imag = vector_real * weight_imag[..., None] - vector_imag * weight_real[..., None]
    right_side = jnp.stack([side_real, side_imag], axis=2).reshape(tiles_count, row_total_count, 2 * directions)
    return (normal, right_side)

def row_terms(coupling, observed, near_gain, far_gain):
    coupling_real = jnp.swapaxes(coupling[:, :, 0, :], 1, 2).astype(jnp.float32)
    coupling_imag = jnp.swapaxes(coupling[:, :, 1, :], 1, 2).astype(jnp.float32)
    near_real, near_imag = (near_gain[:, :, 0, :], near_gain[:, :, 1, :])
    far_real, far_imag = (far_gain[:, :, 0, :], far_gain[:, :, 1, :])
    slope_real = coupling_real * far_real + coupling_imag * far_imag
    slope_imag = coupling_imag * far_real - coupling_real * far_imag
    mirror_real = coupling_real * near_real - coupling_imag * near_imag
    mirror_imag = -(coupling_real * near_imag + coupling_imag * near_real)
    model_real = jnp.sum(near_real * slope_real - near_imag * slope_imag, axis=-1)
    model_imag = jnp.sum(near_real * slope_imag + near_imag * slope_real, axis=-1)
    observed_f = observed.astype(jnp.float32)
    residual_real = observed_f[:, 0, :] - model_real
    residual_imag = observed_f[:, 1, :] - model_imag
    normal_near, right_near = outer_terms(slope_real, slope_imag, residual_real, residual_imag)
    normal_far, right_far = outer_terms(mirror_real, mirror_imag, residual_real, -residual_imag)
    normal = jnp.concatenate([normal_near, normal_far], axis=1).astype(jnp.bfloat16)
    right_side = jnp.concatenate([right_near, right_far], axis=1).astype(jnp.bfloat16)
    return (normal, right_side)

def admm_update(normal, right_side, gain, dual, anchor, rho):
    count, stations = (normal.shape[0], normal.shape[1])
    directions = rho.shape[0]
    normal_blocks = normal.reshape(count, stations, 2, directions, directions)
    ridge_diag = jnp.diag(rho)
    higher_half_records = jnp.concatenate([normal_blocks[:, :, 0] + ridge_diag, -normal_blocks[:, :, 1]], axis=-1)
    lower_rows = jnp.concatenate([normal_blocks[:, :, 1], normal_blocks[:, :, 0] + ridge_diag], axis=-1)
    system = jnp.concatenate([higher_half_records, lower_rows], axis=-2)
    gain_rows = jnp.transpose(gain, (0, 2, 1, 3))
    dual_rows = jnp.transpose(dual, (0, 2, 1, 3))
    anchor_rows = jnp.transpose(anchor, (0, 2, 1, 3))
    target = right_side.reshape(count, stations, 2, directions) - dual_rows - rho * (gain_rows - anchor_rows)
    factor = jnp.linalg.cholesky(system)
    gain_step = jax.scipy.linalg.cho_solve((factor, True), target.reshape(count, stations, 2 * directions)[..., None])[..., 0]
    return gain + jnp.transpose(gain_step.reshape(count, stations, 2, directions), (0, 2, 1, 3))

def fit_consensus(poly_basis, summed):
    gram_matrix = jnp.dot(poly_basis, poly_basis.T, precision=lax.Precision.HIGHEST)
    factor = jnp.linalg.cholesky(gram_matrix)
    coeffs = jax.scipy.linalg.cho_solve((factor, True), summed.reshape(summed.shape[0], -1))
    return coeffs.reshape(summed.shape)

def reference(predicted_sky_response, measured_correlation, keep_indicator, tile_owner, tile_channel, tile_base, pairs, gains, duals, consensus, rho):
    channels = CH_DEV * N_CHAN
    retained_selector = keep_indicator > 0
    predicted_response_kept = jnp.where(retained_selector[:, None, None, :], predicted_sky_response, jnp.zeros_like(predicted_sky_response))
    measured_correlation_kept = jnp.where(retained_selector[:, None, :], measured_correlation, jnp.zeros_like(measured_correlation))
    channel_lookup = (tile_owner[:, 0] * CH_DEV + tile_channel).astype(jnp.int32)
    gain_table = jnp.transpose(gains, (0, 2, 1, 3))
    iteration_tally = predicted_sky_response.shape[0] // TILES_DEV
    normal_matrix_width = 2 * K * K

    def one_block(totals, block_item):
        normal_acc, right_acc = totals
        block_coherency, block_visibility, block_channel, block_base = block_item
        stations = pairs[block_base]
        first_station = stations[:, 0, :]
        station_second = stations[:, 1, :]
        near_gain = gain_table[block_channel[:, None], first_station]
        far_gain = gain_table[block_channel[:, None], station_second]
        normal, right_side = row_terms(block_coherency, block_visibility, near_gain, far_gain)
        normal = lax.optimization_barrier(normal).astype(jnp.float32)
        right_side = lax.optimization_barrier(right_side).astype(jnp.float32)
        segment_ids = (jnp.concatenate([first_station, station_second], axis=1) + block_channel[:, None] * NS).astype(jnp.int32)
        normal_acc = normal_acc + jax.ops.segment_sum(normal.reshape(-1, normal_matrix_width), segment_ids.reshape(-1), num_segments=channels * NS)
        right_acc = right_acc + jax.ops.segment_sum(right_side.reshape(-1, 2 * K), segment_ids.reshape(-1), num_segments=channels * NS)
        return ((normal_acc, right_acc), None)
    block_items = (predicted_response_kept.reshape((iteration_tally, TILES_DEV) + predicted_sky_response.shape[1:]), measured_correlation_kept.reshape((iteration_tally, TILES_DEV) + measured_correlation.shape[1:]), channel_lookup.reshape(iteration_tally, TILES_DEV), tile_base.reshape(iteration_tally, TILES_DEV))
    start_totals = (jnp.zeros((channels * NS, normal_matrix_width), jnp.float32), jnp.zeros((channels * NS, 2 * K), jnp.float32))
    (normal_sum, right_sum), _ = lax.scan(one_block, start_totals, block_items)
    normal_sum = normal_sum.reshape(channels, NS, normal_matrix_width)
    right_sum = right_sum.reshape(channels, NS, 2 * K)
    poly_basis = legendre_rows(channels)
    anchor = jnp.einsum('df,dcsk->fcsk', poly_basis, consensus, precision=lax.Precision.HIGHEST)
    gains_new = admm_update(normal_sum, right_sum, gains, duals, anchor, rho)
    summed = jnp.einsum('df,fcsk->dcsk', poly_basis, gains_new + duals / rho, precision=lax.Precision.HIGHEST)
    consensus_new = fit_consensus(poly_basis, summed)
    duals_new = duals + rho * (gains_new - jnp.einsum('df,dcsk->fcsk', poly_basis, consensus_new, precision=lax.Precision.HIGHEST))
    return (gains_new, consensus_new, duals_new)
```

```python
import functools
import math

import jax
import jax.numpy as jnp
import numpy as np
from jax import lax
from jax.experimental import pallas as pl
from jax.experimental.pallas import tpu as pltpu
from jax.sharding import Mesh
from jax.sharding import PartitionSpec as P

GROUPS_CHAN_SUB = ("groups", "chan_0", "chan_1", "sub")
GROUPS_CHAN = ("groups", "chan_0", "chan_1")
BF, F32 = jnp.bfloat16, jnp.float32
GROUP = 8
HALF = 64


def term_rows(directions):
    real, imag = {}, {}
    for k in range(directions):
        for m in range(k, directions):
            real[k, m] = len(real)
    for k in range(directions):
        for m in range(k + 1, directions):
            imag[k, m] = len(real) + len(imag)
    return real, imag


def legendre_rows(channels):
    positions = jnp.arange(channels, dtype=jnp.float32)
    abscissa = (2.0 * positions - (channels - 1)) / max(channels - 1, 1)
    return jnp.stack(
        [
            jnp.ones_like(abscissa),
            abscissa,
            0.5 * (3.0 * abscissa * abscissa - 1.0),
            0.5 * (5.0 * abscissa * abscissa * abscissa - 3.0 * abscissa),
        ]
    )


def gram_inverse(channels):
    x = (2.0 * np.arange(channels, dtype=np.float64) - (channels - 1)) / max(channels - 1, 1)
    basis = np.stack([np.ones_like(x), x, 0.5 * (3 * x * x - 1), 0.5 * (5 * x * x * x - 3 * x)])
    return np.linalg.inv(basis @ basis.T)


def tile_order(tile_base, bases):
    tiles = tile_base.shape[0]
    slots = tiles + GROUP * bases
    here = jnp.arange(tiles, dtype=jnp.int32)
    same = (tile_base[:, None] == tile_base[None, :]) & (here[None, :] < here[:, None])
    rank = jnp.sum(same.astype(jnp.int32), axis=1)
    rows = jnp.arange(bases, dtype=jnp.int32)
    counts = jnp.sum((tile_base[None, :] == rows[:, None]).astype(jnp.int32), axis=1)
    padded = (counts + GROUP - 1) // GROUP * GROUP
    start = jnp.sum(jnp.where(rows[None, :] < tile_base[:, None], padded[None, :], 0), axis=1)
    place = start + rank
    slot = jnp.arange(slots, dtype=jnp.int32)
    order = jnp.sum(jnp.where(place[None, :] == slot[:, None], here[None, :] - tiles, 0), axis=1) + tiles
    return order.astype(jnp.int32), (jnp.sum(padded) // GROUP).reshape(1).astype(jnp.int32)


def tile_kernel(order, groups, gain_row, home_row, base, sky, seen, keep, pairs, table, out,
                onehot, sky_s, seen_s, keep_s, gain_s, near_far, terms, sums):
    tiles, coupled, rows = sky.shape
    directions = coupled // 2
    bases = pairs.shape[0]
    real, imag = term_rows(directions)
    n_terms = directions * directions + 2 * directions
    devices = out.shape[0] - 1

    station = lax.rem(lax.broadcasted_iota(jnp.int32, (2 * HALF, rows), 0), HALF)
    for b in range(bases):
        for side in range(2):
            onehot[b, :, side * rows:(side + 1) * rows] = jnp.where(
                station == pairs[b, side:side + 1, :], 1.0, 0.0).astype(BF)

    def clear(i, carry):
        out[i] = jnp.zeros((n_terms, 2 * HALF), F32)
        return carry
    lax.fori_loop(0, devices + 1, clear, 0)
    lane = lax.broadcasted_iota(jnp.int32, (1, 2 * HALF), 1)

    def one_group(g, carry):
        for t in range(GROUP):
            named = order[g * GROUP + t]
            tile = jnp.where(named < tiles, named, 0)
            sky_s[pl.ds(t, coupled, stride=GROUP), :] = sky[tile].astype(F32)
            seen_s[pl.ds(t, 2, stride=GROUP), :] = seen[tile].astype(F32)
            keep_s[pl.ds(t, 1), :] = keep[pl.ds(tile, 1), :]
            gain_s[pl.ds(t, coupled, stride=GROUP), :] = table[gain_row[tile]].astype(F32)
        chosen = onehot.at[base[order[g * GROUP]]]
        near_far[...] = jnp.dot(gain_s[...].astype(BF), chosen[...], preferred_element_type=F32)

        kept = keep_s[...] > 0

        def block(ref, i):
            return ref[i * GROUP:(i + 1) * GROUP, :]

        res_r = jnp.where(kept, block(seen_s, 0), 0.0)
        res_i = jnp.where(kept, block(seen_s, 1), 0.0)
        a_r, a_i, b_r, b_i = [], [], [], []
        mod_r = mod_i = None
        for k in range(directions):
            c_r = jnp.where(kept, block(sky_s, 2 * k), 0.0)
            c_i = jnp.where(kept, block(sky_s, 2 * k + 1), 0.0)
            p_r, p_i = (near_far[(2 * k + c) * GROUP:(2 * k + c + 1) * GROUP, :rows] for c in range(2))
            q_r, q_i = (near_far[(2 * k + c) * GROUP:(2 * k + c + 1) * GROUP, rows:] for c in range(2))
            x_r = c_r * q_r + c_i * q_i
            x_i = c_i * q_r - c_r * q_i
            a_r.append(x_r)
            a_i.append(x_i)
            b_r.append(c_r * p_r - c_i * p_i)
            b_i.append(-(c_r * p_i + c_i * p_r))
            m_r = p_r * x_r - p_i * x_i
            m_i = p_r * x_i + p_i * x_r
            mod_r = m_r if mod_r is None else mod_r + m_r
            mod_i = m_i if mod_i is None else mod_i + m_i
        res_r = res_r - mod_r
        res_i = res_i - mod_i

        for side, (v_r, v_i, w_r, w_i) in enumerate(
                ((a_r, a_i, res_r, res_i), (b_r, b_i, res_r, -res_i))):
            made = [None] * n_terms
            pending = {}

            def put(j, value):
                pending[j] = value
                lo = j - j % 2
                if lo in pending and lo + 1 in pending:
                    both = jnp.concatenate([pending.pop(lo), pending.pop(lo + 1)], axis=0)
                    terms[lo * GROUP:(lo + 2) * GROUP, side * rows:(side + 1) * rows] = both.astype(BF)

            for (k, m), j in real.items():
                put(j, v_r[k] * v_r[m] + v_i[k] * v_i[m])
            for (k, m), j in imag.items():
                put(j, v_r[k] * v_i[m] - v_i[k] * v_r[m])
            first = directions * directions
            for k in range(directions):
                put(first + k, v_r[k] * w_r + v_i[k] * w_i)
            for k in range(directions):
                put(first + directions + k, v_r[k] * w_i - v_i[k] * w_r)

        sums[...] = lax.dot_general(terms[...], chosen[...], (((1,), (1,)), ((), ())),
                                    preferred_element_type=F32)
        for t in range(GROUP):
            named = order[g * GROUP + t]
            tile = jnp.where(named < tiles, named, 0)
            home = home_row[tile]
            row = jnp.where(named < tiles, lax.shift_right_logical(home, 1), devices)
            part = jnp.where(lane // HALF == jnp.bitwise_and(home, 1),
                             sums[pl.ds(t, n_terms, stride=GROUP), :], 0.0)
            out[row] = out[row] + part
        return carry

    lax.fori_loop(0, groups[0], one_group, 0)


def tile_sums(sky, seen, keep, order, groups, gain_row, home_row, base, pairs, table, devices):
    tiles, directions, _, rows = sky.shape
    n_terms = directions * directions + 2 * directions
    bases = pairs.shape[0]
    smem = pl.BlockSpec(memory_space=pltpu.SMEM)
    vmem = pl.BlockSpec(memory_space=pltpu.VMEM)
    coupled = 2 * directions
    return pl.pallas_call(
        tile_kernel,
        out_shape=jax.ShapeDtypeStruct((devices + 1, n_terms, 2 * HALF), F32),
        in_specs=[smem] * 5 + [vmem] * 5,
        out_specs=vmem,
        scratch_shapes=[
            pltpu.VMEM((bases, 2 * HALF, 2 * rows), BF),
            pltpu.VMEM((coupled * GROUP, rows), F32),
            pltpu.VMEM((2 * GROUP, rows), F32),
            pltpu.VMEM((GROUP, rows), jnp.int32),
            pltpu.VMEM((coupled * GROUP, 2 * HALF), F32),
            pltpu.VMEM((coupled * GROUP, 2 * rows), F32),
            pltpu.VMEM((n_terms * GROUP, 2 * rows), BF),
            pltpu.VMEM((n_terms * GROUP, 2 * HALF), F32),
        ],
        compiler_params=pltpu.CompilerParams(vmem_limit_bytes=40 * 1024 * 1024),
        name="tile_sums",
    )(order, groups, gain_row, home_row, base, sky.reshape(tiles, coupled, rows), seen, keep, pairs, table)


def eliminate(total, target, rho, full, directions):
    real, imag = term_rows(directions)
    lanes = total.shape[-1]
    for k in range(directions):
        for m in range(directions):
            re = real[min(k, m), max(k, m)]
            value = total[re:re + 1, :]
            if k == m:
                value = value + rho[k:k + 1, :]
                full[1, k * directions + m:k * directions + m + 1, :] = jnp.zeros((1, lanes), F32)
            else:
                im = imag[min(k, m), max(k, m)]
                imv = total[im:im + 1, :]
                full[1, k * directions + m:k * directions + m + 1, :] = imv if k < m else -imv
            full[0, k * directions + m:k * directions + m + 1, :] = value
    row_r = [full[0, k * directions:(k + 1) * directions, :] for k in range(directions)]
    row_i = [full[1, k * directions:(k + 1) * directions, :] for k in range(directions)]
    t_r = [target[k:k + 1, :] for k in range(directions)]
    t_i = [target[directions + k:directions + k + 1, :] for k in range(directions)]
    for k in range(directions):
        inv = 1.0 / row_r[k][k:k + 1, :]
        row_r[k] = row_r[k] * inv
        row_i[k] = row_i[k] * inv
        t_r[k] = t_r[k] * inv
        t_i[k] = t_i[k] * inv
        for m in range(directions):
            if m == k:
                continue
            f_r = row_r[m][k:k + 1, :]
            f_i = row_i[m][k:k + 1, :]
            row_r[m], row_i[m] = (row_r[m] - (f_r * row_r[k] - f_i * row_i[k]),
                                  row_i[m] - (f_r * row_i[k] + f_i * row_r[k]))
            t_r[m], t_i[m] = (t_r[m] - (f_r * t_r[k] - f_i * t_i[k]),
                              t_i[m] - (f_r * t_i[k] + f_i * t_r[k]))
    return jnp.concatenate(t_r + t_i, axis=0)


XS, ZS = "chan_0", "chan_1"


def place():
    return lax.axis_index(XS), lax.axis_index(ZS), lax.axis_index("sub")


def sender(src, dst, send_sem, recv_sem, x, z, s):
    return pltpu.make_async_remote_copy(
        src_ref=src, dst_ref=dst, send_sem=send_sem, recv_sem=recv_sem,
        device_id={XS: x, ZS: z, "sub": s}, device_id_type=pl.DeviceIdType.MESH)


def meet(x, z, s, nx, nz, crossed):
    barrier = pltpu.get_barrier_semaphore()

    def ring(d, carry):
        pl.semaphore_signal(barrier, inc=1, device_id={XS: x, ZS: lax.rem(z + d, nz), "sub": s},
                            device_id_type=pl.DeviceIdType.MESH)
        return carry
    lax.fori_loop(1, nz, ring, 0)
    near = [(e, f) for e in range(nx) for f in range(2) if e + f > 0 and (crossed or e * f == 0)]
    for e, f in near:
        pl.semaphore_signal(barrier, inc=1,
                            device_id={XS: lax.rem(x + e, nx), ZS: z, "sub": s + f - 2 * s * f},
                            device_id_type=pl.DeviceIdType.MESH)
    return barrier, nz - 1 + len(near)


def outward(i, nz):
    return jnp.where(lax.rem(i, 2) == 0, i // 2 + 1, nz - 1 - i // 2)


def gather_kernel(nx, nz, mine, table, z_recv, z_send, x_recv, x_send, c_recv, c_send):
    x, z, s = place()
    here, half = mine.shape[0], mine.shape[0] // 2
    barrier, count = meet(x, z, s, nx, nz, False)
    table[pl.ds((x * nz + z) * here + s * half, half)] = mine[pl.ds(s * half, half)]
    pl.semaphore_wait(barrier, count)

    def block(xx, zz):
        return table.at[pl.ds((xx * nz + zz) * here + s * half, half)]

    def rows(xx, h):
        return table.at[pl.ds(xx * nz * here, nz * here)].reshape(nz, here, *mine.shape[1:]).at[:, pl.ds(h * half, half)]

    own = mine.at[pl.ds(s * half, half)]

    def z_copy(d):
        return sender(own, block(x, z), z_send.at[d], z_recv.at[d], x, lax.rem(z + d, nz), s)

    def start_z(i, carry):
        z_copy(outward(i, nz)).start()
        return carry
    lax.fori_loop(0, nz - 1, start_z, 0)

    def x_copy(src, zz, d, e):
        return sender(src, block(x, zz), x_send.at[e, d], x_recv.at[e, d], lax.rem(x + e, nx), z, s)
    for e in range(1, nx):
        x_copy(own, z, 0, e).start()

    def pass_on(i, carry):
        d = outward(i, nz)
        zz = lax.rem(z + nz - d, nz)
        sender(own, block(x, zz), z_send.at[d], z_recv.at[d], x, z, s).wait_recv()
        for e in range(1, nx):
            x_copy(block(x, zz), zz, d, e).start()
        return carry
    lax.fori_loop(0, nz - 1, pass_on, 0)

    def c_copy(e, h):
        xx = lax.rem(x + nx - e, nx)
        return sender(rows(xx, h), rows(xx, h), c_send.at[e], c_recv.at[e], x, z, 1 - s)
    for e in (0, 1, 3, 2):
        if e > 0:
            xx = lax.rem(x + nx - e, nx)

            def arrived(d, carry):
                zz = lax.rem(z + nz - d, nz)
                sender(own, block(xx, zz), x_send.at[e, d], x_recv.at[e, d], x, z, s).wait_recv()
                return carry
            lax.fori_loop(0, nz, arrived, 0)
        c_copy(e, s).start()
    for e in range(nx):
        c_copy(e, 1 - s).wait_recv()

    def done_z(d, carry):
        z_copy(d).wait_send()
        return carry
    lax.fori_loop(1, nz, done_z, 0)
    for e in range(1, nx):
        def done_x(d, carry):
            x_copy(own, z, d, e).wait_send()
            return carry
        lax.fori_loop(0, nz, done_x, 0)
    for e in range(nx):
        c_copy(e, s).wait_send()


def gather_gains(mine, nx, nz):
    vmem = pl.BlockSpec(memory_space=pltpu.VMEM)
    dma = pltpu.SemaphoreType.DMA
    return pl.pallas_call(
        functools.partial(gather_kernel, nx, nz),
        out_shape=jax.ShapeDtypeStruct((nx * nz * mine.shape[0],) + mine.shape[1:], mine.dtype),
        in_specs=[vmem],
        out_specs=vmem,
        scratch_shapes=[dma((nz,)), dma((nz,)), dma((nx, nz)), dma((nx, nz)), dma((nx,)), dma((nx,))],
        compiler_params=pltpu.CompilerParams(collective_id=0, has_side_effects=True),
        name="gather_gains",
    )(mine)


def packed(v, plain):
    head = v[plain:].astype(BF)
    tail = v[plain:] - head.astype(F32)
    return jnp.concatenate([v[:plain].astype(BF), head, tail.astype(BF)], axis=0)


def unpacked(w, plain):
    v = w.astype(F32)
    mid = (v.shape[0] + plain) // 2
    return jnp.concatenate([v[:plain], v[plain:mid] + v[mid:]], axis=0)


def finish_kernel(nx, nz, inverse, sums, gain, dual, cons, basis, rho, gain_new, cons_new, dual_new,
                  peer, x_out, x_in, z_out, z_in, own_z, total, full, part_out, part_in, ring_in, last_in,
                  c_send, c_recv, x_send, x_recv, z_send, z_recv, p_send, p_recv, r_send, r_recv, l_send, l_recv):
    x, z, s = place()
    directions = rho.shape[0]
    degrees = basis.shape[0]
    plain = directions * directions
    chunk = 4
    nodes = nx * nz
    barrier, count = meet(x, z, s, nx, nz, True)
    pl.semaphore_wait(barrier, count)

    def far(i):
        step = (i + 1) // 2
        return lax.rem(jnp.where(lax.rem(i, 2) == 0, nz // 2 + step, nz // 2 + nz - step), nz)

    def c_copy(e, h):
        xx = lax.rem(x + e, nx)
        return sender(sums.at[pl.ds(h * nodes + xx * nz, nz)], peer.at[pl.ds(xx * nz, nz)],
                      c_send.at[e], c_recv.at[e], x, z, 1 - s)
    order = (2, 1, 3, 0)
    for e in order:
        c_copy(e, 1 - s).start()

    def pair_sum(xx, zz):
        return sums[s * nodes + xx * nz + zz] + peer[xx * nz + zz]

    def x_copy(e, c):
        at = pl.ds(c * chunk, chunk)
        return sender(x_out.at[e, at], x_in.at[e, at], x_send.at[e, c], x_recv.at[e, c],
                      lax.rem(x + e, nx), z, s)
    chunks = nz // chunk
    for e in order[:-1]:
        c_copy(e, s).wait_recv()
    c_copy(0, s).wait_recv()

    def fill_x(c, carry):
        for e in order[:-1]:
            def one(j, inner):
                i = c * chunk + j
                x_out[e, i] = packed(pair_sum(lax.rem(x + e, nx), lax.rem(z + far(i), nz)), plain)
                return inner
            lax.fori_loop(0, chunk, one, 0)
            x_copy(e, c).start()
        return carry
    lax.fori_loop(0, chunks, fill_x, 0)

    def z_copy(i):
        return sender(z_out.at[i], z_in.at[i], z_send.at[i], z_recv.at[i], x, lax.rem(z + far(i), nz), s)

    def fill_z(c, carry):
        for e in order[:-1]:
            x_copy(e, c).wait_recv()

        def one(j, inner):
            i = c * chunk + j
            acc = pair_sum(x, lax.rem(z + far(i), nz))
            for e in range(1, nx):
                acc = acc + unpacked(x_in[e, i], plain)
            z_out[i] = packed(acc, plain)
            own_z[...] = acc

            @pl.when(i < nz - 1)
            def _():
                z_copy(i).start()
            return inner
        lax.fori_loop(0, chunk, one, 0)
        return carry
    lax.fori_loop(0, chunks, fill_z, 0)
    total[...] = own_z[...]

    def take_z(i, carry):
        z_copy(i).wait_recv()
        total[...] = total[...] + unpacked(z_in[i], plain)
        return carry
    lax.fori_loop(0, nz - 1, take_z, 0)

    rho2 = jnp.concatenate([rho[...], rho[...]], axis=0)
    anchor = sum(basis[d:d + 1, :] * cons[d] for d in range(degrees))
    target = total[plain:, :] - dual[...] - rho2 * (gain[...] - anchor)
    new = gain[...] + eliminate(total, target, rho[...], full, directions)
    gain_new[...] = new
    weighted = new + dual[...] / rho2
    left = lax.broadcasted_iota(jnp.int32, (2 * directions, 2 * HALF), 1) < HALF

    def folded(d):
        part = basis[d:d + 1, :] * weighted
        return part + pltpu.roll(part, HALF, axis=1)
    pair = degrees // 2
    both = jnp.concatenate([jnp.where(left, folded(d), folded(d + pair)) for d in range(pair)], axis=0)
    pieces, piece = part_out.shape[0], part_out.shape[1]
    for m in range(pieces):
        part_out[m] = both[m * piece:(m + 1) * piece, :]

    near = [(e, f) for e in range(nx) for f in range(2) if e + f > 0]

    def other(e, f):
        return lax.rem(x + e, nx), s + f - 2 * s * f

    def p_copy(e, f):
        xx, ss = other(e, f)
        return sender(part_out.at[xx * 2 + ss], part_in.at[e * 2 + f], p_send.at[e * 2 + f],
                      p_recv.at[e * 2 + f], xx, z, ss)
    for e, f in near:
        p_copy(e, f).start()
    acc = part_out[x * 2 + s]
    for e, f in near:
        p_copy(e, f).wait_recv()
        acc = acc + part_in[e * 2 + f]
    ring_in[z] = acc

    def r_copy(d):
        zz = lax.rem(z + d, nz)
        return sender(ring_in.at[z], ring_in.at[z], r_send.at[d], r_recv.at[d], x, zz, s)

    def start_r(i, carry):
        r_copy(far(i)).start()
        return carry
    lax.fori_loop(0, nz - 1, start_r, 0)

    def take_r(i, carry):
        d = far(i)
        zz = lax.rem(z + nz - d, nz)
        sender(ring_in.at[zz], ring_in.at[zz], r_send.at[d], r_recv.at[d], x, z, s).wait_recv()
        return carry
    lax.fori_loop(0, nz - 1, take_r, 0)
    acc = ring_in[0]
    for i in range(1, nz):
        acc = acc + ring_in[i]
    me = x * 2 + s
    last_in[me] = acc

    def l_copy(e, f, m):
        xx, ss = other(e, f)
        return sender(last_in.at[m], last_in.at[m], l_send.at[e * 2 + f], l_recv.at[e * 2 + f], xx, z, ss)
    for e, f in near:
        l_copy(e, f, me).start()
    for e, f in near:
        back = lax.rem(x + nx - e, nx) * 2 + (s + f - 2 * s * f)
        l_copy(e, f, back).wait_recv()
    both = jnp.concatenate([last_in[m] for m in range(pieces)], axis=0)
    wide = 2 * directions
    summed = [None] * degrees
    for d in range(pair):
        rows = both[d * wide:(d + 1) * wide, :]
        turned = pltpu.roll(rows, HALF, axis=1)
        summed[d] = jnp.where(left, rows, turned)
        summed[d + pair] = jnp.where(left, turned, rows)
    fit = None
    for d in range(degrees):
        coeff = sum(inverse[d][q] * summed[q] for q in range(degrees))
        cons_new[d] = coeff
        term = basis[d:d + 1, :] * coeff
        fit = term if fit is None else fit + term
    dual_new[...] = dual[...] + rho2 * (new - fit)

    for e in range(nx):
        c_copy(e, 1 - s).wait_send()

    def sent_x(c, carry):
        for e in range(1, nx):
            x_copy(e, c).wait_send()
        return carry
    lax.fori_loop(0, chunks, sent_x, 0)

    def sent_z(i, carry):
        z_copy(i).wait_send()
        r_copy(i + 1).wait_send()
        return carry
    lax.fori_loop(0, nz - 1, sent_z, 0)
    for e, f in near:
        p_copy(e, f).wait_send()
        l_copy(e, f, me).wait_send()


def finish(sums, gain, dual, cons, basis, rho, inverse, nx, nz):
    vmem = pl.BlockSpec(memory_space=pltpu.VMEM)
    dma = pltpu.SemaphoreType.DMA
    degrees, directions = basis.shape[0], rho.shape[0]
    terms, lanes = sums.shape[1:]
    wire = terms + 2 * directions
    pieces = 2 * nx
    piece = degrees * 2 * directions // 2 // pieces
    chunks = nz // 4
    return pl.pallas_call(
        functools.partial(finish_kernel, nx, nz, inverse),
        out_shape=(jax.ShapeDtypeStruct(gain.shape, F32), jax.ShapeDtypeStruct(cons.shape, F32),
                   jax.ShapeDtypeStruct(gain.shape, F32)),
        in_specs=[vmem] * 6,
        out_specs=(vmem, vmem, vmem),
        scratch_shapes=[
            pltpu.VMEM((nx * nz, terms, lanes), F32),
            pltpu.VMEM((nx, nz, wire, lanes), BF),
            pltpu.VMEM((nx, nz, wire, lanes), BF),
            pltpu.VMEM((nz, wire, lanes), BF),
            pltpu.VMEM((nz, wire, lanes), BF),
            pltpu.VMEM((terms, lanes), F32),
            pltpu.VMEM((terms, lanes), F32),
            pltpu.VMEM((2, directions * directions, lanes), F32),
            pltpu.VMEM((pieces, piece, lanes), F32),
            pltpu.VMEM((pieces, piece, lanes), F32),
            pltpu.VMEM((nz, piece, lanes), F32),
            pltpu.VMEM((pieces, piece, lanes), F32),
            dma((nx,)), dma((nx,)), dma((nx, chunks)), dma((nx, chunks)), dma((nz,)), dma((nz,)),
            dma((pieces,)), dma((pieces,)), dma((nz,)), dma((nz,)), dma((pieces,)), dma((pieces,)),
        ],
        compiler_params=pltpu.CompilerParams(collective_id=1, has_side_effects=True,
                                             vmem_limit_bytes=40 * 1024 * 1024),
        name="finish",
    )(sums, gain, dual, cons, basis, rho)


def to_lanes(x):
    h, c, s, k = x.shape
    x = jnp.pad(x, ((0, 0), (0, 0), (0, HALF - s), (0, 0)))
    return jnp.transpose(x, (1, 3, 0, 2)).reshape(c * k, h * HALF)


def from_lanes(x, stations):
    rows, lanes = x.shape
    x = x.reshape(2, rows // 2, lanes // HALF, HALF)[..., :stations]
    return jnp.transpose(x, (2, 0, 3, 1))


def gain_table(gains):
    n, c, s, k = gains.shape
    x = jnp.pad(jnp.transpose(gains, (0, 3, 1, 2)).reshape(n, k * c, s), ((0, 0), (0, 0), (0, HALF - s)))
    head = lax.reduce_precision(x, 8, 7)
    return jnp.concatenate([head, x - head], axis=-1).astype(BF)


def body(sky, seen, keep, tile_owner, tile_channel, tile_base, pairs, gains, duals, consensus, rho):
    channels_here, _, stations, directions = gains.shape
    chan_count = lax.axis_size(("chan_0", "chan_1"))
    sub_count = lax.axis_size("sub")
    half_count = channels_here // sub_count
    devices = chan_count * sub_count
    sub_index = lax.axis_index("sub")
    chan_index = lax.axis_index(("chan_0", "chan_1"))

    nx, nz = lax.axis_size(XS), lax.axis_size(ZS)
    table = gather_gains(gain_table(gains), nx, nz)
    owner = tile_owner[:, 0]
    order, groups = tile_order(tile_base, pairs.shape[0])
    home = ((tile_channel // half_count) * chan_count + owner) * half_count + tile_channel % half_count
    sums = tile_sums(sky, seen, keep, order, groups, owner * channels_here + tile_channel, home,
                     tile_base, pairs, table, devices)

    my_gains = lax.dynamic_slice_in_dim(gains, sub_index * half_count, half_count, 0)
    channels = channels_here * chan_count
    first_channel = (chan_index * sub_count + sub_index) * half_count
    my_basis = lax.dynamic_slice_in_dim(legendre_rows(channels), first_channel, half_count, 1)
    basis = jnp.repeat(my_basis, HALF, axis=1)
    cons = jax.vmap(lambda c: to_lanes(jnp.stack([c, c])))(consensus)
    gain_l, dual_l = to_lanes(my_gains), to_lanes(duals)
    rho_l = jnp.broadcast_to(rho[:, None], (directions, 2 * HALF))
    new_l, fitted, dual_new = finish(sums, gain_l, dual_l, cons, basis, rho_l,
                                     gram_inverse(channels).tolist(), nx, nz)
    consensus_new = jax.vmap(lambda x: from_lanes(x, stations)[0])(fitted)
    return from_lanes(new_l, stations), consensus_new, from_lanes(dual_new, stations)


def solution(mesh):
    groups, subs = mesh.shape["groups"], mesh.shape["sub"]
    torus = Mesh(mesh.devices.reshape(groups, 4, mesh.shape["chan"] // 4, subs), GROUPS_CHAN_SUB)
    return jax.shard_map(
        body,
        mesh=torus,
        in_specs=(
            P(GROUPS_CHAN_SUB, None, None, None),
            P(GROUPS_CHAN_SUB, None, None),
            P(GROUPS_CHAN_SUB, None),
            P(GROUPS_CHAN_SUB, None),
            P(GROUPS_CHAN_SUB),
            P(GROUPS_CHAN_SUB),
            P(),
            P(GROUPS_CHAN, None, None, None),
            P(GROUPS_CHAN_SUB, None, None, None),
            P("groups", None, None, None),
            P(),
        ),
        out_specs=(
            P(GROUPS_CHAN_SUB, None, None, None),
            P("groups", None, None, None),
            P(GROUPS_CHAN_SUB, None, None, None),
        ),
        check_vma=False,
    )
```

```python
import functools

import jax
import jax.numpy as jnp
import numpy as np
from jax import lax
from jax.experimental import pallas as pl
from jax.experimental.pallas import tpu as pltpu
from jax.sharding import Mesh
from jax.sharding import PartitionSpec as P

GROUPS_CHAN_SUB = ("groups", "chan_0", "chan_1", "sub")
GROUPS_CHAN = ("groups", "chan_0", "chan_1")
BF, F32 = jnp.bfloat16, jnp.float32
GROUP = 8
HALF = 64


def term_rows(directions):
    real, imag = {}, {}
    for k in range(directions):
        for m in range(k, directions):
            real[k, m] = len(real)
    for k in range(directions):
        for m in range(k + 1, directions):
            imag[k, m] = len(real) + len(imag)
    return real, imag


def legendre(first, channels):
    lane = lax.broadcasted_iota(jnp.int32, (1, 2 * HALF), 1)
    place = (first + lane // HALF).astype(F32)
    x = (2.0 * place - (channels - 1)) / max(channels - 1, 1)
    return [jnp.ones_like(x), x, 0.5 * (3.0 * x * x - 1.0), 0.5 * (5.0 * x * x * x - 3.0 * x)]


def gram_inverse(channels):
    x = (2.0 * np.arange(channels, dtype=np.float64) - (channels - 1)) / max(channels - 1, 1)
    basis = np.stack([np.ones_like(x), x, 0.5 * (3 * x * x - 1), 0.5 * (5 * x * x * x - 3 * x)])
    return np.linalg.inv(basis @ basis.T)


def tile_order(base, bases, slots):
    tiles = base.shape[1]
    padded_bases = -(-bases // 16) * 16
    member = lax.broadcasted_iota(jnp.int32, (padded_bases, tiles), 0) == base
    hit = jnp.where(member, 1.0, 0.0)
    before = jnp.where(lax.broadcasted_iota(jnp.int32, (tiles, tiles), 0)
                       < lax.broadcasted_iota(jnp.int32, (tiles, tiles), 1), 1.0, 0.0).astype(BF)
    rank = jnp.dot(hit.astype(BF), before, preferred_element_type=F32)
    counts = jnp.sum(hit, axis=1, keepdims=True).astype(jnp.int32)
    groups = lax.shift_right_logical(counts + (GROUP - 1), GROUP.bit_length() - 1).astype(F32)
    lower = jnp.where(lax.broadcasted_iota(jnp.int32, (padded_bases, padded_bases), 1)
                      < lax.broadcasted_iota(jnp.int32, (padded_bases, padded_bases), 0), 1.0, 0.0).astype(BF)
    start = jnp.dot(lower, jnp.broadcast_to(groups, (padded_bases, tiles)).astype(BF),
                    preferred_element_type=F32)
    where = jnp.sum(jnp.where(member, rank + GROUP * start, 0.0), axis=0, keepdims=True).astype(jnp.int32)
    chosen = jnp.where(lax.broadcasted_iota(jnp.int32, (slots, tiles), 0) == where, 1.0, 0.0).astype(BF)
    tile = lax.broadcasted_iota(jnp.int32, (8, tiles), 1)
    kind = lax.broadcasted_iota(jnp.int32, (8, tiles), 0)
    digits = jnp.where(kind == 0, lax.shift_right_logical(tile, 4),
                       jnp.where(kind == 1, jnp.bitwise_and(tile, 15), 1)).astype(F32).astype(BF)
    found = lax.dot_general(digits, chosen, (((1,), (1,)), ((), ())), preferred_element_type=F32)
    named = jnp.where(found[2:3] > 0.5, 16.0 * found[0:1] + found[1:2], float(tiles)).astype(jnp.int32)
    total = jnp.broadcast_to(jnp.sum(groups, axis=0, keepdims=True), (1, 128)).astype(jnp.int32)
    return named, total


def tile_kernel(half_count, order, groups, owner, channel, base, sky, seen, keep, pairs, table, out, onehot, *buffers):
    tiles, coupled, rows = sky.shape
    directions = coupled // 2
    bases = pairs.shape[0]
    real, imag = term_rows(directions)
    n_terms = directions * directions + 2 * directions
    devices = out.shape[0] - 1
    channels_here = table.shape[0] // (devices // 2)
    chans = devices // 2
    buffers = (buffers[0::2], buffers[1::2])

    station = lax.rem(lax.broadcasted_iota(jnp.int32, (2 * HALF, rows), 0), HALF)
    for b in range(bases):
        for side in range(2):
            onehot[b, :, side * rows:(side + 1) * rows] = jnp.where(
                station == pairs[b, side:side + 1, :], 1.0, 0.0).astype(BF)

    def clear(i, carry):
        out[i] = jnp.zeros((n_terms, 2 * HALF), F32)
        return carry
    lax.fori_loop(0, devices + 1, clear, 0)
    lane = lax.broadcasted_iota(jnp.int32, (1, 2 * HALF), 1)

    def chosen(g):
        first = order[0, jnp.maximum(g, 0) * GROUP]
        return onehot.at[base[jnp.minimum(first, tiles - 1)]]

    def load(g, into):
        sky_s, seen_s, keep_s, gain_s, near_far, _, _ = buffers[into]
        for t in range(GROUP):
            named = order[0, g * GROUP + t]
            tile = jnp.where(named < tiles, named, 0)
            sky_s[pl.ds(t, coupled, stride=GROUP), :] = sky[tile].astype(F32)
            seen_s[pl.ds(t, 2, stride=GROUP), :] = seen[tile].astype(F32)
            keep_s[pl.ds(t, 1), :] = keep[pl.ds(tile, 1), :]
            gain_s[pl.ds(t, coupled, stride=GROUP), :] = table[owner[tile] * channels_here + channel[tile]].astype(F32)
        near_far[...] = jnp.dot(gain_s[...].astype(BF), chosen(g)[...], preferred_element_type=F32)

    def products(of):
        sky_s, seen_s, keep_s, _, near_far, terms, _ = buffers[of]
        kept = keep_s[...] > 0

        def block(ref, i):
            return ref[i * GROUP:(i + 1) * GROUP, :]

        res_r = jnp.where(kept, block(seen_s, 0), 0.0)
        res_i = jnp.where(kept, block(seen_s, 1), 0.0)
        a_r, a_i, b_r, b_i = [], [], [], []
        mod_r = mod_i = None
        for k in range(directions):
            c_r = jnp.where(kept, block(sky_s, 2 * k), 0.0)
            c_i = jnp.where(kept, block(sky_s, 2 * k + 1), 0.0)
            p_r, p_i = (block(near_far, c * directions + k)[:, :rows] for c in range(2))
            q_r, q_i = (block(near_far, c * directions + k)[:, rows:] for c in range(2))
            x_r = c_r * q_r + c_i * q_i
            x_i = c_i * q_r - c_r * q_i
            a_r.append(x_r)
            a_i.append(x_i)
            b_r.append(c_r * p_r - c_i * p_i)
            b_i.append(-(c_r * p_i + c_i * p_r))
            m_r = p_r * x_r - p_i * x_i
            m_i = p_r * x_i + p_i * x_r
            mod_r = m_r if mod_r is None else mod_r + m_r
            mod_i = m_i if mod_i is None else mod_i + m_i
        res_r = res_r - mod_r
        res_i = res_i - mod_i

        for side, (v_r, v_i, w_r, w_i) in enumerate(
                ((a_r, a_i, res_r, res_i), (b_r, b_i, res_r, -res_i))):
            pending = {}

            def put(j, value):
                pending[j] = value
                lo = j - j % 2
                if lo in pending and lo + 1 in pending:
                    both = jnp.concatenate([pending.pop(lo), pending.pop(lo + 1)], axis=0)
                    terms[lo * GROUP:(lo + 2) * GROUP, side * rows:(side + 1) * rows] = both.astype(BF)

            for (k, m), j in real.items():
                put(j, v_r[k] * v_r[m] + v_i[k] * v_i[m])
            for (k, m), j in imag.items():
                put(j, v_r[k] * v_i[m] - v_i[k] * v_r[m])
            first = directions * directions
            for k in range(directions):
                put(first + k, v_r[k] * w_r + v_i[k] * w_i)
            for k in range(directions):
                put(first + directions + k, v_r[k] * w_i - v_i[k] * w_r)

    def station_sums(g, of):
        terms, sums = buffers[of][5:]
        sums[...] = lax.dot_general(terms[...], chosen(g)[...], (((1,), (1,)), ((), ())),
                                    preferred_element_type=F32)

    def add_up(g, of):
        sums = buffers[of][6]
        for t in range(GROUP):
            named = jnp.where(g < 0, tiles, order[0, jnp.maximum(g, 0) * GROUP + t])
            tile = jnp.where(named < tiles, named, 0)
            mine = channel[tile]
            row = jnp.where(named < tiles, (mine // half_count) * chans + owner[tile], devices)
            part = jnp.where(lane // HALF == lax.rem(mine, half_count),
                             sums[pl.ds(t, n_terms, stride=GROUP), :], 0.0)
            out[row] = out[row] + part

    def step(g, of):
        station_sums(g - 2, of)
        add_up(g - 3, 1 - of)
        load(g, of)
        products(1 - of)

    def two(i, carry):
        step(2 * i, 0)
        step(2 * i + 1, 1)
        return carry

    lax.fori_loop(0, (groups[0, 0] + 4) // 2, two, 0)


def tile_sums(sky, seen, keep, order, groups, owner, channel, base, pairs, table, devices, half_count):
    tiles, directions, _, rows = sky.shape
    n_terms = directions * directions + 2 * directions
    bases = pairs.shape[0]
    smem = pl.BlockSpec(memory_space=pltpu.SMEM)
    vmem = pl.BlockSpec(memory_space=pltpu.VMEM)
    coupled = 2 * directions
    return pl.pallas_call(
        functools.partial(tile_kernel, half_count),
        out_shape=jax.ShapeDtypeStruct((devices + 1, n_terms, 2 * HALF), F32),
        in_specs=[smem] * 5 + [vmem] * 5,
        out_specs=vmem,
        scratch_shapes=[pltpu.VMEM((bases, 2 * HALF, 2 * rows), BF)] + [
            shape for shape in (
                pltpu.VMEM((coupled * GROUP, rows), F32),
                pltpu.VMEM((2 * GROUP, rows), F32),
                pltpu.VMEM((GROUP, rows), jnp.int32),
                pltpu.VMEM((coupled * GROUP, 2 * HALF), F32),
                pltpu.VMEM((coupled * GROUP, 2 * rows), F32),
                pltpu.VMEM((n_terms * GROUP, 2 * rows), BF),
                pltpu.VMEM((n_terms * GROUP, 2 * HALF), F32),
            ) for _ in range(2)
        ],
        compiler_params=pltpu.CompilerParams(vmem_limit_bytes=18 * 1024 * 1024),
        name="tile_sums",
    )(order, groups, owner, channel, base, sky.reshape(tiles, coupled, rows), seen, keep, pairs, table)


def eliminate(total, target, rho, full, directions):
    real, imag = term_rows(directions)
    lanes = total.shape[-1]
    for k in range(directions):
        for m in range(directions):
            re = real[min(k, m), max(k, m)]
            value = total[re:re + 1, :]
            if k == m:
                value = value + rho[k:k + 1, :]
                full[1, k * directions + m:k * directions + m + 1, :] = jnp.zeros((1, lanes), F32)
            else:
                im = imag[min(k, m), max(k, m)]
                imv = total[im:im + 1, :]
                full[1, k * directions + m:k * directions + m + 1, :] = imv if k < m else -imv
            full[0, k * directions + m:k * directions + m + 1, :] = value
    row_r = [full[0, k * directions:(k + 1) * directions, :] for k in range(directions)]
    row_i = [full[1, k * directions:(k + 1) * directions, :] for k in range(directions)]
    t_r = [target[k:k + 1, :] for k in range(directions)]
    t_i = [target[directions + k:directions + k + 1, :] for k in range(directions)]
    for k in range(directions):
        inv = 1.0 / row_r[k][k:k + 1, :]
        row_r[k] = row_r[k] * inv
        row_i[k] = row_i[k] * inv
        t_r[k] = t_r[k] * inv
        t_i[k] = t_i[k] * inv
        for m in range(directions):
            if m == k:
                continue
            f_r = row_r[m][k:k + 1, :]
            f_i = row_i[m][k:k + 1, :]
            row_r[m], row_i[m] = (row_r[m] - (f_r * row_r[k] - f_i * row_i[k]),
                                  row_i[m] - (f_r * row_i[k] + f_i * row_r[k]))
            t_r[m], t_i[m] = (t_r[m] - (f_r * t_r[k] - f_i * t_i[k]),
                              t_i[m] - (f_r * t_i[k] + f_i * t_r[k]))
    return jnp.concatenate(t_r + t_i, axis=0)


XS, ZS = "chan_0", "chan_1"


def place():
    return lax.axis_index(XS), lax.axis_index(ZS), lax.axis_index("sub")


def sender(src, dst, send_sem, recv_sem, x, z, s):
    return pltpu.make_async_remote_copy(
        src_ref=src, dst_ref=dst, send_sem=send_sem, recv_sem=recv_sem,
        device_id={XS: x, ZS: z, "sub": s}, device_id_type=pl.DeviceIdType.MESH)


def meet(x, z, s, nx, nz, crossed):
    barrier = pltpu.get_barrier_semaphore()

    def ring(d, carry):
        pl.semaphore_signal(barrier, inc=1, device_id={XS: x, ZS: lax.rem(z + d, nz), "sub": s},
                            device_id_type=pl.DeviceIdType.MESH)
        return carry
    lax.fori_loop(1, nz, ring, 0)
    near = [(e, f) for e in range(nx) for f in range(2) if e + f > 0 and (crossed or e * f == 0)]
    for e, f in near:
        pl.semaphore_signal(barrier, inc=1,
                            device_id={XS: lax.rem(x + e, nx), ZS: z, "sub": s + f - 2 * s * f},
                            device_id_type=pl.DeviceIdType.MESH)
    return barrier, nz - 1 + len(near)


def outward(i, nz):
    return jnp.where(lax.rem(i, 2) == 0, i // 2 + 1, nz - 1 - i // 2)


def gather_kernel(nx, nz, bases, gains, base, table, order, groups, wide, mine,
                  z_recv, z_send, x_recv, x_send, c_recv, c_send):
    x, z, s = place()
    here, half = mine.shape[0], mine.shape[0] // 2
    stations = gains.shape[2]
    barrier, count = meet(x, z, s, nx, nz, False)
    wide[...] = jnp.zeros(wide.shape, F32)
    head = gains[...].astype(BF).astype(F32)
    wide[:, :, :stations] = head
    wide[:, :, HALF:HALF + stations] = gains[...] - head
    mine[...] = wide[...].astype(BF)
    table[pl.ds((x * nz + z) * here + s * half, half)] = mine[pl.ds(s * half, half)]
    pl.semaphore_wait(barrier, count)

    def block(xx, zz):
        return table.at[pl.ds((xx * nz + zz) * here + s * half, half)]

    def rows(xx, h):
        return table.at[pl.ds(xx * nz * here, nz * here)].reshape(nz, here, *mine.shape[1:]).at[:, pl.ds(h * half, half)]

    own = mine.at[pl.ds(s * half, half)]

    def z_copy(d):
        return sender(own, block(x, z), z_send.at[d], z_recv.at[d], x, lax.rem(z + d, nz), s)

    def start_z(i, carry):
        z_copy(outward(i, nz)).start()
        return carry
    lax.fori_loop(0, nz - 1, start_z, 0)

    def x_copy(src, zz, d, e):
        return sender(src, block(x, zz), x_send.at[e, d], x_recv.at[e, d], lax.rem(x + e, nx), z, s)
    for e in range(1, nx):
        x_copy(own, z, 0, e).start()
    order[...], groups[...] = tile_order(base[...], bases, order.shape[1])

    def pass_on(i, carry):
        d = outward(i, nz)
        zz = lax.rem(z + nz - d, nz)
        sender(own, block(x, zz), z_send.at[d], z_recv.at[d], x, z, s).wait_recv()
        for e in range(1, nx):
            x_copy(block(x, zz), zz, d, e).start()
        return carry
    lax.fori_loop(0, nz - 1, pass_on, 0)

    def c_copy(e, h):
        xx = lax.rem(x + nx - e, nx)
        return sender(rows(xx, h), rows(xx, h), c_send.at[e], c_recv.at[e], x, z, 1 - s)
    for e in (0, 1, 3, 2):
        if e > 0:
            xx = lax.rem(x + nx - e, nx)

            def arrived(d, carry):
                zz = lax.rem(z + nz - d, nz)
                sender(own, block(xx, zz), x_send.at[e, d], x_recv.at[e, d], x, z, s).wait_recv()
                return carry
            lax.fori_loop(0, nz, arrived, 0)
        c_copy(e, s).start()
    for e in range(nx):
        c_copy(e, 1 - s).wait_recv()

    def done_z(d, carry):
        z_copy(d).wait_send()
        return carry
    lax.fori_loop(1, nz, done_z, 0)
    for e in range(1, nx):
        def done_x(d, carry):
            x_copy(own, z, d, e).wait_send()
            return carry
        lax.fori_loop(0, nz, done_x, 0)
    for e in range(nx):
        c_copy(e, s).wait_send()


def gather_gains(gains, base, bases, nx, nz):
    vmem = pl.BlockSpec(memory_space=pltpu.VMEM)
    dma = pltpu.SemaphoreType.DMA
    here, rows, _ = gains.shape
    slots = -(-(base.shape[1] + GROUP * (bases + 6)) // 128) * 128
    return pl.pallas_call(
        functools.partial(gather_kernel, nx, nz, bases),
        out_shape=(jax.ShapeDtypeStruct((nx * nz * here, rows, 2 * HALF), BF),
                   jax.ShapeDtypeStruct((1, slots), jnp.int32), jax.ShapeDtypeStruct((1, 128), jnp.int32)),
        in_specs=[vmem, vmem],
        out_specs=(vmem, vmem, vmem),
        scratch_shapes=[pltpu.VMEM((here, rows, 2 * HALF), F32), pltpu.VMEM((here, rows, 2 * HALF), BF),
                        dma((nz,)), dma((nz,)), dma((nx, nz)), dma((nx, nz)), dma((nx,)), dma((nx,))],
        compiler_params=pltpu.CompilerParams(collective_id=0, has_side_effects=True,
                                             vmem_limit_bytes=8 * 1024 * 1024),
        name="gather_gains",
    )(gains, base)


def packed(v, plain):
    head = v[plain:].astype(BF)
    tail = v[plain:] - head.astype(F32)
    return jnp.concatenate([v[:plain].astype(BF), head, tail.astype(BF)], axis=0)


def unpacked(w, plain):
    v = w.astype(F32)
    mid = (v.shape[0] + plain) // 2
    return jnp.concatenate([v[:plain], v[plain:mid] + v[mid:]], axis=0)


def finish_kernel(nx, nz, inverse, sums, gains, duals, cons, rho, gain_new, cons_new, dual_new,
                  peer, two_out, two_in, x_out, x_in, z_out, z_in, own_z, total, full, wide,
                  part_out, part_in, ring_in, last_in,
                  c_send, c_recv, t_send, t_recv, x_send, x_recv, z_send, z_recv,
                  p_send, p_recv, r_send, r_recv, l_send, l_recv):
    x, z, s = place()
    directions = rho.shape[0]
    degrees, _, stations = cons.shape
    half_count = duals.shape[0]
    plain = directions * directions
    chunk = 4
    nodes = nx * nz
    barrier, count = meet(x, z, s, nx, nz, True)

    wide[...] = jnp.zeros(wide.shape, F32)
    for h in range(half_count):
        wide[0, :, h * HALF:h * HALF + stations] = gains[s * half_count + h]
        wide[1, :, h * HALF:h * HALF + stations] = duals[h]
        for d in range(degrees):
            wide[2 + d, :, h * HALF:h * HALF + stations] = cons[d]
    basis = legendre(((x * nz + z) * 2 + s) * half_count, 2 * nodes * half_count)
    pl.semaphore_wait(barrier, count)

    def far(i):
        step = (i + 1) // 2
        return lax.rem(jnp.where(lax.rem(i, 2) == 0, nz // 2 + step, nz // 2 + nz - step), nz)

    def c_copy(e, h):
        xx = lax.rem(x + e, nx)
        return sender(sums.at[pl.ds(h * nodes + xx * nz, nz)], peer.at[pl.ds(xx * nz, nz)],
                      c_send.at[e], c_recv.at[e], x, z, 1 - s)
    across, right, left_ = nx // 2, 1, nx - 1
    order = (across, right, left_, 0)
    for e in order:
        c_copy(e, 1 - s).start()

    def pair_sum(xx, zz):
        return sums[s * nodes + xx * nz + zz] + peer[xx * nz + zz]

    chunks = nz // chunk
    share = chunk // 2
    def t_copy(side, c):
        at = pl.ds(c * chunk + side * share, share)
        return sender(two_out.at[at], two_in.at[at], t_send.at[side, c], t_recv.at[side, c],
                      lax.rem(x + (right, left_)[side], nx), z, s)
    c_copy(across, s).wait_recv()

    def fill_two(c, carry):
        def one(j, inner):
            i = c * chunk + j
            two_out[i] = packed(pair_sum(lax.rem(x + across, nx), lax.rem(z + far(i), nz)), plain)
            return inner
        lax.fori_loop(0, chunk, one, 0)
        for side in range(2):
            t_copy(side, c).start()
        return carry
    lax.fori_loop(0, chunks, fill_two, 0)

    def x_copy(side, c):
        at = pl.ds(c * chunk, chunk)
        return sender(x_out.at[side, at], x_in.at[side, at], x_send.at[side, c], x_recv.at[side, c],
                      lax.rem(x + (right, left_)[side], nx), z, s)
    c_copy(right, s).wait_recv()
    c_copy(left_, s).wait_recv()

    def fill_x(c, carry):
        for side in range(2):
            t_copy(side, c).wait_recv()
            xx = lax.rem(x + (right, left_)[side], nx)

            def relayed(j, inner):
                i = c * chunk + side * share + j
                x_out[side, i] = packed(pair_sum(xx, lax.rem(z + far(i), nz)) + unpacked(two_in[i], plain), plain)
                return inner

            def plainly(j, inner):
                i = c * chunk + (1 - side) * share + j
                x_out[side, i] = packed(pair_sum(xx, lax.rem(z + far(i), nz)), plain)
                return inner
            lax.fori_loop(0, share, relayed, 0)
            lax.fori_loop(0, share, plainly, 0)
            x_copy(side, c).start()
        return carry
    lax.fori_loop(0, chunks, fill_x, 0)
    c_copy(0, s).wait_recv()

    def z_copy(i):
        return sender(z_out.at[i], z_in.at[i], z_send.at[i], z_recv.at[i], x, lax.rem(z + far(i), nz), s)

    def fill_z(c, carry):
        for side in range(2):
            x_copy(side, c).wait_recv()

        def one(j, inner):
            i = c * chunk + j
            acc = pair_sum(x, lax.rem(z + far(i), nz))
            for side in range(2):
                acc = acc + unpacked(x_in[side, i], plain)
            z_out[i] = packed(acc, plain)
            own_z[...] = acc

            @pl.when(i < nz - 1)
            def _():
                z_copy(i).start()
            return inner
        lax.fori_loop(0, chunk, one, 0)
        return carry
    lax.fori_loop(0, chunks, fill_z, 0)
    total[...] = own_z[...]

    def take_z(i, carry):
        z_copy(i).wait_recv()
        total[...] = total[...] + unpacked(z_in[i], plain)
        return carry
    lax.fori_loop(0, nz - 1, take_z, 0)

    rho2 = jnp.concatenate([rho[...], rho[...]], axis=0)
    gain, dual = wide[0], wide[1]
    anchor = sum(basis[d] * wide[2 + d] for d in range(degrees))
    target = total[plain:, :] - dual - rho2 * (gain - anchor)
    new = gain + eliminate(total, target, rho[...], full, directions)
    for h in range(half_count):
        gain_new[h] = new[:, h * HALF:h * HALF + stations]
    weighted = new + dual / rho2
    left = lax.broadcasted_iota(jnp.int32, (2 * directions, 2 * HALF), 1) < HALF

    def folded(d):
        part = basis[d] * weighted
        return part + pltpu.roll(part, HALF, axis=1)
    pair = degrees // 2
    both = jnp.concatenate([jnp.where(left, folded(d), folded(d + pair)) for d in range(pair)], axis=0)
    pieces, piece = part_out.shape[0], part_out.shape[1]
    for m in range(pieces):
        part_out[m] = both[m * piece:(m + 1) * piece, :]

    near = [(e, f) for e in range(nx) for f in range(2) if e + f > 0]

    def other(e, f):
        return lax.rem(x + e, nx), s + f - 2 * s * f

    def p_copy(e, f):
        xx, ss = other(e, f)
        return sender(part_out.at[xx * 2 + ss], part_in.at[e * 2 + f], p_send.at[e * 2 + f],
                      p_recv.at[e * 2 + f], xx, z, ss)
    for e, f in near:
        p_copy(e, f).start()
    acc = part_out[x * 2 + s]
    for e, f in near:
        p_copy(e, f).wait_recv()
        acc = acc + part_in[e * 2 + f]
    ring_in[z] = acc

    def r_copy(d):
        zz = lax.rem(z + d, nz)
        return sender(ring_in.at[z], ring_in.at[z], r_send.at[d], r_recv.at[d], x, zz, s)

    def start_r(i, carry):
        r_copy(far(i)).start()
        return carry
    lax.fori_loop(0, nz - 1, start_r, 0)

    def take_r(i, carry):
        d = far(i)
        zz = lax.rem(z + nz - d, nz)
        sender(ring_in.at[zz], ring_in.at[zz], r_send.at[d], r_recv.at[d], x, z, s).wait_recv()
        return carry
    lax.fori_loop(0, nz - 1, take_r, 0)
    acc = ring_in[0]
    for i in range(1, nz):
        acc = acc + ring_in[i]
    me = x * 2 + s
    last_in[me] = acc

    def l_copy(e, f, m):
        xx, ss = other(e, f)
        return sender(last_in.at[m], last_in.at[m], l_send.at[e * 2 + f], l_recv.at[e * 2 + f], xx, z, ss)
    for e, f in near:
        l_copy(e, f, me).start()
    for e, f in near:
        back = lax.rem(x + nx - e, nx) * 2 + (s + f - 2 * s * f)
        l_copy(e, f, back).wait_recv()
    both = jnp.concatenate([last_in[m] for m in range(pieces)], axis=0)
    wide = 2 * directions
    summed = [None] * degrees
    for d in range(pair):
        rows = both[d * wide:(d + 1) * wide, :]
        turned = pltpu.roll(rows, HALF, axis=1)
        summed[d] = jnp.where(left, rows, turned)
        summed[d + pair] = jnp.where(left, turned, rows)
    fit = None
    for d in range(degrees):
        coeff = sum(inverse[d][q] * summed[q] for q in range(degrees))
        cons_new[d] = coeff[:, :stations]
        term = basis[d] * coeff
        fit = term if fit is None else fit + term
    dual_out = dual + rho2 * (new - fit)
    for h in range(half_count):
        dual_new[h] = dual_out[:, h * HALF:h * HALF + stations]

    for e in range(nx):
        c_copy(e, 1 - s).wait_send()

    def sent_x(c, carry):
        for side in range(2):
            t_copy(side, c).wait_send()
            x_copy(side, c).wait_send()
        return carry
    lax.fori_loop(0, chunks, sent_x, 0)

    def sent_z(i, carry):
        z_copy(i).wait_send()
        r_copy(i + 1).wait_send()
        return carry
    lax.fori_loop(0, nz - 1, sent_z, 0)
    for e, f in near:
        p_copy(e, f).wait_send()
        l_copy(e, f, me).wait_send()


def finish(sums, gains, duals, cons, rho, inverse, nx, nz):
    vmem = pl.BlockSpec(memory_space=pltpu.VMEM)
    dma = pltpu.SemaphoreType.DMA
    degrees, rows, _ = cons.shape
    terms, lanes = sums.shape[1:]
    wire = terms + rows
    pieces = 2 * nx
    piece = degrees * rows // 2 // pieces
    chunks = nz // 4
    return pl.pallas_call(
        functools.partial(finish_kernel, nx, nz, inverse),
        out_shape=(jax.ShapeDtypeStruct(duals.shape, F32), jax.ShapeDtypeStruct(cons.shape, F32),
                   jax.ShapeDtypeStruct(duals.shape, F32)),
        in_specs=[vmem] * 5,
        out_specs=(vmem, vmem, vmem),
        scratch_shapes=[
            pltpu.VMEM((nx * nz, terms, lanes), F32),
            pltpu.VMEM((nz, wire, lanes), BF),
            pltpu.VMEM((nz, wire, lanes), BF),
            pltpu.VMEM((2, nz, wire, lanes), BF),
            pltpu.VMEM((2, nz, wire, lanes), BF),
            pltpu.VMEM((nz, wire, lanes), BF),
            pltpu.VMEM((nz, wire, lanes), BF),
            pltpu.VMEM((terms, lanes), F32),
            pltpu.VMEM((terms, lanes), F32),
            pltpu.VMEM((2, rows * rows // 4, lanes), F32),
            pltpu.VMEM((2 + degrees, rows, lanes), F32),
            pltpu.VMEM((pieces, piece, lanes), F32),
            pltpu.VMEM((pieces, piece, lanes), F32),
            pltpu.VMEM((nz, piece, lanes), F32),
            pltpu.VMEM((pieces, piece, lanes), F32),
            dma((nx,)), dma((nx,)), dma((2, chunks)), dma((2, chunks)), dma((2, chunks)), dma((2, chunks)),
            dma((nz,)), dma((nz,)),
            dma((pieces,)), dma((pieces,)), dma((nz,)), dma((nz,)), dma((pieces,)), dma((pieces,)),
        ],
        compiler_params=pltpu.CompilerParams(collective_id=1, has_side_effects=True,
                                             vmem_limit_bytes=18 * 1024 * 1024),
        name="finish",
    )(sums, gains, duals, cons, rho)


def to_rows(x):
    n, c, s, k = x.shape
    return jnp.transpose(x, (0, 1, 3, 2)).reshape(n, c * k, s)


def from_rows(x):
    n, rows, s = x.shape
    return jnp.transpose(x.reshape(n, 2, rows // 2, s), (0, 1, 3, 2))


def body(sky, seen, keep, tile_owner, tile_channel, tile_base, pairs, gains, duals, consensus, rho):
    channels_here, _, _, directions = gains.shape
    nx, nz = lax.axis_size(XS), lax.axis_size(ZS)
    sub_count = lax.axis_size("sub")
    half_count = channels_here // sub_count
    gain_rows = to_rows(gains)
    table, order, groups = gather_gains(gain_rows, tile_base.reshape(1, -1), pairs.shape[0], nx, nz)
    sums = tile_sums(sky, seen, keep, order, groups, tile_owner[:, 0], tile_channel, tile_base, pairs, table,
                     nx * nz * sub_count, half_count)
    rho_rows = jnp.broadcast_to(rho[:, None], (directions, 2 * HALF))
    gain_new, cons_new, dual_new = finish(sums, gain_rows, to_rows(duals), to_rows(consensus), rho_rows,
                                          gram_inverse(channels_here * nx * nz).tolist(), nx, nz)
    return from_rows(gain_new), from_rows(cons_new), from_rows(dual_new)


def solution(mesh):
    groups, subs = mesh.shape["groups"], mesh.shape["sub"]
    torus = Mesh(mesh.devices.reshape(groups, 4, mesh.shape["chan"] // 4, subs), GROUPS_CHAN_SUB)
    return jax.shard_map(
        body,
        mesh=torus,
        in_specs=(
            P(GROUPS_CHAN_SUB, None, None, None),
            P(GROUPS_CHAN_SUB, None, None),
            P(GROUPS_CHAN_SUB, None),
            P(GROUPS_CHAN_SUB, None),
            P(GROUPS_CHAN_SUB),
            P(GROUPS_CHAN_SUB),
            P(),
            P(GROUPS_CHAN, None, None, None),
            P(GROUPS_CHAN_SUB, None, None, None),
            P("groups", None, None, None),
            P(),
        ),
        out_specs=(
            P(GROUPS_CHAN_SUB, None, None, None),
            P("groups", None, None, None),
            P(GROUPS_CHAN_SUB, None, None, None),
        ),
        check_vma=False,
    )
```

```python
import functools

import jax
import jax.numpy as jnp
import numpy as np
from jax import lax
from jax.experimental import pallas as pl
from jax.experimental.pallas import tpu as pltpu
from jax.sharding import Mesh
from jax.sharding import PartitionSpec as P

GROUPS_CHAN_SUB = ("groups", "chan_0", "chan_1", "sub")
GROUPS_CHAN = ("groups", "chan_0", "chan_1")
BF, F32 = jnp.bfloat16, jnp.float32
GROUP = 8
HALF = 64


def term_rows(directions):
    real, imag = {}, {}
    for k in range(directions):
        for m in range(k, directions):
            real[k, m] = len(real)
    for k in range(directions):
        for m in range(k + 1, directions):
            imag[k, m] = len(real) + len(imag)
    return real, imag


def legendre(first, channels):
    lane = lax.broadcasted_iota(jnp.int32, (1, 2 * HALF), 1)
    place = (first + lane // HALF).astype(F32)
    x = (2.0 * place - (channels - 1)) / max(channels - 1, 1)
    return [jnp.ones_like(x), x, 0.5 * (3.0 * x * x - 1.0), 0.5 * (5.0 * x * x * x - 3.0 * x)]


def gram_inverse(channels):
    x = (2.0 * np.arange(channels, dtype=np.float64) - (channels - 1)) / max(channels - 1, 1)
    basis = np.stack([np.ones_like(x), x, 0.5 * (3 * x * x - 1), 0.5 * (5 * x * x * x - 3 * x)])
    return np.linalg.inv(basis @ basis.T)


def tile_order(base, bases, slots):
    tiles = base.shape[1]
    padded_bases = -(-bases // 16) * 16
    member = lax.broadcasted_iota(jnp.int32, (padded_bases, tiles), 0) == base
    hit = jnp.where(member, 1.0, 0.0)
    before = jnp.where(lax.broadcasted_iota(jnp.int32, (tiles, tiles), 0)
                       < lax.broadcasted_iota(jnp.int32, (tiles, tiles), 1), 1.0, 0.0).astype(BF)
    rank = jnp.dot(hit.astype(BF), before, preferred_element_type=F32)
    counts = jnp.sum(hit, axis=1, keepdims=True).astype(jnp.int32)
    groups = lax.shift_right_logical(counts + (GROUP - 1), GROUP.bit_length() - 1).astype(F32)
    lower = jnp.where(lax.broadcasted_iota(jnp.int32, (padded_bases, padded_bases), 1)
                      < lax.broadcasted_iota(jnp.int32, (padded_bases, padded_bases), 0), 1.0, 0.0).astype(BF)
    start = jnp.dot(lower, jnp.broadcast_to(groups, (padded_bases, tiles)).astype(BF),
                    preferred_element_type=F32)
    where = jnp.sum(jnp.where(member, rank + GROUP * start, 0.0), axis=0, keepdims=True).astype(jnp.int32)
    chosen = jnp.where(lax.broadcasted_iota(jnp.int32, (slots, tiles), 0) == where, 1.0, 0.0).astype(BF)
    tile = lax.broadcasted_iota(jnp.int32, (8, tiles), 1)
    kind = lax.broadcasted_iota(jnp.int32, (8, tiles), 0)
    digits = jnp.where(kind == 0, lax.shift_right_logical(tile, 4),
                       jnp.where(kind == 1, jnp.bitwise_and(tile, 15), 1)).astype(F32).astype(BF)
    found = lax.dot_general(digits, chosen, (((1,), (1,)), ((), ())), preferred_element_type=F32)
    named = jnp.where(found[2:3] > 0.5, 16.0 * found[0:1] + found[1:2], float(tiles)).astype(jnp.int32)
    total = jnp.broadcast_to(jnp.sum(groups, axis=0, keepdims=True), (1, 128)).astype(jnp.int32)
    return named, total


def tile_kernel(half_count, order, groups, table, far_owner, far_channel, far_base, far_sky, far_seen, far_keep,
                far_pairs, out, onehot, owner, channel, base, sky, seen, keep, pairs, arrived, *buffers):
    fetched = [pltpu.make_async_copy(src, dst, arrived.at[i]) for i, (src, dst) in enumerate((
        (far_pairs, pairs), (far_base, base), (far_owner, owner), (far_channel, channel),
        (far_sky, sky), (far_seen, seen), (far_keep, keep)))]
    for copy in fetched:
        copy.start()
    tiles, coupled, rows = sky.shape
    directions = coupled // 2
    bases = pairs.shape[0]
    real, imag = term_rows(directions)
    n_terms = directions * directions + 2 * directions
    devices = out.shape[0] - 1
    channels_here = table.shape[0] // (devices // 2)
    chans = devices // 2
    buffers = (buffers[0::2], buffers[1::2])

    def clear(i, carry):
        out[i] = jnp.zeros((n_terms, 2 * HALF), F32)
        return carry
    lax.fori_loop(0, devices + 1, clear, 0)
    fetched[0].wait()
    station = lax.rem(lax.broadcasted_iota(jnp.int32, (2 * HALF, rows), 0), HALF)
    for b in range(bases):
        for side in range(2):
            onehot[b, :, side * rows:(side + 1) * rows] = jnp.where(
                station == pairs[b, side:side + 1, :], 1.0, 0.0).astype(BF)

    for copy in fetched[1:]:
        copy.wait()
    lane = lax.broadcasted_iota(jnp.int32, (1, 2 * HALF), 1)

    def chosen(g):
        first = order[0, jnp.maximum(g, 0) * GROUP]
        return onehot.at[base[jnp.minimum(first, tiles - 1)]]

    def load(g, into):
        sky_s, seen_s, keep_s, gain_s, near_far, _, _ = buffers[into]
        for t in range(GROUP):
            named = order[0, g * GROUP + t]
            tile = jnp.where(named < tiles, named, 0)
            sky_s[pl.ds(t, coupled, stride=GROUP), :] = sky[tile].astype(F32)
            seen_s[pl.ds(t, 2, stride=GROUP), :] = seen[tile].astype(F32)
            keep_s[pl.ds(t, 1), :] = keep[pl.ds(tile, 1), :]
            gain_s[pl.ds(t, coupled, stride=GROUP), :] = table[owner[tile] * channels_here + channel[tile]].astype(F32)
        near_far[...] = jnp.dot(gain_s[...].astype(BF), chosen(g)[...], preferred_element_type=F32)

    def products(of):
        sky_s, seen_s, keep_s, _, near_far, terms, _ = buffers[of]
        kept = keep_s[...] > 0

        def block(ref, i):
            return ref[i * GROUP:(i + 1) * GROUP, :]

        res_r = jnp.where(kept, block(seen_s, 0), 0.0)
        res_i = jnp.where(kept, block(seen_s, 1), 0.0)
        a_r, a_i, b_r, b_i = [], [], [], []
        mod_r = mod_i = None
        for k in range(directions):
            c_r = jnp.where(kept, block(sky_s, 2 * k), 0.0)
            c_i = jnp.where(kept, block(sky_s, 2 * k + 1), 0.0)
            p_r, p_i = (block(near_far, c * directions + k)[:, :rows] for c in range(2))
            q_r, q_i = (block(near_far, c * directions + k)[:, rows:] for c in range(2))
            x_r = c_r * q_r + c_i * q_i
            x_i = c_i * q_r - c_r * q_i
            a_r.append(x_r)
            a_i.append(x_i)
            b_r.append(c_r * p_r - c_i * p_i)
            b_i.append(-(c_r * p_i + c_i * p_r))
            m_r = p_r * x_r - p_i * x_i
            m_i = p_r * x_i + p_i * x_r
            mod_r = m_r if mod_r is None else mod_r + m_r
            mod_i = m_i if mod_i is None else mod_i + m_i
        res_r = res_r - mod_r
        res_i = res_i - mod_i

        for side, (v_r, v_i, w_r, w_i) in enumerate(
                ((a_r, a_i, res_r, res_i), (b_r, b_i, res_r, -res_i))):
            pending = {}

            def put(j, value):
                pending[j] = value
                lo = j - j % 2
                if lo in pending and lo + 1 in pending:
                    both = jnp.concatenate([pending.pop(lo), pending.pop(lo + 1)], axis=0)
                    terms[lo * GROUP:(lo + 2) * GROUP, side * rows:(side + 1) * rows] = both.astype(BF)

            for (k, m), j in real.items():
                put(j, v_r[k] * v_r[m] + v_i[k] * v_i[m])
            for (k, m), j in imag.items():
                put(j, v_r[k] * v_i[m] - v_i[k] * v_r[m])
            first = directions * directions
            for k in range(directions):
                put(first + k, v_r[k] * w_r + v_i[k] * w_i)
            for k in range(directions):
                put(first + directions + k, v_r[k] * w_i - v_i[k] * w_r)

    def station_sums(g, of):
        terms, sums = buffers[of][5:]
        sums[...] = lax.dot_general(terms[...], chosen(g)[...], (((1,), (1,)), ((), ())),
                                    preferred_element_type=F32)

    def add_up(g, of):
        sums = buffers[of][6]
        for t in range(GROUP):
            named = jnp.where(g < 0, tiles, order[0, jnp.maximum(g, 0) * GROUP + t])
            tile = jnp.where(named < tiles, named, 0)
            mine = channel[tile]
            row = jnp.where(named < tiles, (mine // half_count) * chans + owner[tile], devices)
            part = jnp.where(lane // HALF == lax.rem(mine, half_count),
                             sums[pl.ds(t, n_terms, stride=GROUP), :], 0.0)
            out[row] = out[row] + part

    def step(g, of):
        station_sums(g - 2, of)
        add_up(g - 3, 1 - of)
        load(g, of)
        products(1 - of)

    def two(i, carry):
        step(2 * i, 0)
        step(2 * i + 1, 1)
        return carry

    lax.fori_loop(0, (groups[0, 0] + 4) // 2, two, 0)


def tile_sums(sky, seen, keep, order, groups, owner, channel, base, pairs, table, devices, half_count):
    tiles, directions, _, rows = sky.shape
    n_terms = directions * directions + 2 * directions
    bases = pairs.shape[0]
    smem = pl.BlockSpec(memory_space=pltpu.SMEM)
    vmem = pl.BlockSpec(memory_space=pltpu.VMEM)
    hbm = pl.BlockSpec(memory_space=pltpu.HBM)
    coupled = 2 * directions
    return pl.pallas_call(
        functools.partial(tile_kernel, half_count),
        out_shape=jax.ShapeDtypeStruct((devices + 1, n_terms, 2 * HALF), F32),
        in_specs=[smem] * 2 + [vmem] + [hbm] * 7,
        out_specs=vmem,
        scratch_shapes=[
            pltpu.VMEM((bases, 2 * HALF, 2 * rows), BF),
            pltpu.SMEM((tiles,), jnp.int32), pltpu.SMEM((tiles,), jnp.int32), pltpu.SMEM((tiles,), jnp.int32),
            pltpu.VMEM((tiles, coupled, rows), BF), pltpu.VMEM(seen.shape, BF),
            pltpu.VMEM(keep.shape, jnp.int32), pltpu.VMEM(pairs.shape, jnp.int32),
            pltpu.SemaphoreType.DMA((7,)),
        ] + [
            shape for shape in (
                pltpu.VMEM((coupled * GROUP, rows), F32),
                pltpu.VMEM((2 * GROUP, rows), F32),
                pltpu.VMEM((GROUP, rows), jnp.int32),
                pltpu.VMEM((coupled * GROUP, 2 * HALF), F32),
                pltpu.VMEM((coupled * GROUP, 2 * rows), F32),
                pltpu.VMEM((n_terms * GROUP, 2 * rows), BF),
                pltpu.VMEM((n_terms * GROUP, 2 * HALF), F32),
            ) for _ in range(2)
        ],
        compiler_params=pltpu.CompilerParams(vmem_limit_bytes=18 * 1024 * 1024),
        name="tile_sums",
    )(order, groups, table, owner, channel, base, sky.reshape(tiles, coupled, rows), seen, keep, pairs)


def eliminate(total, target, rho, full, directions):
    real, imag = term_rows(directions)
    lanes = total.shape[-1]
    for k in range(directions):
        for m in range(directions):
            re = real[min(k, m), max(k, m)]
            value = total[re:re + 1, :]
            if k == m:
                value = value + rho[k:k + 1, :]
                full[1, k * directions + m:k * directions + m + 1, :] = jnp.zeros((1, lanes), F32)
            else:
                im = imag[min(k, m), max(k, m)]
                imv = total[im:im + 1, :]
                full[1, k * directions + m:k * directions + m + 1, :] = imv if k < m else -imv
            full[0, k * directions + m:k * directions + m + 1, :] = value
    row_r = [full[0, k * directions:(k + 1) * directions, :] for k in range(directions)]
    row_i = [full[1, k * directions:(k + 1) * directions, :] for k in range(directions)]
    t_r = [target[k:k + 1, :] for k in range(directions)]
    t_i = [target[directions + k:directions + k + 1, :] for k in range(directions)]
    for k in range(directions):
        inv = 1.0 / row_r[k][k:k + 1, :]
        row_r[k] = row_r[k] * inv
        row_i[k] = row_i[k] * inv
        t_r[k] = t_r[k] * inv
        t_i[k] = t_i[k] * inv
        for m in range(directions):
            if m == k:
                continue
            f_r = row_r[m][k:k + 1, :]
            f_i = row_i[m][k:k + 1, :]
            row_r[m], row_i[m] = (row_r[m] - (f_r * row_r[k] - f_i * row_i[k]),
                                  row_i[m] - (f_r * row_i[k] + f_i * row_r[k]))
            t_r[m], t_i[m] = (t_r[m] - (f_r * t_r[k] - f_i * t_i[k]),
                              t_i[m] - (f_r * t_i[k] + f_i * t_r[k]))
    return jnp.concatenate(t_r + t_i, axis=0)


XS, ZS = "chan_0", "chan_1"


def place():
    return lax.axis_index(XS), lax.axis_index(ZS), lax.axis_index("sub")


def sender(src, dst, send_sem, recv_sem, x, z, s):
    return pltpu.make_async_remote_copy(
        src_ref=src, dst_ref=dst, send_sem=send_sem, recv_sem=recv_sem,
        device_id={XS: x, ZS: z, "sub": s}, device_id_type=pl.DeviceIdType.MESH)


def meet(x, z, s, nx, nz, crossed):
    barrier = pltpu.get_barrier_semaphore()

    def ring(d, carry):
        pl.semaphore_signal(barrier, inc=1, device_id={XS: x, ZS: lax.rem(z + d, nz), "sub": s},
                            device_id_type=pl.DeviceIdType.MESH)
        return carry
    lax.fori_loop(1, nz, ring, 0)
    near = [(e, f) for e in range(nx) for f in range(2) if e + f > 0 and (crossed or e * f == 0)]
    for e, f in near:
        pl.semaphore_signal(barrier, inc=1,
                            device_id={XS: lax.rem(x + e, nx), ZS: z, "sub": s + f - 2 * s * f},
                            device_id_type=pl.DeviceIdType.MESH)
    return barrier, nz - 1 + len(near)


def outward(i, nz):
    return jnp.where(lax.rem(i, 2) == 0, i // 2 + 1, nz - 1 - i // 2)


def gather_kernel(nx, nz, bases, far_gains, far_base, table, order, groups, gains, base, wide, mine, arrived,
                  z_recv, z_send, x_recv, x_send, c_recv, c_send):
    x, z, s = place()
    here, half = mine.shape[0], mine.shape[0] // 2
    stations = gains.shape[2]
    fetched = [pltpu.make_async_copy(far_gains, gains, arrived.at[0]),
               pltpu.make_async_copy(far_base, base, arrived.at[1])]
    for copy in fetched:
        copy.start()
    barrier, count = meet(x, z, s, nx, nz, False)
    wide[...] = jnp.zeros(wide.shape, F32)
    for copy in fetched:
        copy.wait()
    head = gains[...].astype(BF).astype(F32)
    wide[:, :, :stations] = head
    wide[:, :, HALF:HALF + stations] = gains[...] - head
    mine[...] = wide[...].astype(BF)
    table[pl.ds((x * nz + z) * here + s * half, half)] = mine[pl.ds(s * half, half)]
    pl.semaphore_wait(barrier, count)

    def block(xx, zz):
        return table.at[pl.ds((xx * nz + zz) * here + s * half, half)]

    def rows(xx, h):
        return table.at[pl.ds(xx * nz * here, nz * here)].reshape(nz, here, *mine.shape[1:]).at[:, pl.ds(h * half, half)]

    own = mine.at[pl.ds(s * half, half)]

    def z_copy(d):
        return sender(own, block(x, z), z_send.at[d], z_recv.at[d], x, lax.rem(z + d, nz), s)

    def start_z(i, carry):
        z_copy(outward(i, nz)).start()
        return carry
    lax.fori_loop(0, nz - 1, start_z, 0)

    def x_copy(src, xx, zz, d, e, to):
        return sender(src, block(xx, zz), x_send.at[e, d], x_recv.at[e, d], to, z, s)

    def took_x(e, d):
        xx, zz = lax.rem(x + nx - e, nx), lax.rem(z + nz - d, nz)
        sender(own, block(xx, zz), x_send.at[e, d], x_recv.at[e, d], x, z, s).wait_recv()
        return xx, zz
    right, left = lax.rem(x + 1, nx), lax.rem(x + nx - 1, nx)
    across = nx // 2
    by_turns = [0] + [i // 2 + 1 if i % 2 == 0 else nz - 1 - i // 2 for i in range(nz - 1)]
    lag = 3
    for p in range(nz + lag):
        if p < nz:
            d = by_turns[p]
            zz = lax.rem(z + nz - d, nz)
            if d > 0:
                sender(own, block(x, zz), z_send.at[d], z_recv.at[d], x, z, s).wait_recv()
            src = own if d == 0 else block(x, zz)
            x_copy(src, x, zz, d, 1, right).start()
            x_copy(src, x, zz, d, nx - 1, left).start()
            if d == 0:
                order[...], groups[...] = tile_order(base[...], bases, order.shape[1])
        if p >= lag:
            d = by_turns[p - lag]
            e, to = ((1, right), (nx - 1, left))[(p - lag) % 2]
            xx, zz = took_x(e, d)
            x_copy(block(xx, zz), xx, zz, d, across, to).start()
            took_x(nx - e, d)

    def c_copy(e, h):
        xx = lax.rem(x + nx - e, nx)
        return sender(rows(xx, h), rows(xx, h), c_send.at[e], c_recv.at[e], x, z, 1 - s)
    for e in (0, 1, nx - 1):
        c_copy(e, s).start()
    for d in by_turns:
        took_x(across, d)
    c_copy(across, s).start()
    for e in range(nx):
        c_copy(e, 1 - s).wait_recv()

    def done_z(d, carry):
        z_copy(d).wait_send()
        return carry
    lax.fori_loop(1, nz, done_z, 0)

    def done_x(d, carry):
        for e in range(1, nx):
            x_copy(own, x, z, d, e, x).wait_send()
        return carry
    lax.fori_loop(0, nz, done_x, 0)
    for e in range(nx):
        c_copy(e, s).wait_send()


def gather_gains(gains, base, bases, nx, nz):
    vmem = pl.BlockSpec(memory_space=pltpu.VMEM)
    dma = pltpu.SemaphoreType.DMA
    here, rows, _ = gains.shape
    slots = -(-(base.shape[1] + GROUP * (bases + 6)) // 128) * 128
    return pl.pallas_call(
        functools.partial(gather_kernel, nx, nz, bases),
        out_shape=(jax.ShapeDtypeStruct((nx * nz * here, rows, 2 * HALF), BF),
                   jax.ShapeDtypeStruct((1, slots), jnp.int32), jax.ShapeDtypeStruct((1, 128), jnp.int32)),
        in_specs=[pl.BlockSpec(memory_space=pltpu.HBM)] * 2,
        out_specs=(vmem, vmem, vmem),
        scratch_shapes=[pltpu.VMEM(gains.shape, F32), pltpu.VMEM(base.shape, jnp.int32),
                        pltpu.VMEM((here, rows, 2 * HALF), F32), pltpu.VMEM((here, rows, 2 * HALF), BF), dma((2,)),
                        dma((nz,)), dma((nz,)), dma((nx, nz)), dma((nx, nz)), dma((nx,)), dma((nx,))],
        compiler_params=pltpu.CompilerParams(collective_id=0, has_side_effects=True,
                                             vmem_limit_bytes=8 * 1024 * 1024),
        name="gather_gains",
    )(gains, base)


def packed(v, plain):
    head = v[plain:].astype(BF)
    tail = v[plain:] - head.astype(F32)
    return jnp.concatenate([v[:plain].astype(BF), head, tail.astype(BF)], axis=0)


def unpacked(w, plain):
    v = w.astype(F32)
    mid = (v.shape[0] + plain) // 2
    return jnp.concatenate([v[:plain], v[plain:mid] + v[mid:]], axis=0)


def finish_kernel(nx, nz, inverse, sums, gains, duals, cons, rho, gain_new, cons_new, dual_new,
                  peer, two_out, two_in, x_out, x_in, z_out, z_in, z_sum, total, full, wide,
                  part_out, part_in, ring_in, last_in,
                  c_send, c_recv, t_send, t_recv, x_send, x_recv, z_send, z_recv,
                  p_send, p_recv, r_send, r_recv, l_send, l_recv):
    x, z, s = place()
    directions = rho.shape[0]
    degrees, _, stations = cons.shape
    half_count = duals.shape[0]
    plain = directions * directions
    chunk = 4
    nodes = nx * nz
    barrier, count = meet(x, z, s, nx, nz, True)

    wide[...] = jnp.zeros(wide.shape, F32)
    for h in range(half_count):
        wide[0, :, h * HALF:h * HALF + stations] = gains[s * half_count + h]
        wide[1, :, h * HALF:h * HALF + stations] = duals[h]
        for d in range(degrees):
            wide[2 + d, :, h * HALF:h * HALF + stations] = cons[d]
    basis = legendre(((x * nz + z) * 2 + s) * half_count, 2 * nodes * half_count)
    pl.semaphore_wait(barrier, count)

    def far(i):
        if isinstance(i, int):
            return (nz // 2 + (i + 1) // 2 * (1 if i % 2 == 0 else -1)) % nz
        step = (i + 1) // 2
        return lax.rem(jnp.where(lax.rem(i, 2) == 0, nz // 2 + step, nz // 2 + nz - step), nz)

    def c_copy(e, h):
        xx = lax.rem(x + e, nx)
        return sender(sums.at[pl.ds(h * nodes + xx * nz, nz)], peer.at[pl.ds(xx * nz, nz)],
                      c_send.at[e], c_recv.at[e], x, z, 1 - s)
    across, right, left_ = nx // 2, 1, nx - 1
    order = (across, right, left_, 0)
    for e in order:
        c_copy(e, 1 - s).start()

    def pair_sum(xx, zz):
        return sums[s * nodes + xx * nz + zz] + peer[xx * nz + zz]

    chunks = nz // chunk
    share = chunk // 2
    def t_copy(side, c):
        at = pl.ds(c * chunk + side * share, share)
        return sender(two_out.at[at], two_in.at[at], t_send.at[side, c], t_recv.at[side, c],
                      lax.rem(x + (right, left_)[side], nx), z, s)

    def fill_two(c):
        def one(j, inner):
            i = c * chunk + j
            two_out[i] = packed(pair_sum(lax.rem(x + across, nx), lax.rem(z + far(i), nz)), plain)
            return inner
        lax.fori_loop(0, chunk, one, 0)
        for side in range(2):
            t_copy(side, c).start()

    def x_copy(side, c):
        at = pl.ds(c * chunk, chunk)
        return sender(x_out.at[side, at], x_in.at[side, at], x_send.at[side, c], x_recv.at[side, c],
                      lax.rem(x + (right, left_)[side], nx), z, s)

    def fill_x(c):
        for side in range(2):
            t_copy(side, c).wait_recv()
            xx = lax.rem(x + (right, left_)[side], nx)

            def relayed(j, inner):
                i = c * chunk + side * share + j
                x_out[side, i] = packed(pair_sum(xx, lax.rem(z + far(i), nz)) + unpacked(two_in[i], plain), plain)
                return inner

            def plainly(j, inner):
                i = c * chunk + (1 - side) * share + j
                x_out[side, i] = packed(pair_sum(xx, lax.rem(z + far(i), nz)), plain)
                return inner
            lax.fori_loop(0, share, relayed, 0)
            lax.fori_loop(0, share, plainly, 0)
            x_copy(side, c).start()

    quarter = nz // 4
    n_far = 2 * quarter - 1
    odd = lax.rem(z, 2)

    def hop(i):
        d = far(i)
        if i >= n_far:
            return d
        if i == 0:
            return quarter + 2 * quarter * odd
        return d - quarter if i % 2 == 1 else d + quarter

    def z_copy(i):
        return sender(z_out.at[i], z_in.at[i], z_send.at[i], z_recv.at[i], x, lax.rem(z + hop(i), nz), s)

    def fill_z(c):
        for side in range(2):
            x_copy(side, c).wait_recv()

        def one(j, inner):
            i = c * chunk + j
            acc = pair_sum(x, lax.rem(z + far(i), nz))
            for side in range(2):
                acc = acc + unpacked(x_in[side, i], plain)
            z_out[i] = packed(acc, plain)
            z_sum[i] = acc
            return inner
        lax.fori_loop(0, chunk, one, 0)
        for i in range(c * chunk, (c + 1) * chunk):
            if i not in (n_far, n_far + 1, nz - 1):
                z_copy(i).start()

    def relay_z():
        for i in range(n_far):
            z_copy(i).wait_recv()
            to = n_far + odd if i == 0 else n_far + (i + 1) % 2
            z_sum[to] = z_sum[to] + unpacked(z_in[i], plain)
        for i in (n_far, n_far + 1):
            z_out[i] = packed(z_sum[i], plain)
        for i in (n_far, n_far + 1):
            z_copy(i).start()

    c_copy(across, s).wait_recv()
    for c in range(chunks - 1):
        fill_two(c)
    c_copy(right, s).wait_recv()
    c_copy(left_, s).wait_recv()
    fill_x(0)
    fill_two(chunks - 1)
    fill_x(1)
    c_copy(0, s).wait_recv()
    for c in range(chunks):
        if c == chunks - 1:
            relay_z()
        fill_z(c)
        if c + 2 < chunks:
            fill_x(c + 2)
    acc = z_sum[nz - 1]
    for i in list(range(n_far + 2, nz - 1)) + [n_far, n_far + 1]:
        z_copy(i).wait_recv()
        acc = acc + unpacked(z_in[i], plain)
    total[...] = acc

    rho2 = jnp.concatenate([rho[...], rho[...]], axis=0)
    gain, dual = wide[0], wide[1]
    anchor = sum(basis[d] * wide[2 + d] for d in range(degrees))
    target = total[plain:, :] - dual - rho2 * (gain - anchor)
    new = gain + eliminate(total, target, rho[...], full, directions)
    for h in range(half_count):
        gain_new[h] = new[:, h * HALF:h * HALF + stations]
    weighted = new + dual / rho2
    left = lax.broadcasted_iota(jnp.int32, (2 * directions, 2 * HALF), 1) < HALF

    def folded(d):
        part = basis[d] * weighted
        return part + pltpu.roll(part, HALF, axis=1)
    pair = degrees // 2
    both = jnp.concatenate([jnp.where(left, folded(d), folded(d + pair)) for d in range(pair)], axis=0)
    pieces, piece = part_out.shape[0], part_out.shape[1]
    for m in range(pieces):
        part_out[m] = both[m * piece:(m + 1) * piece, :]

    near = [(e, f) for e in range(nx) for f in range(2) if e + f > 0]

    def other(e, f):
        return lax.rem(x + e, nx), s + f - 2 * s * f

    def p_copy(e, f):
        xx, ss = other(e, f)
        return sender(part_out.at[xx * 2 + ss], part_in.at[e * 2 + f], p_send.at[e * 2 + f],
                      p_recv.at[e * 2 + f], xx, z, ss)
    for e, f in near:
        p_copy(e, f).start()
    acc = part_out[x * 2 + s]
    for e, f in near:
        p_copy(e, f).wait_recv()
        acc = acc + part_in[e * 2 + f]
    ring_in[z] = acc

    def r_copy(d):
        zz = lax.rem(z + d, nz)
        return sender(ring_in.at[z], ring_in.at[z], r_send.at[d], r_recv.at[d], x, zz, s)

    def start_r(i, carry):
        r_copy(far(i)).start()
        return carry
    lax.fori_loop(0, nz - 1, start_r, 0)

    def take_r(i, carry):
        d = far(i)
        zz = lax.rem(z + nz - d, nz)
        sender(ring_in.at[zz], ring_in.at[zz], r_send.at[d], r_recv.at[d], x, z, s).wait_recv()
        return carry
    lax.fori_loop(0, nz - 1, take_r, 0)
    acc = ring_in[0]
    for i in range(1, nz):
        acc = acc + ring_in[i]
    me = x * 2 + s
    last_in[me] = acc

    def l_copy(e, f, m):
        xx, ss = other(e, f)
        return sender(last_in.at[m], last_in.at[m], l_send.at[e * 2 + f], l_recv.at[e * 2 + f], xx, z, ss)
    for e, f in near:
        l_copy(e, f, me).start()
    for e, f in near:
        back = lax.rem(x + nx - e, nx) * 2 + (s + f - 2 * s * f)
        l_copy(e, f, back).wait_recv()
    both = jnp.concatenate([last_in[m] for m in range(pieces)], axis=0)
    wide = 2 * directions
    summed = [None] * degrees
    for d in range(pair):
        rows = both[d * wide:(d + 1) * wide, :]
        turned = pltpu.roll(rows, HALF, axis=1)
        summed[d] = jnp.where(left, rows, turned)
        summed[d + pair] = jnp.where(left, turned, rows)
    fit = None
    for d in range(degrees):
        coeff = sum(inverse[d][q] * summed[q] for q in range(degrees))
        cons_new[d] = coeff[:, :stations]
        term = basis[d] * coeff
        fit = term if fit is None else fit + term
    dual_out = dual + rho2 * (new - fit)
    for h in range(half_count):
        dual_new[h] = dual_out[:, h * HALF:h * HALF + stations]

    for e in range(nx):
        c_copy(e, 1 - s).wait_send()

    for c in range(chunks):
        for side in range(2):
            t_copy(side, c).wait_send()
            x_copy(side, c).wait_send()
    for i in range(nz - 1):
        z_copy(i).wait_send()
        r_copy(i + 1).wait_send()
    for e, f in near:
        p_copy(e, f).wait_send()
        l_copy(e, f, me).wait_send()


def finish(sums, gains, duals, cons, rho, inverse, nx, nz):
    vmem = pl.BlockSpec(memory_space=pltpu.VMEM)
    dma = pltpu.SemaphoreType.DMA
    degrees, rows, _ = cons.shape
    terms, lanes = sums.shape[1:]
    wire = terms + rows
    pieces = 2 * nx
    piece = degrees * rows // 2 // pieces
    chunks = nz // 4
    return pl.pallas_call(
        functools.partial(finish_kernel, nx, nz, inverse),
        out_shape=(jax.ShapeDtypeStruct(duals.shape, F32), jax.ShapeDtypeStruct(cons.shape, F32),
                   jax.ShapeDtypeStruct(duals.shape, F32)),
        in_specs=[vmem] * 5,
        out_specs=(vmem, vmem, vmem),
        scratch_shapes=[
            pltpu.VMEM((nx * nz, terms, lanes), F32),
            pltpu.VMEM((nz, wire, lanes), BF),
            pltpu.VMEM((nz, wire, lanes), BF),
            pltpu.VMEM((2, nz, wire, lanes), BF),
            pltpu.VMEM((2, nz, wire, lanes), BF),
            pltpu.VMEM((nz, wire, lanes), BF),
            pltpu.VMEM((nz, wire, lanes), BF),
            pltpu.VMEM((nz, terms, lanes), F32),
            pltpu.VMEM((terms, lanes), F32),
            pltpu.VMEM((2, rows * rows // 4, lanes), F32),
            pltpu.VMEM((2 + degrees, rows, lanes), F32),
            pltpu.VMEM((pieces, piece, lanes), F32),
            pltpu.VMEM((pieces, piece, lanes), F32),
            pltpu.VMEM((nz, piece, lanes), F32),
            pltpu.VMEM((pieces, piece, lanes), F32),
            dma((nx,)), dma((nx,)), dma((2, chunks)), dma((2, chunks)), dma((2, chunks)), dma((2, chunks)),
            dma((nz,)), dma((nz,)),
            dma((pieces,)), dma((pieces,)), dma((nz,)), dma((nz,)), dma((pieces,)), dma((pieces,)),
        ],
        compiler_params=pltpu.CompilerParams(collective_id=1, has_side_effects=True,
                                             vmem_limit_bytes=18 * 1024 * 1024),
        name="finish",
    )(sums, gains, duals, cons, rho)


def to_rows(x):
    n, c, s, k = x.shape
    return jnp.transpose(x, (0, 1, 3, 2)).reshape(n, c * k, s)


def from_rows(x):
    n, rows, s = x.shape
    return jnp.transpose(x.reshape(n, 2, rows // 2, s), (0, 1, 3, 2))


def body(sky, seen, keep, tile_owner, tile_channel, tile_base, pairs, gains, duals, consensus, rho):
    channels_here, _, _, directions = gains.shape
    nx, nz = lax.axis_size(XS), lax.axis_size(ZS)
    sub_count = lax.axis_size("sub")
    half_count = channels_here // sub_count
    gain_rows = to_rows(gains)
    table, order, groups = gather_gains(gain_rows, tile_base.reshape(1, -1), pairs.shape[0], nx, nz)
    sums = tile_sums(sky, seen, keep, order, groups, tile_owner[:, 0], tile_channel, tile_base, pairs, table,
                     nx * nz * sub_count, half_count)
    rho_rows = jnp.broadcast_to(rho[:, None], (directions, 2 * HALF))
    gain_new, cons_new, dual_new = finish(sums, gain_rows, to_rows(duals), to_rows(consensus), rho_rows,
                                          gram_inverse(channels_here * nx * nz).tolist(), nx, nz)
    return from_rows(gain_new), from_rows(cons_new), from_rows(dual_new)


def solution(mesh):
    groups, subs = mesh.shape["groups"], mesh.shape["sub"]
    torus = Mesh(mesh.devices.reshape(groups, 4, mesh.shape["chan"] // 4, subs), GROUPS_CHAN_SUB)
    return jax.shard_map(
        body,
        mesh=torus,
        in_specs=(
            P(GROUPS_CHAN_SUB, None, None, None),
            P(GROUPS_CHAN_SUB, None, None),
            P(GROUPS_CHAN_SUB, None),
            P(GROUPS_CHAN_SUB, None),
            P(GROUPS_CHAN_SUB),
            P(GROUPS_CHAN_SUB),
            P(),
            P(GROUPS_CHAN, None, None, None),
            P(GROUPS_CHAN_SUB, None, None, None),
            P("groups", None, None, None),
            P(),
        ),
        out_specs=(
            P(GROUPS_CHAN_SUB, None, None, None),
            P("groups", None, None, None),
            P(GROUPS_CHAN_SUB, None, None, None),
        ),
        check_vma=False,
    )
```

```python
import functools

import jax
import jax.numpy as jnp
import numpy as np
from jax import lax
from jax.experimental import pallas as pl
from jax.experimental.pallas import tpu as pltpu
from jax.sharding import Mesh
from jax.sharding import PartitionSpec as P

GROUPS_CHAN_SUB = ("groups", "chan_0", "chan_1", "sub")
GROUPS_CHAN = ("groups", "chan_0", "chan_1")
BF, F32 = jnp.bfloat16, jnp.float32
GROUP = 8
HALF = 64


def term_rows(directions):
    real, imag = {}, {}
    for k in range(directions):
        for m in range(k, directions):
            real[k, m] = len(real)
    for k in range(directions):
        for m in range(k + 1, directions):
            imag[k, m] = len(real) + len(imag)
    return real, imag


def legendre(first, channels):
    lane = lax.broadcasted_iota(jnp.int32, (1, 2 * HALF), 1)
    place = (first + lane // HALF).astype(F32)
    x = (2.0 * place - (channels - 1)) / max(channels - 1, 1)
    return [jnp.ones_like(x), x, 0.5 * (3.0 * x * x - 1.0), 0.5 * (5.0 * x * x * x - 3.0 * x)]


def gram_inverse(channels):
    x = (2.0 * np.arange(channels, dtype=np.float64) - (channels - 1)) / max(channels - 1, 1)
    basis = np.stack([np.ones_like(x), x, 0.5 * (3 * x * x - 1), 0.5 * (5 * x * x * x - 3 * x)])
    return np.linalg.inv(basis @ basis.T)


def tile_order(base, bases, slots):
    tiles = base.shape[1]
    padded_bases = -(-bases // 16) * 16
    member = lax.broadcasted_iota(jnp.int32, (padded_bases, tiles), 0) == base
    hit = jnp.where(member, 1.0, 0.0)
    before = jnp.where(lax.broadcasted_iota(jnp.int32, (tiles, tiles), 0)
                       < lax.broadcasted_iota(jnp.int32, (tiles, tiles), 1), 1.0, 0.0).astype(BF)
    rank = jnp.dot(hit.astype(BF), before, preferred_element_type=F32)
    counts = jnp.sum(hit, axis=1, keepdims=True).astype(jnp.int32)
    groups = lax.shift_right_logical(counts + (GROUP - 1), GROUP.bit_length() - 1).astype(F32)
    lower = jnp.where(lax.broadcasted_iota(jnp.int32, (padded_bases, padded_bases), 1)
                      < lax.broadcasted_iota(jnp.int32, (padded_bases, padded_bases), 0), 1.0, 0.0).astype(BF)
    start = jnp.dot(lower, jnp.broadcast_to(groups, (padded_bases, tiles)).astype(BF),
                    preferred_element_type=F32)
    where = jnp.sum(jnp.where(member, rank + GROUP * start, 0.0), axis=0, keepdims=True).astype(jnp.int32)
    chosen = jnp.where(lax.broadcasted_iota(jnp.int32, (slots, tiles), 0) == where, 1.0, 0.0).astype(BF)
    tile = lax.broadcasted_iota(jnp.int32, (8, tiles), 1)
    kind = lax.broadcasted_iota(jnp.int32, (8, tiles), 0)
    digits = jnp.where(kind == 0, lax.shift_right_logical(tile, 4),
                       jnp.where(kind == 1, jnp.bitwise_and(tile, 15), 1)).astype(F32).astype(BF)
    found = lax.dot_general(digits, chosen, (((1,), (1,)), ((), ())), preferred_element_type=F32)
    named = jnp.where(found[2:3] > 0.5, 16.0 * found[0:1] + found[1:2], float(tiles)).astype(jnp.int32)
    total = jnp.broadcast_to(jnp.sum(groups, axis=0, keepdims=True), (1, 128)).astype(jnp.int32)
    return named, total


def tile_kernel(half_count, order, groups, owner, channel, base, sky, seen, keep, pairs, table, out, onehot, *buffers):
    tiles, coupled, rows = sky.shape
    directions = coupled // 2
    bases = pairs.shape[0]
    real, imag = term_rows(directions)
    n_terms = directions * directions + 2 * directions
    devices = out.shape[0] - 1
    channels_here = table.shape[0] // (devices // 2)
    chans = devices // 2
    buffers = (buffers[0::2], buffers[1::2])

    station = lax.rem(lax.broadcasted_iota(jnp.int32, (2 * HALF, rows), 0), HALF)
    for b in range(bases):
        for side in range(2):
            onehot[b, :, side * rows:(side + 1) * rows] = jnp.where(
                station == pairs[b, side:side + 1, :], 1.0, 0.0).astype(BF)

    def clear(i, carry):
        out[i] = jnp.zeros((n_terms, 2 * HALF), F32)
        return carry
    lax.fori_loop(0, devices + 1, clear, 0)
    lane = lax.broadcasted_iota(jnp.int32, (1, 2 * HALF), 1)

    def chosen(g):
        first = order[0, jnp.maximum(g, 0) * GROUP]
        return onehot.at[base[jnp.minimum(first, tiles - 1)]]

    def load(g, into):
        sky_s, seen_s, keep_s, gain_s, near_far, _, _ = buffers[into]
        for t in range(GROUP):
            named = order[0, g * GROUP + t]
            tile = jnp.where(named < tiles, named, 0)
            sky_s[pl.ds(t, coupled, stride=GROUP), :] = sky[tile].astype(F32)
            seen_s[pl.ds(t, 2, stride=GROUP), :] = seen[tile].astype(F32)
            keep_s[pl.ds(t, 1), :] = keep[pl.ds(tile, 1), :]
            gain_s[pl.ds(t, coupled, stride=GROUP), :] = table[owner[tile] * channels_here + channel[tile]].astype(F32)
        near_far[...] = jnp.dot(gain_s[...].astype(BF), chosen(g)[...], preferred_element_type=F32)

    def products(of):
        sky_s, seen_s, keep_s, _, near_far, terms, _ = buffers[of]
        kept = keep_s[...] > 0

        def block(ref, i):
            return ref[i * GROUP:(i + 1) * GROUP, :]

        res_r = jnp.where(kept, block(seen_s, 0), 0.0)
        res_i = jnp.where(kept, block(seen_s, 1), 0.0)
        a_r, a_i, b_r, b_i = [], [], [], []
        mod_r = mod_i = None
        for k in range(directions):
            c_r = jnp.where(kept, block(sky_s, 2 * k), 0.0)
            c_i = jnp.where(kept, block(sky_s, 2 * k + 1), 0.0)
            p_r, p_i = (block(near_far, c * directions + k)[:, :rows] for c in range(2))
            q_r, q_i = (block(near_far, c * directions + k)[:, rows:] for c in range(2))
            x_r = c_r * q_r + c_i * q_i
            x_i = c_i * q_r - c_r * q_i
            a_r.append(x_r)
            a_i.append(x_i)
            b_r.append(c_r * p_r - c_i * p_i)
            b_i.append(-(c_r * p_i + c_i * p_r))
            m_r = p_r * x_r - p_i * x_i
            m_i = p_r * x_i + p_i * x_r
            mod_r = m_r if mod_r is None else mod_r + m_r
            mod_i = m_i if mod_i is None else mod_i + m_i
        res_r = res_r - mod_r
        res_i = res_i - mod_i

        for side, (v_r, v_i, w_r, w_i) in enumerate(
                ((a_r, a_i, res_r, res_i), (b_r, b_i, res_r, -res_i))):
            pending = {}

            def put(j, value):
                pending[j] = value
                lo = j - j % 2
                if lo in pending and lo + 1 in pending:
                    both = jnp.concatenate([pending.pop(lo), pending.pop(lo + 1)], axis=0)
                    terms[lo * GROUP:(lo + 2) * GROUP, side * rows:(side + 1) * rows] = both.astype(BF)

            for (k, m), j in real.items():
                put(j, v_r[k] * v_r[m] + v_i[k] * v_i[m])
            for (k, m), j in imag.items():
                put(j, v_r[k] * v_i[m] - v_i[k] * v_r[m])
            first = directions * directions
            for k in range(directions):
                put(first + k, v_r[k] * w_r + v_i[k] * w_i)
            for k in range(directions):
                put(first + directions + k, v_r[k] * w_i - v_i[k] * w_r)

    def station_sums(g, of):
        terms, sums = buffers[of][5:]
        sums[...] = lax.dot_general(terms[...], chosen(g)[...], (((1,), (1,)), ((), ())),
                                    preferred_element_type=F32)

    def add_up(g, of):
        sums = buffers[of][6]
        for t in range(GROUP):
            named = jnp.where(g < 0, tiles, order[0, jnp.maximum(g, 0) * GROUP + t])
            tile = jnp.where(named < tiles, named, 0)
            mine = channel[tile]
            row = jnp.where(named < tiles, (mine // half_count) * chans + owner[tile], devices)
            part = jnp.where(lane // HALF == lax.rem(mine, half_count),
                             sums[pl.ds(t, n_terms, stride=GROUP), :], 0.0)
            out[row] = out[row] + part

    def step(g, of):
        station_sums(g - 2, of)
        add_up(g - 3, 1 - of)
        load(g, of)
        products(1 - of)

    def two(i, carry):
        step(2 * i, 0)
        step(2 * i + 1, 1)
        return carry

    lax.fori_loop(0, (groups[0, 0] + 4) // 2, two, 0)


def tile_sums(sky, seen, keep, order, groups, owner, channel, base, pairs, table, devices, half_count):
    tiles, directions, _, rows = sky.shape
    n_terms = directions * directions + 2 * directions
    bases = pairs.shape[0]
    smem = pl.BlockSpec(memory_space=pltpu.SMEM)
    vmem = pl.BlockSpec(memory_space=pltpu.VMEM)
    coupled = 2 * directions
    return pl.pallas_call(
        functools.partial(tile_kernel, half_count),
        out_shape=jax.ShapeDtypeStruct((devices + 1, n_terms, 2 * HALF), F32),
        in_specs=[smem] * 5 + [vmem] * 5,
        out_specs=vmem,
        scratch_shapes=[pltpu.VMEM((bases, 2 * HALF, 2 * rows), BF)] + [
            shape for shape in (
                pltpu.VMEM((coupled * GROUP, rows), F32),
                pltpu.VMEM((2 * GROUP, rows), F32),
                pltpu.VMEM((GROUP, rows), jnp.int32),
                pltpu.VMEM((coupled * GROUP, 2 * HALF), F32),
                pltpu.VMEM((coupled * GROUP, 2 * rows), F32),
                pltpu.VMEM((n_terms * GROUP, 2 * rows), BF),
                pltpu.VMEM((n_terms * GROUP, 2 * HALF), F32),
            ) for _ in range(2)
        ],
        compiler_params=pltpu.CompilerParams(vmem_limit_bytes=18 * 1024 * 1024),
        name="tile_sums",
    )(order, groups, owner, channel, base, sky.reshape(tiles, coupled, rows), seen, keep, pairs, table)


def eliminate(total, target, rho, full, directions):
    real, imag = term_rows(directions)
    lanes = total.shape[-1]
    for k in range(directions):
        for m in range(directions):
            re = real[min(k, m), max(k, m)]
            value = total[re:re + 1, :]
            if k == m:
                value = value + rho[k:k + 1, :]
                full[1, k * directions + m:k * directions + m + 1, :] = jnp.zeros((1, lanes), F32)
            else:
                im = imag[min(k, m), max(k, m)]
                imv = total[im:im + 1, :]
                full[1, k * directions + m:k * directions + m + 1, :] = imv if k < m else -imv
            full[0, k * directions + m:k * directions + m + 1, :] = value
    row_r = [full[0, k * directions:(k + 1) * directions, :] for k in range(directions)]
    row_i = [full[1, k * directions:(k + 1) * directions, :] for k in range(directions)]
    t_r = [target[k:k + 1, :] for k in range(directions)]
    t_i = [target[directions + k:directions + k + 1, :] for k in range(directions)]
    for k in range(directions):
        inv = 1.0 / row_r[k][k:k + 1, :]
        row_r[k] = row_r[k] * inv
        row_i[k] = row_i[k] * inv
        t_r[k] = t_r[k] * inv
        t_i[k] = t_i[k] * inv
        for m in range(directions):
            if m == k:
                continue
            f_r = row_r[m][k:k + 1, :]
            f_i = row_i[m][k:k + 1, :]
            row_r[m], row_i[m] = (row_r[m] - (f_r * row_r[k] - f_i * row_i[k]),
                                  row_i[m] - (f_r * row_i[k] + f_i * row_r[k]))
            t_r[m], t_i[m] = (t_r[m] - (f_r * t_r[k] - f_i * t_i[k]),
                              t_i[m] - (f_r * t_i[k] + f_i * t_r[k]))
    return jnp.concatenate(t_r + t_i, axis=0)


XS, ZS = "chan_0", "chan_1"


def place():
    return lax.axis_index(XS), lax.axis_index(ZS), lax.axis_index("sub")


def sender(src, dst, send_sem, recv_sem, x, z, s):
    return pltpu.make_async_remote_copy(
        src_ref=src, dst_ref=dst, send_sem=send_sem, recv_sem=recv_sem,
        device_id={XS: x, ZS: z, "sub": s}, device_id_type=pl.DeviceIdType.MESH)


def meet(x, z, s, nx, nz, reach, crossed):
    barrier = pltpu.get_barrier_semaphore()

    def ring(d, carry):
        pl.semaphore_signal(barrier, inc=1, device_id={XS: x, ZS: lax.rem(z + d, nz), "sub": s},
                            device_id_type=pl.DeviceIdType.MESH)
        return carry
    lax.fori_loop(1, reach + 1, ring, 0)
    lax.fori_loop(max(reach + 1, nz - reach), nz, ring, 0)
    near = [(e, f) for e in range(nx) for f in range(2) if e + f > 0 and (crossed or e * f == 0)]
    for e, f in near:
        pl.semaphore_signal(barrier, inc=1,
                            device_id={XS: lax.rem(x + e, nx), ZS: z, "sub": s + f - 2 * s * f},
                            device_id_type=pl.DeviceIdType.MESH)
    return barrier, min(nz - 1, 2 * reach) + len(near)


def outward(i, nz):
    return jnp.where(lax.rem(i, 2) == 0, i // 2 + 1, nz - 1 - i // 2)


def gather_kernel(nx, nz, bases, gains, base, table, order, groups, wide, mine,
                  z_recv, z_send, x_recv, x_send, c_recv, c_send):
    x, z, s = place()
    here, half = mine.shape[0], mine.shape[0] // 2
    stations = gains.shape[2]
    barrier, count = meet(x, z, s, nx, nz, nz - 1, False)
    wide[...] = jnp.zeros(wide.shape, F32)
    head = gains[...].astype(BF).astype(F32)
    wide[:, :, :stations] = head
    wide[:, :, HALF:HALF + stations] = gains[...] - head
    mine[...] = wide[...].astype(BF)
    table[pl.ds((x * nz + z) * here + s * half, half)] = mine[pl.ds(s * half, half)]
    pl.semaphore_wait(barrier, count)

    def block(xx, zz):
        return table.at[pl.ds((xx * nz + zz) * here + s * half, half)]

    def rows(xx, h):
        return table.at[pl.ds(xx * nz * here, nz * here)].reshape(nz, here, *mine.shape[1:]).at[:, pl.ds(h * half, half)]

    own = mine.at[pl.ds(s * half, half)]

    def z_copy(d):
        return sender(own, block(x, z), z_send.at[d], z_recv.at[d], x, lax.rem(z + d, nz), s)

    def start_z(i, carry):
        z_copy(outward(i, nz)).start()
        return carry
    lax.fori_loop(0, nz - 1, start_z, 0)

    def x_copy(src, zz, d, e):
        return sender(src, block(x, zz), x_send.at[e, d], x_recv.at[e, d], lax.rem(x + e, nx), z, s)
    for e in range(1, nx):
        x_copy(own, z, 0, e).start()
    order[...], groups[...] = tile_order(base[...], bases, order.shape[1])

    def pass_on(i, carry):
        d = outward(i, nz)
        zz = lax.rem(z + nz - d, nz)
        sender(own, block(x, zz), z_send.at[d], z_recv.at[d], x, z, s).wait_recv()
        for e in range(1, nx):
            x_copy(block(x, zz), zz, d, e).start()
        return carry
    lax.fori_loop(0, nz - 1, pass_on, 0)

    def c_copy(e, h):
        xx = lax.rem(x + nx - e, nx)
        return sender(rows(xx, h), rows(xx, h), c_send.at[e], c_recv.at[e], x, z, 1 - s)
    for e in (0, 1, 3, 2):
        if e > 0:
            xx = lax.rem(x + nx - e, nx)

            def arrived(d, carry):
                zz = lax.rem(z + nz - d, nz)
                sender(own, block(xx, zz), x_send.at[e, d], x_recv.at[e, d], x, z, s).wait_recv()
                return carry
            lax.fori_loop(0, nz, arrived, 0)
        c_copy(e, s).start()
    for e in range(nx):
        c_copy(e, 1 - s).wait_recv()

    def done_z(d, carry):
        z_copy(d).wait_send()
        return carry
    lax.fori_loop(1, nz, done_z, 0)
    for e in range(1, nx):
        def done_x(d, carry):
            x_copy(own, z, d, e).wait_send()
            return carry
        lax.fori_loop(0, nz, done_x, 0)
    for e in range(nx):
        c_copy(e, s).wait_send()


def gather_gains(gains, base, bases, nx, nz):
    vmem = pl.BlockSpec(memory_space=pltpu.VMEM)
    dma = pltpu.SemaphoreType.DMA
    here, rows, _ = gains.shape
    slots = -(-(base.shape[1] + GROUP * (bases + 6)) // 128) * 128
    return pl.pallas_call(
        functools.partial(gather_kernel, nx, nz, bases),
        out_shape=(jax.ShapeDtypeStruct((nx * nz * here, rows, 2 * HALF), BF),
                   jax.ShapeDtypeStruct((1, slots), jnp.int32), jax.ShapeDtypeStruct((1, 128), jnp.int32)),
        in_specs=[vmem, vmem],
        out_specs=(vmem, vmem, vmem),
        scratch_shapes=[pltpu.VMEM((here, rows, 2 * HALF), F32), pltpu.VMEM((here, rows, 2 * HALF), BF),
                        dma((nz,)), dma((nz,)), dma((nx, nz)), dma((nx, nz)), dma((nx,)), dma((nx,))],
        compiler_params=pltpu.CompilerParams(collective_id=0, has_side_effects=True,
                                             vmem_limit_bytes=8 * 1024 * 1024),
        cost_estimate=pl.CostEstimate(flops=20000000000, bytes_accessed=20000000, transcendentals=0),
        name="gather_gains",
    )(gains, base)


def packed(v, plain):
    head = v[plain:].astype(BF)
    tail = v[plain:] - head.astype(F32)
    return jnp.concatenate([v[:plain].astype(BF), head, tail.astype(BF)], axis=0)


def unpacked(w, plain):
    v = w.astype(F32)
    mid = (v.shape[0] + plain) // 2
    return jnp.concatenate([v[:plain], v[plain:mid] + v[mid:]], axis=0)


def finish_kernel(nx, nz, inverse, sums, gains, duals, cons, rho, gain_new, cons_new, dual_new,
                  peer, two_out, two_in, x_out, x_in, z_out, z_in, z_sum, total, full, wide,
                  part_out, part_in, ring_in, last_in,
                  c_send, c_recv, t_send, t_recv, x_send, x_recv, z_send, z_recv,
                  p_send, p_recv, r_send, r_recv, l_send, l_recv, token):
    x, z, s = place()
    directions = rho.shape[0]
    degrees, _, stations = cons.shape
    half_count = duals.shape[0]
    plain = directions * directions
    chunk = 4
    nodes = nx * nz
    barrier, count = meet(x, z, s, nx, nz, 1, True)

    wide[...] = jnp.zeros(wide.shape, F32)
    for h in range(half_count):
        wide[0, :, h * HALF:h * HALF + stations] = gains[s * half_count + h]
        wide[1, :, h * HALF:h * HALF + stations] = duals[h]
        for d in range(degrees):
            wide[2 + d, :, h * HALF:h * HALF + stations] = cons[d]
    basis = legendre(((x * nz + z) * 2 + s) * half_count, 2 * nodes * half_count)
    pl.semaphore_wait(barrier, count)

    def far(i):
        if isinstance(i, int):
            return (nz // 2 + (i + 1) // 2 * (1 if i % 2 == 0 else -1)) % nz
        step = (i + 1) // 2
        return lax.rem(jnp.where(lax.rem(i, 2) == 0, nz // 2 + step, nz // 2 + nz - step), nz)

    def tell():
        for side in range(2):
            pl.semaphore_signal(token.at[side], inc=1, device_id={XS: x, ZS: lax.rem(z + (1, nz - 1)[side], nz), "sub": s},
                                device_id_type=pl.DeviceIdType.MESH)

    def hear():
        for side in range(2):
            pl.semaphore_wait(token.at[side], 1)
    n_tokens = nz // 2 - 1
    tell()

    def c_copy(e, h):
        xx = lax.rem(x + e, nx)
        return sender(sums.at[pl.ds(h * nodes + xx * nz, nz)], peer.at[pl.ds(xx * nz, nz)],
                      c_send.at[e], c_recv.at[e], x, z, 1 - s)
    across, right, left_ = nx // 2, 1, nx - 1
    order = (across, right, left_, 0)
    for e in order:
        c_copy(e, 1 - s).start()

    def pair_sum(xx, zz):
        return sums[s * nodes + xx * nz + zz] + peer[xx * nz + zz]

    chunks = nz // chunk
    share = chunk // 2
    def t_copy(side, c):
        at = pl.ds(c * chunk + side * share, share)
        return sender(two_out.at[at], two_in.at[at], t_send.at[side, c], t_recv.at[side, c],
                      lax.rem(x + (right, left_)[side], nx), z, s)

    def fill_two(c):
        def one(j, inner):
            i = c * chunk + j
            two_out[i] = packed(pair_sum(lax.rem(x + across, nx), lax.rem(z + far(i), nz)), plain)
            return inner
        lax.fori_loop(0, chunk, one, 0)
        for side in range(2):
            t_copy(side, c).start()

    def x_copy(side, c):
        at = pl.ds(c * chunk, chunk)
        return sender(x_out.at[side, at], x_in.at[side, at], x_send.at[side, c], x_recv.at[side, c],
                      lax.rem(x + (right, left_)[side], nx), z, s)

    def fill_x(c):
        for side in range(2):
            t_copy(side, c).wait_recv()
            xx = lax.rem(x + (right, left_)[side], nx)

            def relayed(j, inner):
                i = c * chunk + side * share + j
                x_out[side, i] = packed(pair_sum(xx, lax.rem(z + far(i), nz)) + unpacked(two_in[i], plain), plain)
                return inner

            def plainly(j, inner):
                i = c * chunk + (1 - side) * share + j
                x_out[side, i] = packed(pair_sum(xx, lax.rem(z + far(i), nz)), plain)
                return inner
            lax.fori_loop(0, share, relayed, 0)
            lax.fori_loop(0, share, plainly, 0)
            x_copy(side, c).start()

    quarter = nz // 4
    n_far = 2 * quarter - 1
    odd = lax.rem(z, 2)

    def hop(i):
        d = far(i)
        if i >= n_far:
            return d
        if i == 0:
            return quarter + 2 * quarter * odd
        return d - quarter if i % 2 == 1 else d + quarter

    def z_copy(i):
        return sender(z_out.at[i], z_in.at[i], z_send.at[i], z_recv.at[i], x, lax.rem(z + hop(i), nz), s)

    def fill_z(c):
        for side in range(2):
            x_copy(side, c).wait_recv()

        def one(j, inner):
            i = c * chunk + j
            acc = pair_sum(x, lax.rem(z + far(i), nz))
            for side in range(2):
                acc = acc + unpacked(x_in[side, i], plain)
            z_out[i] = packed(acc, plain)
            z_sum[i] = acc
            return inner
        lax.fori_loop(0, chunk, one, 0)
        for i in range(c * chunk, (c + 1) * chunk):
            if i not in (n_far, n_far + 1, nz - 1):
                z_copy(i).start()

    def relay_z():
        for i in range(n_far):
            z_copy(i).wait_recv()
            to = n_far + odd if i == 0 else n_far + (i + 1) % 2
            z_sum[to] = z_sum[to] + unpacked(z_in[i], plain)
        for i in (n_far, n_far + 1):
            z_out[i] = packed(z_sum[i], plain)
        for i in (n_far, n_far + 1):
            z_copy(i).start()

    c_copy(across, s).wait_recv()
    hear()
    tell()
    for c in range(chunks - 1):
        fill_two(c)
    hear()
    tell()
    c_copy(right, s).wait_recv()
    c_copy(left_, s).wait_recv()
    fill_x(0)
    hear()
    tell()
    fill_two(chunks - 1)
    fill_x(1)
    c_copy(0, s).wait_recv()
    for c in range(chunks):
        if c == chunks - 1:
            relay_z()
        fill_z(c)
        if c + 2 < chunks:
            fill_x(c + 2)
        hear()
        if c + 4 < n_tokens:
            tell()
    acc = z_sum[nz - 1]
    for i in list(range(n_far + 2, nz - 1)) + [n_far, n_far + 1]:
        z_copy(i).wait_recv()
        acc = acc + unpacked(z_in[i], plain)
    total[...] = acc

    rho2 = jnp.concatenate([rho[...], rho[...]], axis=0)
    gain, dual = wide[0], wide[1]
    anchor = sum(basis[d] * wide[2 + d] for d in range(degrees))
    target = total[plain:, :] - dual - rho2 * (gain - anchor)
    new = gain + eliminate(total, target, rho[...], full, directions)
    for h in range(half_count):
        gain_new[h] = new[:, h * HALF:h * HALF + stations]
    weighted = new + dual / rho2
    left = lax.broadcasted_iota(jnp.int32, (2 * directions, 2 * HALF), 1) < HALF

    def folded(d):
        part = basis[d] * weighted
        return part + pltpu.roll(part, HALF, axis=1)
    pair = degrees // 2
    both = jnp.concatenate([jnp.where(left, folded(d), folded(d + pair)) for d in range(pair)], axis=0)
    pieces, piece = part_out.shape[0], part_out.shape[1]
    for m in range(pieces):
        part_out[m] = both[m * piece:(m + 1) * piece, :]

    near = [(e, f) for e in range(nx) for f in range(2) if e + f > 0]

    def other(e, f):
        return lax.rem(x + e, nx), s + f - 2 * s * f

    def p_copy(e, f):
        xx, ss = other(e, f)
        return sender(part_out.at[xx * 2 + ss], part_in.at[e * 2 + f], p_send.at[e * 2 + f],
                      p_recv.at[e * 2 + f], xx, z, ss)
    for e, f in near:
        p_copy(e, f).start()
    acc = part_out[x * 2 + s]
    for e, f in near:
        p_copy(e, f).wait_recv()
        acc = acc + part_in[e * 2 + f]
    ring_in[z] = acc

    def r_copy(d):
        zz = lax.rem(z + d, nz)
        return sender(ring_in.at[z], ring_in.at[z], r_send.at[d], r_recv.at[d], x, zz, s)

    def start_r(i, carry):
        r_copy(far(i)).start()
        return carry
    lax.fori_loop(0, nz - 1, start_r, 0)

    def take_r(i, carry):
        d = far(i)
        zz = lax.rem(z + nz - d, nz)
        sender(ring_in.at[zz], ring_in.at[zz], r_send.at[d], r_recv.at[d], x, z, s).wait_recv()
        return carry
    lax.fori_loop(0, nz - 1, take_r, 0)
    acc = ring_in[0]
    for i in range(1, nz):
        acc = acc + ring_in[i]
    me = x * 2 + s
    last_in[me] = acc

    def l_copy(e, f, m):
        xx, ss = other(e, f)
        return sender(last_in.at[m], last_in.at[m], l_send.at[e * 2 + f], l_recv.at[e * 2 + f], xx, z, ss)
    for e, f in near:
        l_copy(e, f, me).start()
    for e, f in near:
        back = lax.rem(x + nx - e, nx) * 2 + (s + f - 2 * s * f)
        l_copy(e, f, back).wait_recv()
    both = jnp.concatenate([last_in[m] for m in range(pieces)], axis=0)
    wide = 2 * directions
    summed = [None] * degrees
    for d in range(pair):
        rows = both[d * wide:(d + 1) * wide, :]
        turned = pltpu.roll(rows, HALF, axis=1)
        summed[d] = jnp.where(left, rows, turned)
        summed[d + pair] = jnp.where(left, turned, rows)
    fit = None
    for d in range(degrees):
        coeff = sum(inverse[d][q] * summed[q] for q in range(degrees))
        cons_new[d] = coeff[:, :stations]
        term = basis[d] * coeff
        fit = term if fit is None else fit + term
    dual_out = dual + rho2 * (new - fit)
    for h in range(half_count):
        dual_new[h] = dual_out[:, h * HALF:h * HALF + stations]

    for e in range(nx):
        c_copy(e, 1 - s).wait_send()

    for c in range(chunks):
        for side in range(2):
            t_copy(side, c).wait_send()
            x_copy(side, c).wait_send()
    for i in range(nz - 1):
        z_copy(i).wait_send()
        r_copy(i + 1).wait_send()
    for e, f in near:
        p_copy(e, f).wait_send()
        l_copy(e, f, me).wait_send()


def finish(sums, gains, duals, cons, rho, inverse, nx, nz):
    vmem = pl.BlockSpec(memory_space=pltpu.VMEM)
    dma = pltpu.SemaphoreType.DMA
    degrees, rows, _ = cons.shape
    terms, lanes = sums.shape[1:]
    wire = terms + rows
    pieces = 2 * nx
    piece = degrees * rows // 2 // pieces
    chunks = nz // 4
    return pl.pallas_call(
        functools.partial(finish_kernel, nx, nz, inverse),
        out_shape=(jax.ShapeDtypeStruct(duals.shape, F32), jax.ShapeDtypeStruct(cons.shape, F32),
                   jax.ShapeDtypeStruct(duals.shape, F32)),
        in_specs=[vmem] * 5,
        out_specs=(vmem, vmem, vmem),
        scratch_shapes=[
            pltpu.VMEM((nx * nz, terms, lanes), F32),
            pltpu.VMEM((nz, wire, lanes), BF),
            pltpu.VMEM((nz, wire, lanes), BF),
            pltpu.VMEM((2, nz, wire, lanes), BF),
            pltpu.VMEM((2, nz, wire, lanes), BF),
            pltpu.VMEM((nz, wire, lanes), BF),
            pltpu.VMEM((nz, wire, lanes), BF),
            pltpu.VMEM((nz, terms, lanes), F32),
            pltpu.VMEM((terms, lanes), F32),
            pltpu.VMEM((2, rows * rows // 4, lanes), F32),
            pltpu.VMEM((2 + degrees, rows, lanes), F32),
            pltpu.VMEM((pieces, piece, lanes), F32),
            pltpu.VMEM((pieces, piece, lanes), F32),
            pltpu.VMEM((nz, piece, lanes), F32),
            pltpu.VMEM((pieces, piece, lanes), F32),
            dma((nx,)), dma((nx,)), dma((2, chunks)), dma((2, chunks)), dma((2, chunks)), dma((2, chunks)),
            dma((nz,)), dma((nz,)),
            dma((pieces,)), dma((pieces,)), dma((nz,)), dma((nz,)), dma((pieces,)), dma((pieces,)),
            pltpu.SemaphoreType.REGULAR((2,)),
        ],
        compiler_params=pltpu.CompilerParams(collective_id=1, has_side_effects=True,
                                             vmem_limit_bytes=18 * 1024 * 1024),
        name="finish",
    )(sums, gains, duals, cons, rho)


def to_rows(x):
    n, c, s, k = x.shape
    return jnp.transpose(x, (0, 1, 3, 2)).reshape(n, c * k, s)


def from_rows(x):
    n, rows, s = x.shape
    return jnp.transpose(x.reshape(n, 2, rows // 2, s), (0, 1, 3, 2))


def body(sky, seen, keep, tile_owner, tile_channel, tile_base, pairs, gains, duals, consensus, rho):
    channels_here, _, _, directions = gains.shape
    nx, nz = lax.axis_size(XS), lax.axis_size(ZS)
    sub_count = lax.axis_size("sub")
    half_count = channels_here // sub_count
    gain_rows = to_rows(gains)
    table, order, groups = gather_gains(gain_rows, tile_base.reshape(1, -1), pairs.shape[0], nx, nz)
    sums = tile_sums(sky, seen, keep, order, groups, tile_owner[:, 0], tile_channel, tile_base, pairs, table,
                     nx * nz * sub_count, half_count)
    rho_rows = jnp.broadcast_to(rho[:, None], (directions, 2 * HALF))
    gain_new, cons_new, dual_new = finish(sums, gain_rows, to_rows(duals), to_rows(consensus), rho_rows,
                                          gram_inverse(channels_here * nx * nz).tolist(), nx, nz)
    return from_rows(gain_new), from_rows(cons_new), from_rows(dual_new)


def solution(mesh):
    groups, subs = mesh.shape["groups"], mesh.shape["sub"]
    torus = Mesh(mesh.devices.reshape(groups, 4, mesh.shape["chan"] // 4, subs), GROUPS_CHAN_SUB)
    return jax.shard_map(
        body,
        mesh=torus,
        in_specs=(
            P(GROUPS_CHAN_SUB, None, None, None),
            P(GROUPS_CHAN_SUB, None, None),
            P(GROUPS_CHAN_SUB, None),
            P(GROUPS_CHAN_SUB, None),
            P(GROUPS_CHAN_SUB),
            P(GROUPS_CHAN_SUB),
            P(),
            P(GROUPS_CHAN, None, None, None),
            P(GROUPS_CHAN_SUB, None, None, None),
            P("groups", None, None, None),
            P(),
        ),
        out_specs=(
            P(GROUPS_CHAN_SUB, None, None, None),
            P("groups", None, None, None),
            P(GROUPS_CHAN_SUB, None, None, None),
        ),
        check_vma=False,
    )
```

```python
import functools

import jax
import jax.numpy as jnp
import numpy as np
from jax import lax
from jax.experimental import pallas as pl
from jax.experimental.pallas import tpu as pltpu
from jax.sharding import Mesh
from jax.sharding import PartitionSpec as P

GROUPS_CHAN_SUB = ("groups", "chan_0", "chan_1", "sub")
GROUPS_CHAN = ("groups", "chan_0", "chan_1")
BF, F32 = jnp.bfloat16, jnp.float32
GROUP = 8
HALF = 64


def term_rows(directions):
    real, imag = {}, {}
    for k in range(directions):
        for m in range(k, directions):
            real[k, m] = len(real)
    for k in range(directions):
        for m in range(k + 1, directions):
            imag[k, m] = len(real) + len(imag)
    return real, imag


def legendre(first, channels):
    lane = lax.broadcasted_iota(jnp.int32, (1, 2 * HALF), 1)
    place = (first + lane // HALF).astype(F32)
    x = (2.0 * place - (channels - 1)) / max(channels - 1, 1)
    return [jnp.ones_like(x), x, 0.5 * (3.0 * x * x - 1.0), 0.5 * (5.0 * x * x * x - 3.0 * x)]


def gram_inverse(channels):
    x = (2.0 * np.arange(channels, dtype=np.float64) - (channels - 1)) / max(channels - 1, 1)
    basis = np.stack([np.ones_like(x), x, 0.5 * (3 * x * x - 1), 0.5 * (5 * x * x * x - 3 * x)])
    return np.linalg.inv(basis @ basis.T)


def tile_order(base, bases, slots):
    tiles = base.shape[1]
    padded_bases = -(-bases // 16) * 16
    member = lax.broadcasted_iota(jnp.int32, (padded_bases, tiles), 0) == base
    hit = jnp.where(member, 1.0, 0.0)
    before = jnp.where(lax.broadcasted_iota(jnp.int32, (tiles, tiles), 0)
                       < lax.broadcasted_iota(jnp.int32, (tiles, tiles), 1), 1.0, 0.0).astype(BF)
    rank = jnp.dot(hit.astype(BF), before, preferred_element_type=F32)
    counts = jnp.sum(hit, axis=1, keepdims=True).astype(jnp.int32)
    groups = lax.shift_right_logical(counts + (GROUP - 1), GROUP.bit_length() - 1).astype(F32)
    lower = jnp.where(lax.broadcasted_iota(jnp.int32, (padded_bases, padded_bases), 1)
                      < lax.broadcasted_iota(jnp.int32, (padded_bases, padded_bases), 0), 1.0, 0.0).astype(BF)
    start = jnp.dot(lower, jnp.broadcast_to(groups, (padded_bases, tiles)).astype(BF),
                    preferred_element_type=F32)
    where = jnp.sum(jnp.where(member, rank + GROUP * start, 0.0), axis=0, keepdims=True).astype(jnp.int32)
    chosen = jnp.where(lax.broadcasted_iota(jnp.int32, (slots, tiles), 0) == where, 1.0, 0.0).astype(BF)
    tile = lax.broadcasted_iota(jnp.int32, (8, tiles), 1)
    kind = lax.broadcasted_iota(jnp.int32, (8, tiles), 0)
    digits = jnp.where(kind == 0, lax.shift_right_logical(tile, 4),
                       jnp.where(kind == 1, jnp.bitwise_and(tile, 15), 1)).astype(F32).astype(BF)
    found = lax.dot_general(digits, chosen, (((1,), (1,)), ((), ())), preferred_element_type=F32)
    named = jnp.where(found[2:3] > 0.5, 16.0 * found[0:1] + found[1:2], float(tiles)).astype(jnp.int32)
    total = jnp.broadcast_to(jnp.sum(groups, axis=0, keepdims=True), (1, 128)).astype(jnp.int32)
    return named, total


def tile_kernel(half_count, order, groups, owner, channel, base, sky, seen, keep, pairs, table, out, onehot, *buffers):
    tiles, coupled, rows = sky.shape
    directions = coupled // 2
    bases = pairs.shape[0]
    real, imag = term_rows(directions)
    n_terms = directions * directions + 2 * directions
    devices = out.shape[0] - 1
    channels_here = table.shape[0] // (devices // 2)
    chans = devices // 2
    buffers = (buffers[0::2], buffers[1::2])

    station = lax.rem(lax.broadcasted_iota(jnp.int32, (2 * HALF, rows), 0), HALF)
    for b in range(bases):
        for side in range(2):
            onehot[b, :, side * rows:(side + 1) * rows] = jnp.where(
                station == pairs[b, side:side + 1, :], 1.0, 0.0).astype(BF)

    def clear(i, carry):
        out[i] = jnp.zeros((n_terms, 2 * HALF), F32)
        return carry
    lax.fori_loop(0, devices + 1, clear, 0)
    lane = lax.broadcasted_iota(jnp.int32, (1, 2 * HALF), 1)

    def chosen(g):
        first = order[0, jnp.maximum(g, 0) * GROUP]
        return onehot.at[base[jnp.minimum(first, tiles - 1)]]

    def load(g, into):
        sky_s, seen_s, keep_s, gain_s, near_far, _, _ = buffers[into]
        for t in range(GROUP):
            named = order[0, g * GROUP + t]
            tile = jnp.where(named < tiles, named, 0)
            kept = keep[pl.ds(tile, 1), :] > 0
            sky_s[pl.ds(t, coupled, stride=GROUP), :] = jnp.where(kept, sky[tile].astype(F32), 0.0)
            seen_s[pl.ds(t, 2, stride=GROUP), :] = jnp.where(kept, seen[tile].astype(F32), 0.0)
            gain_s[pl.ds(t, coupled, stride=GROUP), :] = table[owner[tile] * channels_here + channel[tile]].astype(F32)
        near_far[...] = jnp.dot(gain_s[...].astype(BF), chosen(g)[...], preferred_element_type=F32)

    def products(of):
        sky_s, seen_s, keep_s, _, near_far, terms, _ = buffers[of]
        def block(ref, i):
            return ref[i * GROUP:(i + 1) * GROUP, :]

        res_r = block(seen_s, 0)
        res_i = block(seen_s, 1)
        v_r, v_i = [], []
        for k in range(directions):
            c_r = block(sky_s, 2 * k)
            c_i = block(sky_s, 2 * k + 1)
            p_r, p_i = (block(near_far, c * directions + k)[:, :rows] for c in range(2))
            q_r, q_i = (block(near_far, c * directions + k)[:, rows:] for c in range(2))
            x_r = c_r * q_r + c_i * q_i
            x_i = c_i * q_r - c_r * q_i
            v_r.append(x_r)
            v_i.append(x_i)
            res_r = res_r - (p_r * x_r - p_i * x_i)
            res_i = res_i - (p_r * x_i + p_i * x_r)
        w_r, w_i = res_r, res_i

        for side in range(2):
            pending = {}

            def put(j, value):
                pending[j] = value
                lo = j - j % 2
                if lo in pending and lo + 1 in pending:
                    both = jnp.concatenate([pending.pop(lo), pending.pop(lo + 1)], axis=0)
                    terms[lo * GROUP:(lo + 2) * GROUP, side * rows:(side + 1) * rows] = both.astype(BF)

            if side == 1:
                v_r, v_i, w_i = [], [], -res_i
                for k in range(directions):
                    c_r = block(sky_s, 2 * k)
                    c_i = block(sky_s, 2 * k + 1)
                    p_r, p_i = (block(near_far, c * directions + k)[:, :rows] for c in range(2))
                    v_r.append(c_r * p_r - c_i * p_i)
                    v_i.append(-(c_r * p_i + c_i * p_r))
            for (k, m), j in real.items():
                put(j, v_r[k] * v_r[m] + v_i[k] * v_i[m])
            for (k, m), j in imag.items():
                put(j, v_r[k] * v_i[m] - v_i[k] * v_r[m])
            first = directions * directions
            for k in range(directions):
                put(first + k, v_r[k] * w_r + v_i[k] * w_i)
            for k in range(directions):
                put(first + directions + k, v_r[k] * w_i - v_i[k] * w_r)

    def station_sums(g, of):
        terms, sums = buffers[of][5:]
        sums[...] = lax.dot_general(terms[...], chosen(g)[...], (((1,), (1,)), ((), ())),
                                    preferred_element_type=F32)

    def add_up(g, of):
        sums = buffers[of][6]
        for t in range(GROUP):
            named = jnp.where(g < 0, tiles, order[0, jnp.maximum(g, 0) * GROUP + t])
            tile = jnp.where(named < tiles, named, 0)
            mine = channel[tile]
            row = jnp.where(named < tiles, (mine // half_count) * chans + owner[tile], devices)
            part = jnp.where(lane // HALF == lax.rem(mine, half_count),
                             sums[pl.ds(t, n_terms, stride=GROUP), :], 0.0)
            out[row] = out[row] + part

    def step(g, of):
        station_sums(g - 2, of)
        add_up(g - 3, 1 - of)
        load(g, of)
        products(1 - of)

    def two(i, carry):
        step(2 * i, 0)
        step(2 * i + 1, 1)
        return carry

    lax.fori_loop(0, (groups[0, 0] + 4) // 2, two, 0)


def tile_sums(sky, seen, keep, order, groups, owner, channel, base, pairs, table, devices, half_count):
    tiles, directions, _, rows = sky.shape
    n_terms = directions * directions + 2 * directions
    bases = pairs.shape[0]
    smem = pl.BlockSpec(memory_space=pltpu.SMEM)
    vmem = pl.BlockSpec(memory_space=pltpu.VMEM)
    coupled = 2 * directions
    return pl.pallas_call(
        functools.partial(tile_kernel, half_count),
        out_shape=jax.ShapeDtypeStruct((devices + 1, n_terms, 2 * HALF), F32),
        in_specs=[smem] * 5 + [vmem] * 5,
        out_specs=vmem,
        scratch_shapes=[pltpu.VMEM((bases, 2 * HALF, 2 * rows), BF)] + [
            shape for shape in (
                pltpu.VMEM((coupled * GROUP, rows), F32),
                pltpu.VMEM((2 * GROUP, rows), F32),
                pltpu.VMEM((GROUP, rows), jnp.int32),
                pltpu.VMEM((coupled * GROUP, 2 * HALF), F32),
                pltpu.VMEM((coupled * GROUP, 2 * rows), F32),
                pltpu.VMEM((n_terms * GROUP, 2 * rows), BF),
                pltpu.VMEM((n_terms * GROUP, 2 * HALF), F32),
            ) for _ in range(2)
        ],
        compiler_params=pltpu.CompilerParams(vmem_limit_bytes=18 * 1024 * 1024),
        name="tile_sums",
    )(order, groups, owner, channel, base, sky.reshape(tiles, coupled, rows), seen, keep, pairs, table)


def eliminate(total, target, rho, full, directions):
    real, imag = term_rows(directions)
    lanes = total.shape[-1]
    for k in range(directions):
        for m in range(directions):
            re = real[min(k, m), max(k, m)]
            value = total[re:re + 1, :]
            if k == m:
                value = value + rho[k:k + 1, :]
                full[1, k * directions + m:k * directions + m + 1, :] = jnp.zeros((1, lanes), F32)
            else:
                im = imag[min(k, m), max(k, m)]
                imv = total[im:im + 1, :]
                full[1, k * directions + m:k * directions + m + 1, :] = imv if k < m else -imv
            full[0, k * directions + m:k * directions + m + 1, :] = value
    row_r = [full[0, k * directions:(k + 1) * directions, :] for k in range(directions)]
    row_i = [full[1, k * directions:(k + 1) * directions, :] for k in range(directions)]
    t_r = [target[k:k + 1, :] for k in range(directions)]
    t_i = [target[directions + k:directions + k + 1, :] for k in range(directions)]
    for k in range(directions):
        inv = 1.0 / row_r[k][k:k + 1, :]
        row_r[k] = row_r[k] * inv
        row_i[k] = row_i[k] * inv
        t_r[k] = t_r[k] * inv
        t_i[k] = t_i[k] * inv
        for m in range(directions):
            if m == k:
                continue
            f_r = row_r[m][k:k + 1, :]
            f_i = row_i[m][k:k + 1, :]
            row_r[m], row_i[m] = (row_r[m] - (f_r * row_r[k] - f_i * row_i[k]),
                                  row_i[m] - (f_r * row_i[k] + f_i * row_r[k]))
            t_r[m], t_i[m] = (t_r[m] - (f_r * t_r[k] - f_i * t_i[k]),
                              t_i[m] - (f_r * t_i[k] + f_i * t_r[k]))
    return jnp.concatenate(t_r + t_i, axis=0)


XS, ZS = "chan_0", "chan_1"


def place():
    return lax.axis_index(XS), lax.axis_index(ZS), lax.axis_index("sub")


def sender(src, dst, send_sem, recv_sem, x, z, s):
    return pltpu.make_async_remote_copy(
        src_ref=src, dst_ref=dst, send_sem=send_sem, recv_sem=recv_sem,
        device_id={XS: x, ZS: z, "sub": s}, device_id_type=pl.DeviceIdType.MESH)


def meet(x, z, s, nx, nz, reach, crossed):
    barrier = pltpu.get_barrier_semaphore()

    def ring(d, carry):
        pl.semaphore_signal(barrier, inc=1, device_id={XS: x, ZS: lax.rem(z + d, nz), "sub": s},
                            device_id_type=pl.DeviceIdType.MESH)
        return carry
    lax.fori_loop(1, reach + 1, ring, 0)
    lax.fori_loop(max(reach + 1, nz - reach), nz, ring, 0)
    near = [(e, f) for e in range(nx) for f in range(2) if e + f > 0 and (crossed or e * f == 0)]
    for e, f in near:
        pl.semaphore_signal(barrier, inc=1,
                            device_id={XS: lax.rem(x + e, nx), ZS: z, "sub": s + f - 2 * s * f},
                            device_id_type=pl.DeviceIdType.MESH)
    return barrier, min(nz - 1, 2 * reach) + len(near)


def outward(i, nz):
    return jnp.where(lax.rem(i, 2) == 0, i // 2 + 1, nz - 1 - i // 2)


def gather_kernel(nx, nz, bases, gains, base, table, order, groups, wide, mine,
                  z_recv, z_send, x_recv, x_send, c_recv, c_send):
    x, z, s = place()
    here, half = mine.shape[0], mine.shape[0] // 2
    stations = gains.shape[2]
    barrier, count = meet(x, z, s, nx, nz, nz - 1, False)
    wide[...] = jnp.zeros(wide.shape, F32)
    head = gains[...].astype(BF).astype(F32)
    wide[:, :, :stations] = head
    wide[:, :, HALF:HALF + stations] = gains[...] - head
    mine[...] = wide[...].astype(BF)
    table[pl.ds((x * nz + z) * here + s * half, half)] = mine[pl.ds(s * half, half)]
    pl.semaphore_wait(barrier, count)

    def block(xx, zz):
        return table.at[pl.ds((xx * nz + zz) * here + s * half, half)]

    def rows(xx, h):
        return table.at[pl.ds(xx * nz * here, nz * here)].reshape(nz, here, *mine.shape[1:]).at[:, pl.ds(h * half, half)]

    own = mine.at[pl.ds(s * half, half)]

    def z_copy(d):
        return sender(own, block(x, z), z_send.at[d], z_recv.at[d], x, lax.rem(z + d, nz), s)

    def start_z(i, carry):
        z_copy(outward(nz - 2 - i, nz)).start()
        return carry
    lax.fori_loop(0, nz - 1, start_z, 0)

    def x_copy(src, zz, d, e):
        return sender(src, block(x, zz), x_send.at[e, d], x_recv.at[e, d], lax.rem(x + e, nx), z, s)
    for e in range(1, nx):
        x_copy(own, z, 0, e).start()
    order[...], groups[...] = tile_order(base[...], bases, order.shape[1])

    def pass_on(i, carry):
        d = outward(i, nz)
        zz = lax.rem(z + nz - d, nz)
        sender(own, block(x, zz), z_send.at[d], z_recv.at[d], x, z, s).wait_recv()
        for e in (nx // 2, 1, nx - 1):
            x_copy(block(x, zz), zz, d, e).start()
        return carry
    lax.fori_loop(0, nz - 1, pass_on, 0)

    def c_copy(e, h):
        xx = lax.rem(x + nx - e, nx)
        return sender(rows(xx, h), rows(xx, h), c_send.at[e], c_recv.at[e], x, z, 1 - s)
    for e in (0, 1, 3, 2):
        if e > 0:
            xx = lax.rem(x + nx - e, nx)

            def arrived(d, carry):
                zz = lax.rem(z + nz - d, nz)
                sender(own, block(xx, zz), x_send.at[e, d], x_recv.at[e, d], x, z, s).wait_recv()
                return carry
            lax.fori_loop(0, nz, arrived, 0)
        c_copy(e, s).start()
    for e in range(nx):
        c_copy(e, 1 - s).wait_recv()

    def done_z(d, carry):
        z_copy(d).wait_send()
        return carry
    lax.fori_loop(1, nz, done_z, 0)
    for e in range(1, nx):
        def done_x(d, carry):
            x_copy(own, z, d, e).wait_send()
            return carry
        lax.fori_loop(0, nz, done_x, 0)
    for e in range(nx):
        c_copy(e, s).wait_send()


def gather_gains(gains, base, bases, nx, nz):
    vmem = pl.BlockSpec(memory_space=pltpu.VMEM)
    dma = pltpu.SemaphoreType.DMA
    here, rows, _ = gains.shape
    slots = -(-(base.shape[1] + GROUP * (bases + 6)) // 128) * 128
    return pl.pallas_call(
        functools.partial(gather_kernel, nx, nz, bases),
        out_shape=(jax.ShapeDtypeStruct((nx * nz * here, rows, 2 * HALF), BF),
                   jax.ShapeDtypeStruct((1, slots), jnp.int32), jax.ShapeDtypeStruct((1, 128), jnp.int32)),
        in_specs=[vmem, vmem],
        out_specs=(vmem, vmem, vmem),
        scratch_shapes=[pltpu.VMEM((here, rows, 2 * HALF), F32), pltpu.VMEM((here, rows, 2 * HALF), BF),
                        dma((nz,)), dma((nz,)), dma((nx, nz)), dma((nx, nz)), dma((nx,)), dma((nx,))],
        compiler_params=pltpu.CompilerParams(collective_id=0, has_side_effects=True,
                                             vmem_limit_bytes=8 * 1024 * 1024),
        cost_estimate=pl.CostEstimate(flops=20000000000, bytes_accessed=20000000, transcendentals=0),
        name="gather_gains",
    )(gains, base)


def packed(v, plain):
    head = v[plain:].astype(BF)
    tail = v[plain:] - head.astype(F32)
    return jnp.concatenate([v[:plain].astype(BF), head, tail.astype(BF)], axis=0)


def unpacked(w, plain):
    v = w.astype(F32)
    mid = (v.shape[0] + plain) // 2
    return jnp.concatenate([v[:plain], v[plain:mid] + v[mid:]], axis=0)


def finish_kernel(nx, nz, inverse, sums, gains, duals, cons, rho, result,
                  peer, two_out, two_in, x_out, x_in, z_out, z_in, z_sum, total, full, wide,
                  part_out, part_in, ring_in, last_in,
                  c_send, c_recv, t_send, t_recv, x_send, x_recv, z_send, z_recv,
                  p_send, p_recv, r_send, r_recv, l_send, l_recv, token):
    x, z, s = place()
    directions = rho.shape[0]
    degrees, _, stations = cons.shape
    half_count = duals.shape[0]
    gain_new, dual_new = result.at[:half_count], result.at[half_count:2 * half_count]
    cons_new = result.at[2 * half_count:]
    plain = directions * directions
    chunk = 4
    nodes = nx * nz
    barrier, count = meet(x, z, s, nx, nz, 1, True)

    wide[...] = jnp.zeros(wide.shape, F32)
    for h in range(half_count):
        wide[0, :, h * HALF:h * HALF + stations] = gains[s * half_count + h]
        wide[1, :, h * HALF:h * HALF + stations] = duals[h]
        for d in range(degrees):
            wide[2 + d, :, h * HALF:h * HALF + stations] = cons[d]
    basis = legendre(((x * nz + z) * 2 + s) * half_count, 2 * nodes * half_count)
    pl.semaphore_wait(barrier, count)

    def far(i):
        if isinstance(i, int):
            return (nz // 2 + (i + 1) // 2 * (1 if i % 2 == 0 else -1)) % nz
        step = (i + 1) // 2
        return lax.rem(jnp.where(lax.rem(i, 2) == 0, nz // 2 + step, nz // 2 + nz - step), nz)

    def tell():
        for side in range(2):
            pl.semaphore_signal(token.at[side], inc=1, device_id={XS: x, ZS: lax.rem(z + (1, nz - 1)[side], nz), "sub": s},
                                device_id_type=pl.DeviceIdType.MESH)

    def hear():
        for side in range(2):
            pl.semaphore_wait(token.at[side], 1)
    n_tokens = nz // 2 - 1
    tell()

    def c_copy(e, h):
        xx = lax.rem(x + e, nx)
        return sender(sums.at[pl.ds(h * nodes + xx * nz, nz)], peer.at[pl.ds(xx * nz, nz)],
                      c_send.at[e], c_recv.at[e], x, z, 1 - s)
    across, right, left_ = nx // 2, 1, nx - 1
    order = (across, right, left_, 0)
    for e in order:
        c_copy(e, 1 - s).start()

    def pair_sum(xx, zz):
        return sums[s * nodes + xx * nz + zz] + peer[xx * nz + zz]

    chunks = nz // chunk
    share = chunk // 2
    def t_copy(side, c):
        at = pl.ds(c * chunk + side * share, share)
        return sender(two_out.at[at], two_in.at[at], t_send.at[side, c], t_recv.at[side, c],
                      lax.rem(x + (right, left_)[side], nx), z, s)

    def fill_two(c):
        def one(j, inner):
            i = c * chunk + j
            two_out[i] = packed(pair_sum(lax.rem(x + across, nx), lax.rem(z + far(i), nz)), plain)
            return inner
        lax.fori_loop(0, chunk, one, 0)
        for side in range(2):
            t_copy(side, c).start()

    def x_copy(side, c):
        at = pl.ds(c * chunk, chunk)
        return sender(x_out.at[side, at], x_in.at[side, at], x_send.at[side, c], x_recv.at[side, c],
                      lax.rem(x + (right, left_)[side], nx), z, s)

    def fill_x(c):
        for side in range(2):
            t_copy(side, c).wait_recv()
            xx = lax.rem(x + (right, left_)[side], nx)

            def relayed(j, inner):
                i = c * chunk + side * share + j
                x_out[side, i] = packed(pair_sum(xx, lax.rem(z + far(i), nz)) + unpacked(two_in[i], plain), plain)
                return inner

            def plainly(j, inner):
                i = c * chunk + (1 - side) * share + j
                x_out[side, i] = packed(pair_sum(xx, lax.rem(z + far(i), nz)), plain)
                return inner
            lax.fori_loop(0, share, relayed, 0)
            lax.fori_loop(0, share, plainly, 0)
            x_copy(side, c).start()

    quarter = nz // 4
    n_far = 2 * quarter - 1
    odd = lax.rem(z, 2)

    def hop(i):
        d = far(i)
        if i >= n_far:
            return d
        if i == 0:
            return quarter + 2 * quarter * odd
        return d - quarter if i % 2 == 1 else d + quarter

    def z_copy(i):
        return sender(z_out.at[i], z_in.at[i], z_send.at[i], z_recv.at[i], x, lax.rem(z + hop(i), nz), s)

    def fill_z(c):
        for side in range(2):
            x_copy(side, c).wait_recv()

        def one(j, inner):
            i = c * chunk + j
            acc = pair_sum(x, lax.rem(z + far(i), nz))
            for side in range(2):
                acc = acc + unpacked(x_in[side, i], plain)
            z_out[i] = packed(acc, plain)
            z_sum[i] = acc
            return inner
        lax.fori_loop(0, chunk, one, 0)
        for i in range(c * chunk, (c + 1) * chunk):
            if i not in (n_far, n_far + 1, nz - 1):
                z_copy(i).start()

    def relay_z():
        for i in range(n_far):
            z_copy(i).wait_recv()
            to = n_far + odd if i == 0 else n_far + (i + 1) % 2
            z_sum[to] = z_sum[to] + unpacked(z_in[i], plain)
        for i in (n_far, n_far + 1):
            z_out[i] = packed(z_sum[i], plain)
        for i in (n_far, n_far + 1):
            z_copy(i).start()

    c_copy(across, s).wait_recv()
    hear()
    tell()
    for c in range(chunks - 1):
        fill_two(c)
    hear()
    tell()
    c_copy(right, s).wait_recv()
    c_copy(left_, s).wait_recv()
    fill_x(0)
    hear()
    tell()
    fill_two(chunks - 1)
    fill_x(1)
    c_copy(0, s).wait_recv()
    for c in range(chunks):
        if c == chunks - 1:
            relay_z()
        fill_z(c)
        if c + 2 < chunks:
            fill_x(c + 2)
        hear()
        if c + 4 < n_tokens:
            tell()
    acc = z_sum[nz - 1]
    for i in list(range(n_far + 2, nz - 1)) + [n_far, n_far + 1]:
        z_copy(i).wait_recv()
        acc = acc + unpacked(z_in[i], plain)
    total[...] = acc

    rho2 = jnp.concatenate([rho[...], rho[...]], axis=0)
    gain, dual = wide[0], wide[1]
    anchor = sum(basis[d] * wide[2 + d] for d in range(degrees))
    target = total[plain:, :] - dual - rho2 * (gain - anchor)
    new = gain + eliminate(total, target, rho[...], full, directions)
    for h in range(half_count):
        gain_new[h] = new[:, h * HALF:h * HALF + stations]
    weighted = new + dual / rho2
    left = lax.broadcasted_iota(jnp.int32, (2 * directions, 2 * HALF), 1) < HALF

    def folded(d):
        part = basis[d] * weighted
        return part + pltpu.roll(part, HALF, axis=1)
    pair = degrees // 2
    both = jnp.concatenate([jnp.where(left, folded(d), folded(d + pair)) for d in range(pair)], axis=0)
    pieces, piece = part_out.shape[0], part_out.shape[1]
    for m in range(pieces):
        part_out[m] = both[m * piece:(m + 1) * piece, :]

    near = [(e, f) for e in range(nx) for f in range(2) if e + f > 0]

    def other(e, f):
        return lax.rem(x + e, nx), s + f - 2 * s * f

    def p_copy(e, f):
        xx, ss = other(e, f)
        return sender(part_out.at[xx * 2 + ss], part_in.at[e * 2 + f], p_send.at[e * 2 + f],
                      p_recv.at[e * 2 + f], xx, z, ss)
    for e, f in near:
        p_copy(e, f).start()
    acc = part_out[x * 2 + s]
    for e, f in near:
        p_copy(e, f).wait_recv()
        acc = acc + part_in[e * 2 + f]
    ring_in[z] = acc

    def r_copy(d):
        zz = lax.rem(z + d, nz)
        return sender(ring_in.at[z], ring_in.at[z], r_send.at[d], r_recv.at[d], x, zz, s)

    def start_r(i, carry):
        r_copy(far(i)).start()
        return carry
    lax.fori_loop(0, nz - 1, start_r, 0)

    def take_r(i, carry):
        d = far(i)
        zz = lax.rem(z + nz - d, nz)
        sender(ring_in.at[zz], ring_in.at[zz], r_send.at[d], r_recv.at[d], x, z, s).wait_recv()
        return carry
    lax.fori_loop(0, nz - 1, take_r, 0)
    acc = ring_in[0]
    for i in range(1, nz):
        acc = acc + ring_in[i]
    me = x * 2 + s
    last_in[me] = acc

    def l_copy(e, f, m):
        xx, ss = other(e, f)
        return sender(last_in.at[m], last_in.at[m], l_send.at[e * 2 + f], l_recv.at[e * 2 + f], xx, z, ss)
    for e, f in near:
        l_copy(e, f, me).start()
    for e, f in near:
        back = lax.rem(x + nx - e, nx) * 2 + (s + f - 2 * s * f)
        l_copy(e, f, back).wait_recv()
    both = jnp.concatenate([last_in[m] for m in range(pieces)], axis=0)
    wide = 2 * directions
    summed = [None] * degrees
    for d in range(pair):
        rows = both[d * wide:(d + 1) * wide, :]
        turned = pltpu.roll(rows, HALF, axis=1)
        summed[d] = jnp.where(left, rows, turned)
        summed[d + pair] = jnp.where(left, turned, rows)
    fit = None
    for d in range(degrees):
        coeff = sum(inverse[d][q] * summed[q] for q in range(degrees))
        cons_new[d] = coeff[:, :stations]
        term = basis[d] * coeff
        fit = term if fit is None else fit + term
    dual_out = dual + rho2 * (new - fit)
    for h in range(half_count):
        dual_new[h] = dual_out[:, h * HALF:h * HALF + stations]

    for e in range(nx):
        c_copy(e, 1 - s).wait_send()

    for c in range(chunks):
        for side in range(2):
            t_copy(side, c).wait_send()
            x_copy(side, c).wait_send()
    for i in range(nz - 1):
        z_copy(i).wait_send()
        r_copy(i + 1).wait_send()
    for e, f in near:
        p_copy(e, f).wait_send()
        l_copy(e, f, me).wait_send()


def finish(sums, gains, duals, cons, rho, inverse, nx, nz):
    vmem = pl.BlockSpec(memory_space=pltpu.VMEM)
    dma = pltpu.SemaphoreType.DMA
    degrees, rows, _ = cons.shape
    terms, lanes = sums.shape[1:]
    wire = terms + rows
    pieces = 2 * nx
    piece = degrees * rows // 2 // pieces
    chunks = nz // 4
    return pl.pallas_call(
        functools.partial(finish_kernel, nx, nz, inverse),
        out_shape=jax.ShapeDtypeStruct((2 * duals.shape[0] + cons.shape[0],) + cons.shape[1:], F32),
        in_specs=[vmem] * 5,
        out_specs=vmem,
        scratch_shapes=[
            pltpu.VMEM((nx * nz, terms, lanes), F32),
            pltpu.VMEM((nz, wire, lanes), BF),
            pltpu.VMEM((nz, wire, lanes), BF),
            pltpu.VMEM((2, nz, wire, lanes), BF),
            pltpu.VMEM((2, nz, wire, lanes), BF),
            pltpu.VMEM((nz, wire, lanes), BF),
            pltpu.VMEM((nz, wire, lanes), BF),
            pltpu.VMEM((nz, terms, lanes), F32),
            pltpu.VMEM((terms, lanes), F32),
            pltpu.VMEM((2, rows * rows // 4, lanes), F32),
            pltpu.VMEM((2 + degrees, rows, lanes), F32),
            pltpu.VMEM((pieces, piece, lanes), F32),
            pltpu.VMEM((pieces, piece, lanes), F32),
            pltpu.VMEM((nz, piece, lanes), F32),
            pltpu.VMEM((pieces, piece, lanes), F32),
            dma((nx,)), dma((nx,)), dma((2, chunks)), dma((2, chunks)), dma((2, chunks)), dma((2, chunks)),
            dma((nz,)), dma((nz,)),
            dma((pieces,)), dma((pieces,)), dma((nz,)), dma((nz,)), dma((pieces,)), dma((pieces,)),
            pltpu.SemaphoreType.REGULAR((2,)),
        ],
        compiler_params=pltpu.CompilerParams(collective_id=1, has_side_effects=True,
                                             vmem_limit_bytes=18 * 1024 * 1024),
        name="finish",
    )(sums, gains, duals, cons, rho)


def to_rows(x):
    n, c, s, k = x.shape
    return jnp.transpose(x, (0, 1, 3, 2)).reshape(n, c * k, s)


def from_rows(x):
    n, rows, s = x.shape
    return jnp.transpose(x.reshape(n, 2, rows // 2, s), (0, 1, 3, 2))


def body(sky, seen, keep, tile_owner, tile_channel, tile_base, pairs, gains, duals, consensus, rho):
    channels_here, _, _, directions = gains.shape
    nx, nz = lax.axis_size(XS), lax.axis_size(ZS)
    sub_count = lax.axis_size("sub")
    half_count = channels_here // sub_count
    gain_rows = to_rows(gains)
    table, order, groups = gather_gains(gain_rows, tile_base.reshape(1, -1), pairs.shape[0], nx, nz)
    sums = tile_sums(sky, seen, keep, order, groups, tile_owner[:, 0], tile_channel, tile_base, pairs, table,
                     nx * nz * sub_count, half_count)
    rho_rows = jnp.broadcast_to(rho[:, None], (directions, 2 * HALF))
    result = finish(sums, gain_rows, to_rows(duals), to_rows(consensus), rho_rows,
                                          gram_inverse(channels_here * nx * nz).tolist(), nx, nz)
    return (from_rows(result[:half_count]), from_rows(result[2 * half_count:]),
            from_rows(result[half_count:2 * half_count]))


def solution(mesh):
    groups, subs = mesh.shape["groups"], mesh.shape["sub"]
    torus = Mesh(mesh.devices.reshape(groups, 4, mesh.shape["chan"] // 4, subs), GROUPS_CHAN_SUB)
    return jax.shard_map(
        body,
        mesh=torus,
        in_specs=(
            P(GROUPS_CHAN_SUB, None, None, None),
            P(GROUPS_CHAN_SUB, None, None),
            P(GROUPS_CHAN_SUB, None),
            P(GROUPS_CHAN_SUB, None),
            P(GROUPS_CHAN_SUB),
            P(GROUPS_CHAN_SUB),
            P(),
            P(GROUPS_CHAN, None, None, None),
            P(GROUPS_CHAN_SUB, None, None, None),
            P("groups", None, None, None),
            P(),
        ),
        out_specs=(
            P(GROUPS_CHAN_SUB, None, None, None),
            P("groups", None, None, None),
            P(GROUPS_CHAN_SUB, None, None, None),
        ),
        check_vma=False,
    )
```

```python
import functools

import jax
import jax.numpy as jnp
import numpy as np
from jax import lax
from jax.experimental import pallas as pl
from jax.experimental.pallas import tpu as pltpu
from jax.sharding import Mesh
from jax.sharding import PartitionSpec as P

GROUPS_CHAN_SUB = ("groups", "chan_0", "chan_1", "sub")
GROUPS_CHAN = ("groups", "chan_0", "chan_1")
BF, F32 = jnp.bfloat16, jnp.float32
GROUP = 8
HALF = 64


def term_rows(directions):
    real, imag = {}, {}
    for k in range(directions):
        for m in range(k, directions):
            real[k, m] = len(real)
    for k in range(directions):
        for m in range(k + 1, directions):
            imag[k, m] = len(real) + len(imag)
    return real, imag


def legendre(first, channels):
    lane = lax.broadcasted_iota(jnp.int32, (1, 2 * HALF), 1)
    place = (first + lane // HALF).astype(F32)
    x = (2.0 * place - (channels - 1)) / max(channels - 1, 1)
    return [jnp.ones_like(x), x, 0.5 * (3.0 * x * x - 1.0), 0.5 * (5.0 * x * x * x - 3.0 * x)]


def gram_inverse(channels):
    x = (2.0 * np.arange(channels, dtype=np.float64) - (channels - 1)) / max(channels - 1, 1)
    basis = np.stack([np.ones_like(x), x, 0.5 * (3 * x * x - 1), 0.5 * (5 * x * x * x - 3 * x)])
    return np.linalg.inv(basis @ basis.T)


def tile_order(base, bases, slots):
    tiles = base.shape[1]
    padded_bases = -(-bases // 16) * 16
    member = lax.broadcasted_iota(jnp.int32, (padded_bases, tiles), 0) == base
    hit = jnp.where(member, 1.0, 0.0)
    before = jnp.where(lax.broadcasted_iota(jnp.int32, (tiles, tiles), 0)
                       < lax.broadcasted_iota(jnp.int32, (tiles, tiles), 1), 1.0, 0.0).astype(BF)
    rank = jnp.dot(hit.astype(BF), before, preferred_element_type=F32)
    counts = jnp.sum(hit, axis=1, keepdims=True).astype(jnp.int32)
    groups = lax.shift_right_logical(counts + (GROUP - 1), GROUP.bit_length() - 1).astype(F32)
    lower = jnp.where(lax.broadcasted_iota(jnp.int32, (padded_bases, padded_bases), 1)
                      < lax.broadcasted_iota(jnp.int32, (padded_bases, padded_bases), 0), 1.0, 0.0).astype(BF)
    start = jnp.dot(lower, jnp.broadcast_to(groups, (padded_bases, tiles)).astype(BF),
                    preferred_element_type=F32)
    where = jnp.sum(jnp.where(member, rank + GROUP * start, 0.0), axis=0, keepdims=True).astype(jnp.int32)
    chosen = jnp.where(lax.broadcasted_iota(jnp.int32, (slots, tiles), 0) == where, 1.0, 0.0).astype(BF)
    tile = lax.broadcasted_iota(jnp.int32, (8, tiles), 1)
    kind = lax.broadcasted_iota(jnp.int32, (8, tiles), 0)
    digits = jnp.where(kind == 0, lax.shift_right_logical(tile, 4),
                       jnp.where(kind == 1, jnp.bitwise_and(tile, 15), 1)).astype(F32).astype(BF)
    found = lax.dot_general(digits, chosen, (((1,), (1,)), ((), ())), preferred_element_type=F32)
    named = jnp.where(found[2:3] > 0.5, 16.0 * found[0:1] + found[1:2], float(tiles)).astype(jnp.int32)
    total = jnp.broadcast_to(jnp.sum(groups, axis=0, keepdims=True), (1, 128)).astype(jnp.int32)
    return named, total


def tile_kernel(half_count, order, groups, owner, channel, base, sky, seen, keep, pairs, table, out, onehot, *buffers):
    tiles, coupled, rows = sky.shape
    directions = coupled // 2
    bases = pairs.shape[0]
    real, imag = term_rows(directions)
    n_terms = directions * directions + 2 * directions
    devices = out.shape[0] - 1
    channels_here = table.shape[0] // (devices // 2)
    chans = devices // 2
    buffers = (buffers[0::2], buffers[1::2])

    station = lax.rem(lax.broadcasted_iota(jnp.int32, (2 * HALF, rows), 0), HALF)
    for b in range(bases):
        for side in range(2):
            onehot[b, :, side * rows:(side + 1) * rows] = jnp.where(
                station == pairs[b, side:side + 1, :], 1.0, 0.0).astype(BF)

    def clear(i, carry):
        out[i] = jnp.zeros((n_terms, 2 * HALF), F32)
        return carry
    lax.fori_loop(0, devices + 1, clear, 0)
    lane = lax.broadcasted_iota(jnp.int32, (1, 2 * HALF), 1)

    def chosen(g):
        first = order[0, jnp.maximum(g, 0) * GROUP]
        return onehot.at[base[jnp.minimum(first, tiles - 1)]]

    def load(g, into):
        sky_s, seen_s, keep_s, gain_s, near_far, _, _ = buffers[into]
        for t in range(GROUP):
            named = order[0, g * GROUP + t]
            tile = jnp.where(named < tiles, named, 0)
            kept = keep[pl.ds(tile, 1), :] > 0
            sky_s[pl.ds(t, coupled, stride=GROUP), :] = jnp.where(kept, sky[tile].astype(F32), 0.0)
            seen_s[pl.ds(t, 2, stride=GROUP), :] = jnp.where(kept, seen[tile].astype(F32), 0.0)
            gain_s[pl.ds(t, coupled, stride=GROUP), :] = table[owner[tile] * channels_here + channel[tile]].astype(F32)
        near_far[...] = jnp.dot(gain_s[...].astype(BF), chosen(g)[...], preferred_element_type=F32)

    def products(of):
        sky_s, seen_s, keep_s, _, near_far, terms, _ = buffers[of]
        def block(ref, i):
            return ref[i * GROUP:(i + 1) * GROUP, :]

        res_r = block(seen_s, 0)
        res_i = block(seen_s, 1)
        v_r, v_i = [], []
        for k in range(directions):
            c_r = block(sky_s, 2 * k)
            c_i = block(sky_s, 2 * k + 1)
            p_r, p_i = (block(near_far, c * directions + k)[:, :rows] for c in range(2))
            q_r, q_i = (block(near_far, c * directions + k)[:, rows:] for c in range(2))
            x_r = c_r * q_r + c_i * q_i
            x_i = c_i * q_r - c_r * q_i
            v_r.append(x_r)
            v_i.append(x_i)
            res_r = res_r - (p_r * x_r - p_i * x_i)
            res_i = res_i - (p_r * x_i + p_i * x_r)
        w_r, w_i = res_r, res_i

        for side in range(2):
            pending = {}

            def put(j, value):
                pending[j] = value
                lo = j - j % 2
                if lo in pending and lo + 1 in pending:
                    both = jnp.concatenate([pending.pop(lo), pending.pop(lo + 1)], axis=0)
                    terms[lo * GROUP:(lo + 2) * GROUP, side * rows:(side + 1) * rows] = both.astype(BF)

            if side == 1:
                v_r, v_i, w_i = [], [], -res_i
                for k in range(directions):
                    c_r = block(sky_s, 2 * k)
                    c_i = block(sky_s, 2 * k + 1)
                    p_r, p_i = (block(near_far, c * directions + k)[:, :rows] for c in range(2))
                    v_r.append(c_r * p_r - c_i * p_i)
                    v_i.append(-(c_r * p_i + c_i * p_r))
            for (k, m), j in real.items():
                put(j, v_r[k] * v_r[m] + v_i[k] * v_i[m])
            for (k, m), j in imag.items():
                put(j, v_r[k] * v_i[m] - v_i[k] * v_r[m])
            first = directions * directions
            for k in range(directions):
                put(first + k, v_r[k] * w_r + v_i[k] * w_i)
            for k in range(directions):
                put(first + directions + k, v_r[k] * w_i - v_i[k] * w_r)

    def station_sums(g, of):
        terms, sums = buffers[of][5:]
        sums[...] = lax.dot_general(terms[...], chosen(g)[...], (((1,), (1,)), ((), ())),
                                    preferred_element_type=F32)

    def add_up(g, of):
        sums = buffers[of][6]
        for t in range(GROUP):
            named = jnp.where(g < 0, tiles, order[0, jnp.maximum(g, 0) * GROUP + t])
            tile = jnp.where(named < tiles, named, 0)
            mine = channel[tile]
            row = jnp.where(named < tiles, (mine // half_count) * chans + owner[tile], devices)
            part = jnp.where(lane // HALF == lax.rem(mine, half_count),
                             sums[pl.ds(t, n_terms, stride=GROUP), :], 0.0)
            out[row] = out[row] + part

    def step(g, of):
        station_sums(g - 2, of)
        add_up(g - 3, 1 - of)
        load(g, of)
        products(1 - of)

    def two(i, carry):
        step(2 * i, 0)
        step(2 * i + 1, 1)
        return carry

    lax.fori_loop(0, (groups[0, 0] + 4) // 2, two, 0)


def tile_sums(sky, seen, keep, order, groups, owner, channel, base, pairs, table, devices, half_count):
    tiles, directions, _, rows = sky.shape
    n_terms = directions * directions + 2 * directions
    bases = pairs.shape[0]
    smem = pl.BlockSpec(memory_space=pltpu.SMEM)
    vmem = pl.BlockSpec(memory_space=pltpu.VMEM)
    coupled = 2 * directions
    return pl.pallas_call(
        functools.partial(tile_kernel, half_count),
        out_shape=jax.ShapeDtypeStruct((devices + 1, n_terms, 2 * HALF), F32),
        in_specs=[smem] * 5 + [vmem] * 5,
        out_specs=vmem,
        scratch_shapes=[pltpu.VMEM((bases, 2 * HALF, 2 * rows), BF)] + [
            shape for shape in (
                pltpu.VMEM((coupled * GROUP, rows), F32),
                pltpu.VMEM((2 * GROUP, rows), F32),
                pltpu.VMEM((GROUP, rows), jnp.int32),
                pltpu.VMEM((coupled * GROUP, 2 * HALF), F32),
                pltpu.VMEM((coupled * GROUP, 2 * rows), F32),
                pltpu.VMEM((n_terms * GROUP, 2 * rows), BF),
                pltpu.VMEM((n_terms * GROUP, 2 * HALF), F32),
            ) for _ in range(2)
        ],
        compiler_params=pltpu.CompilerParams(vmem_limit_bytes=18 * 1024 * 1024),
        name="tile_sums",
    )(order, groups, owner, channel, base, sky.reshape(tiles, coupled, rows), seen, keep, pairs, table)


def eliminate(total, target, rho, full, directions):
    real, imag = term_rows(directions)
    lanes = total.shape[-1]
    for k in range(directions):
        for m in range(directions):
            re = real[min(k, m), max(k, m)]
            value = total[re:re + 1, :]
            if k == m:
                value = value + rho[k:k + 1, :]
                full[1, k * directions + m:k * directions + m + 1, :] = jnp.zeros((1, lanes), F32)
            else:
                im = imag[min(k, m), max(k, m)]
                imv = total[im:im + 1, :]
                full[1, k * directions + m:k * directions + m + 1, :] = imv if k < m else -imv
            full[0, k * directions + m:k * directions + m + 1, :] = value
    row_r = [full[0, k * directions:(k + 1) * directions, :] for k in range(directions)]
    row_i = [full[1, k * directions:(k + 1) * directions, :] for k in range(directions)]
    t_r = [target[k:k + 1, :] for k in range(directions)]
    t_i = [target[directions + k:directions + k + 1, :] for k in range(directions)]
    for k in range(directions):
        inv = 1.0 / row_r[k][k:k + 1, :]
        row_r[k] = row_r[k] * inv
        row_i[k] = row_i[k] * inv
        t_r[k] = t_r[k] * inv
        t_i[k] = t_i[k] * inv
        for m in range(directions):
            if m == k:
                continue
            f_r = row_r[m][k:k + 1, :]
            f_i = row_i[m][k:k + 1, :]
            row_r[m], row_i[m] = (row_r[m] - (f_r * row_r[k] - f_i * row_i[k]),
                                  row_i[m] - (f_r * row_i[k] + f_i * row_r[k]))
            t_r[m], t_i[m] = (t_r[m] - (f_r * t_r[k] - f_i * t_i[k]),
                              t_i[m] - (f_r * t_i[k] + f_i * t_r[k]))
    return jnp.concatenate(t_r + t_i, axis=0)


XS, ZS = "chan_0", "chan_1"


def place():
    return lax.axis_index(XS), lax.axis_index(ZS), lax.axis_index("sub")


def sender(src, dst, send_sem, recv_sem, x, z, s):
    return pltpu.make_async_remote_copy(
        src_ref=src, dst_ref=dst, send_sem=send_sem, recv_sem=recv_sem,
        device_id={XS: x, ZS: z, "sub": s}, device_id_type=pl.DeviceIdType.MESH)


def meet(x, z, s, nx, nz, reach, crossed):
    barrier = pltpu.get_barrier_semaphore()

    def ring(d, carry):
        pl.semaphore_signal(barrier, inc=1, device_id={XS: x, ZS: lax.rem(z + d, nz), "sub": s},
                            device_id_type=pl.DeviceIdType.MESH)
        return carry
    lax.fori_loop(1, reach + 1, ring, 0)
    lax.fori_loop(max(reach + 1, nz - reach), nz, ring, 0)
    near = [(e, f) for e in range(nx) for f in range(2) if e + f > 0 and (crossed or e * f == 0)]
    for e, f in near:
        pl.semaphore_signal(barrier, inc=1,
                            device_id={XS: lax.rem(x + e, nx), ZS: z, "sub": s + f - 2 * s * f},
                            device_id_type=pl.DeviceIdType.MESH)
    return barrier, min(nz - 1, 2 * reach) + len(near)


def outward(i, nz):
    return jnp.where(lax.rem(i, 2) == 0, i // 2 + 1, nz - 1 - i // 2)


def gather_kernel(nx, nz, bases, gains, base, table, order, groups, wide, mine,
                  z_recv, z_send, x_recv, x_send, c_recv, c_send):
    x, z, s = place()
    here, half = mine.shape[0], mine.shape[0] // 2
    stations = gains.shape[2]
    barrier, count = meet(x, z, s, nx, nz, nz - 1, False)
    wide[...] = jnp.zeros(wide.shape, F32)
    head = gains[...].astype(BF).astype(F32)
    wide[:, :, :stations] = head
    wide[:, :, HALF:HALF + stations] = gains[...] - head
    mine[...] = wide[...].astype(BF)
    table[pl.ds((x * nz + z) * here + s * half, half)] = mine[pl.ds(s * half, half)]
    pl.semaphore_wait(barrier, count)

    def block(xx, zz):
        return table.at[pl.ds((xx * nz + zz) * here + s * half, half)]

    def rows(xx, h):
        return table.at[pl.ds(xx * nz * here, nz * here)].reshape(nz, here, *mine.shape[1:]).at[:, pl.ds(h * half, half)]

    own = mine.at[pl.ds(s * half, half)]

    def z_copy(d):
        return sender(own, block(x, z), z_send.at[d], z_recv.at[d], x, lax.rem(z + d, nz), s)

    def start_z(i, carry):
        z_copy(outward(nz - 2 - i, nz)).start()
        return carry
    lax.fori_loop(0, nz - 1, start_z, 0)

    def x_copy(src, zz, d, e):
        return sender(src, block(x, zz), x_send.at[e, d], x_recv.at[e, d], lax.rem(x + e, nx), z, s)
    for e in range(1, nx):
        x_copy(own, z, 0, e).start()
    order[...], groups[...] = tile_order(base[...], bases, order.shape[1])

    def pass_on(i, carry):
        d = outward(i, nz)
        zz = lax.rem(z + nz - d, nz)
        sender(own, block(x, zz), z_send.at[d], z_recv.at[d], x, z, s).wait_recv()
        for e in (nx // 2, 1, nx - 1):
            x_copy(block(x, zz), zz, d, e).start()
        return carry
    lax.fori_loop(0, nz - 1, pass_on, 0)

    def c_copy(e, h):
        xx = lax.rem(x + nx - e, nx)
        return sender(rows(xx, h), rows(xx, h), c_send.at[e], c_recv.at[e], x, z, 1 - s)
    for e in (0, 1, 3, 2):
        if e > 0:
            xx = lax.rem(x + nx - e, nx)

            def arrived(d, carry):
                zz = lax.rem(z + nz - d, nz)
                sender(own, block(xx, zz), x_send.at[e, d], x_recv.at[e, d], x, z, s).wait_recv()
                return carry
            lax.fori_loop(0, nz, arrived, 0)
        c_copy(e, s).start()
    for e in range(nx):
        c_copy(e, 1 - s).wait_recv()

    def done_z(d, carry):
        z_copy(d).wait_send()
        return carry
    lax.fori_loop(1, nz, done_z, 0)
    for e in range(1, nx):
        def done_x(d, carry):
            x_copy(own, z, d, e).wait_send()
            return carry
        lax.fori_loop(0, nz, done_x, 0)
    for e in range(nx):
        c_copy(e, s).wait_send()


def gather_gains(gains, base, bases, nx, nz):
    vmem = pl.BlockSpec(memory_space=pltpu.VMEM)
    dma = pltpu.SemaphoreType.DMA
    here, rows, _ = gains.shape
    slots = -(-(base.shape[1] + GROUP * (bases + 6)) // 128) * 128
    return pl.pallas_call(
        functools.partial(gather_kernel, nx, nz, bases),
        out_shape=(jax.ShapeDtypeStruct((nx * nz * here, rows, 2 * HALF), BF),
                   jax.ShapeDtypeStruct((1, slots), jnp.int32), jax.ShapeDtypeStruct((1, 128), jnp.int32)),
        in_specs=[vmem, vmem],
        out_specs=(vmem, vmem, vmem),
        scratch_shapes=[pltpu.VMEM((here, rows, 2 * HALF), F32), pltpu.VMEM((here, rows, 2 * HALF), BF),
                        dma((nz,)), dma((nz,)), dma((nx, nz)), dma((nx, nz)), dma((nx,)), dma((nx,))],
        compiler_params=pltpu.CompilerParams(collective_id=0, has_side_effects=True,
                                             vmem_limit_bytes=8 * 1024 * 1024),
        cost_estimate=pl.CostEstimate(flops=20000000000, bytes_accessed=20000000, transcendentals=0),
        name="gather_gains",
    )(gains, base)


def packed(v, plain):
    head = v[plain:].astype(BF)
    tail = v[plain:] - head.astype(F32)
    return jnp.concatenate([v[:plain].astype(BF), head, tail.astype(BF)], axis=0)


def unpacked(w, plain):
    v = w.astype(F32)
    mid = (v.shape[0] + plain) // 2
    return jnp.concatenate([v[:plain], v[plain:mid] + v[mid:]], axis=0)


def finish_kernel(nx, nz, inverse, sums, gains, duals, cons, rho, result,
                  peer, two_out, two_in, x_out, x_in, z_out, z_in, z_sum, total, full, wide,
                  part_out, part_in, ring_in, last_in,
                  c_send, c_recv, t_send, t_recv, x_send, x_recv, z_send, z_recv,
                  p_send, p_recv, r_send, r_recv, l_send, l_recv, token):
    x, z, s = place()
    directions = rho.shape[0]
    degrees, _, stations = cons.shape
    half_count = duals.shape[0]
    gain_new, dual_new = result.at[:half_count], result.at[half_count:2 * half_count]
    cons_new = result.at[2 * half_count:]
    plain = directions * directions
    chunk = 4
    nodes = nx * nz
    barrier, count = meet(x, z, s, nx, nz, 1, True)

    wide[...] = jnp.zeros(wide.shape, F32)
    for h in range(half_count):
        wide[0, :, h * HALF:h * HALF + stations] = gains[s * half_count + h]
        wide[1, :, h * HALF:h * HALF + stations] = duals[h]
        for d in range(degrees):
            wide[2 + d, :, h * HALF:h * HALF + stations] = cons[d]
    basis = legendre(((x * nz + z) * 2 + s) * half_count, 2 * nodes * half_count)
    pl.semaphore_wait(barrier, count)

    def far(i):
        if isinstance(i, int):
            return (nz // 2 + (i + 1) // 2 * (1 if i % 2 == 0 else -1)) % nz
        step = (i + 1) // 2
        return lax.rem(jnp.where(lax.rem(i, 2) == 0, nz // 2 + step, nz // 2 + nz - step), nz)

    def tell():
        for side in range(2):
            pl.semaphore_signal(token.at[side], inc=1, device_id={XS: x, ZS: lax.rem(z + (1, nz - 1)[side], nz), "sub": s},
                                device_id_type=pl.DeviceIdType.MESH)

    def hear():
        for side in range(2):
            pl.semaphore_wait(token.at[side], 1)
    n_tokens = nz // 2 - 1
    tell()

    def c_copy(e, h):
        xx = lax.rem(x + e, nx)
        return sender(sums.at[pl.ds(h * nodes + xx * nz, nz)], peer.at[pl.ds(xx * nz, nz)],
                      c_send.at[e], c_recv.at[e], x, z, 1 - s)
    across, right, left_ = nx // 2, 1, nx - 1
    order = (across, right, left_, 0)
    for e in order:
        c_copy(e, 1 - s).start()

    def pair_sum(xx, zz):
        return sums[s * nodes + xx * nz + zz] + peer[xx * nz + zz]

    chunks = nz // chunk
    share = chunk // 2
    def t_copy(side, c):
        at = pl.ds(c * chunk + side * share, share)
        return sender(two_out.at[at], two_in.at[at], t_send.at[side, c], t_recv.at[side, c],
                      lax.rem(x + (right, left_)[side], nx), z, s)

    def fill_two(c):
        def one(j, inner):
            i = c * chunk + j
            two_out[i] = packed(pair_sum(lax.rem(x + across, nx), lax.rem(z + far(i), nz)), plain)
            return inner
        lax.fori_loop(0, chunk, one, 0, unroll=True)
        for side in range(2):
            t_copy(side, c).start()

    def x_copy(side, c):
        at = pl.ds(c * chunk, chunk)
        return sender(x_out.at[side, at], x_in.at[side, at], x_send.at[side, c], x_recv.at[side, c],
                      lax.rem(x + (right, left_)[side], nx), z, s)

    def fill_x(c):
        for side in range(2):
            xx = lax.rem(x + (right, left_)[side], nx)

            def relayed(j, inner):
                i = c * chunk + side * share + j
                x_out[side, i] = packed(pair_sum(xx, lax.rem(z + far(i), nz)) + unpacked(two_in[i], plain), plain)
                return inner

            def plainly(j, inner):
                i = c * chunk + (1 - side) * share + j
                x_out[side, i] = packed(pair_sum(xx, lax.rem(z + far(i), nz)), plain)
                return inner
            lax.fori_loop(0, share, plainly, 0, unroll=True)
            t_copy(side, c).wait_recv()
            lax.fori_loop(0, share, relayed, 0, unroll=True)
            x_copy(side, c).start()

    quarter = nz // 4
    n_far = 2 * quarter - 1
    odd = lax.rem(z, 2)

    def hop(i):
        d = far(i)
        if i >= n_far:
            return d
        if i == 0:
            return quarter + 2 * quarter * odd
        return d - quarter if i % 2 == 1 else d + quarter

    def z_copy(i):
        return sender(z_out.at[i], z_in.at[i], z_send.at[i], z_recv.at[i], x, lax.rem(z + hop(i), nz), s)

    def fill_z(c):
        for side in range(2):
            x_copy(side, c).wait_recv()

        def one(j, inner):
            i = c * chunk + j
            acc = pair_sum(x, lax.rem(z + far(i), nz))
            for side in range(2):
                acc = acc + unpacked(x_in[side, i], plain)
            z_out[i] = packed(acc, plain)
            z_sum[i] = acc
            return inner
        lax.fori_loop(0, chunk, one, 0, unroll=True)
        for i in range(c * chunk, (c + 1) * chunk):
            if i not in (n_far, n_far + 1, nz - 1):
                z_copy(i).start()

    def relay_z():
        for i in range(n_far):
            z_copy(i).wait_recv()
            to = n_far + odd if i == 0 else n_far + (i + 1) % 2
            z_sum[to] = z_sum[to] + unpacked(z_in[i], plain)
        for i in (n_far, n_far + 1):
            z_out[i] = packed(z_sum[i], plain)
        for i in (n_far, n_far + 1):
            z_copy(i).start()

    c_copy(across, s).wait_recv()
    hear()
    tell()
    for c in range(chunks - 1):
        fill_two(c)
    hear()
    tell()
    c_copy(right, s).wait_recv()
    c_copy(left_, s).wait_recv()
    fill_x(0)
    hear()
    tell()
    fill_two(chunks - 1)
    fill_x(1)
    c_copy(0, s).wait_recv()
    for c in range(chunks):
        if c == chunks - 1:
            relay_z()
        fill_z(c)
        if c + 2 < chunks:
            fill_x(c + 2)
        hear()
        if c + 4 < n_tokens:
            tell()
    acc = z_sum[nz - 1]
    for i in list(range(n_far + 2, nz - 1)) + [n_far, n_far + 1]:
        z_copy(i).wait_recv()
        acc = acc + unpacked(z_in[i], plain)
    total[...] = acc

    rho2 = jnp.concatenate([rho[...], rho[...]], axis=0)
    gain, dual = wide[0], wide[1]
    anchor = sum(basis[d] * wide[2 + d] for d in range(degrees))
    target = total[plain:, :] - dual - rho2 * (gain - anchor)
    new = gain + eliminate(total, target, rho[...], full, directions)
    for h in range(half_count):
        gain_new[h] = new[:, h * HALF:h * HALF + stations]
    weighted = new + dual / rho2
    left = lax.broadcasted_iota(jnp.int32, (2 * directions, 2 * HALF), 1) < HALF

    def folded(d):
        part = basis[d] * weighted
        return part + pltpu.roll(part, HALF, axis=1)
    pair = degrees // 2
    both = jnp.concatenate([jnp.where(left, folded(d), folded(d + pair)) for d in range(pair)], axis=0)
    pieces, piece = part_out.shape[0], part_out.shape[1]
    for m in range(pieces):
        part_out[m] = both[m * piece:(m + 1) * piece, :]

    near = [(e, f) for e in range(nx) for f in range(2) if e + f > 0]

    def other(e, f):
        return lax.rem(x + e, nx), s + f - 2 * s * f

    def p_copy(e, f):
        xx, ss = other(e, f)
        return sender(part_out.at[xx * 2 + ss], part_in.at[e * 2 + f], p_send.at[e * 2 + f],
                      p_recv.at[e * 2 + f], xx, z, ss)
    for e, f in near:
        p_copy(e, f).start()
    acc = part_out[x * 2 + s]
    for e, f in near:
        p_copy(e, f).wait_recv()
        acc = acc + part_in[e * 2 + f]
    ring_in[z] = acc

    def r_copy(d):
        zz = lax.rem(z + d, nz)
        return sender(ring_in.at[z], ring_in.at[z], r_send.at[d], r_recv.at[d], x, zz, s)

    def start_r(i, carry):
        r_copy(far(i)).start()
        return carry
    lax.fori_loop(0, nz - 1, start_r, 0)

    def take_r(i, carry):
        d = far(i)
        zz = lax.rem(z + nz - d, nz)
        sender(ring_in.at[zz], ring_in.at[zz], r_send.at[d], r_recv.at[d], x, z, s).wait_recv()
        return carry
    lax.fori_loop(0, nz - 1, take_r, 0)
    acc = ring_in[0]
    for i in range(1, nz):
        acc = acc + ring_in[i]
    me = x * 2 + s
    last_in[me] = acc

    def l_copy(e, f, m):
        xx, ss = other(e, f)
        return sender(last_in.at[m], last_in.at[m], l_send.at[e * 2 + f], l_recv.at[e * 2 + f], xx, z, ss)
    for e, f in near:
        l_copy(e, f, me).start()
    for e, f in near:
        back = lax.rem(x + nx - e, nx) * 2 + (s + f - 2 * s * f)
        l_copy(e, f, back).wait_recv()
    both = jnp.concatenate([last_in[m] for m in range(pieces)], axis=0)
    wide = 2 * directions
    summed = [None] * degrees
    for d in range(pair):
        rows = both[d * wide:(d + 1) * wide, :]
        turned = pltpu.roll(rows, HALF, axis=1)
        summed[d] = jnp.where(left, rows, turned)
        summed[d + pair] = jnp.where(left, turned, rows)
    fit = None
    for d in range(degrees):
        coeff = sum(inverse[d][q] * summed[q] for q in range(degrees))
        cons_new[d] = coeff[:, :stations]
        term = basis[d] * coeff
        fit = term if fit is None else fit + term
    dual_out = dual + rho2 * (new - fit)
    for h in range(half_count):
        dual_new[h] = dual_out[:, h * HALF:h * HALF + stations]

    for e in range(nx):
        c_copy(e, 1 - s).wait_send()

    for c in range(chunks):
        for side in range(2):
            t_copy(side, c).wait_send()
            x_copy(side, c).wait_send()
    for i in range(nz - 1):
        z_copy(i).wait_send()
        r_copy(i + 1).wait_send()
    for e, f in near:
        p_copy(e, f).wait_send()
        l_copy(e, f, me).wait_send()


def finish(sums, gains, duals, cons, rho, inverse, nx, nz):
    vmem = pl.BlockSpec(memory_space=pltpu.VMEM)
    dma = pltpu.SemaphoreType.DMA
    degrees, rows, _ = cons.shape
    terms, lanes = sums.shape[1:]
    wire = terms + rows
    pieces = 2 * nx
    piece = degrees * rows // 2 // pieces
    chunks = nz // 4
    return pl.pallas_call(
        functools.partial(finish_kernel, nx, nz, inverse),
        out_shape=jax.ShapeDtypeStruct((2 * duals.shape[0] + cons.shape[0],) + cons.shape[1:], F32),
        in_specs=[vmem] * 5,
        out_specs=vmem,
        scratch_shapes=[
            pltpu.VMEM((nx * nz, terms, lanes), F32),
            pltpu.VMEM((nz, wire, lanes), BF),
            pltpu.VMEM((nz, wire, lanes), BF),
            pltpu.VMEM((2, nz, wire, lanes), BF),
            pltpu.VMEM((2, nz, wire, lanes), BF),
            pltpu.VMEM((nz, wire, lanes), BF),
            pltpu.VMEM((nz, wire, lanes), BF),
            pltpu.VMEM((nz, terms, lanes), F32),
            pltpu.VMEM((terms, lanes), F32),
            pltpu.VMEM((2, rows * rows // 4, lanes), F32),
            pltpu.VMEM((2 + degrees, rows, lanes), F32),
            pltpu.VMEM((pieces, piece, lanes), F32),
            pltpu.VMEM((pieces, piece, lanes), F32),
            pltpu.VMEM((nz, piece, lanes), F32),
            pltpu.VMEM((pieces, piece, lanes), F32),
            dma((nx,)), dma((nx,)), dma((2, chunks)), dma((2, chunks)), dma((2, chunks)), dma((2, chunks)),
            dma((nz,)), dma((nz,)),
            dma((pieces,)), dma((pieces,)), dma((nz,)), dma((nz,)), dma((pieces,)), dma((pieces,)),
            pltpu.SemaphoreType.REGULAR((2,)),
        ],
        compiler_params=pltpu.CompilerParams(collective_id=1, has_side_effects=True,
                                             vmem_limit_bytes=18 * 1024 * 1024),
        name="finish",
    )(sums, gains, duals, cons, rho)


def to_rows(x):
    n, c, s, k = x.shape
    return jnp.transpose(x, (0, 1, 3, 2)).reshape(n, c * k, s)


def from_rows(x):
    n, rows, s = x.shape
    return jnp.transpose(x.reshape(n, 2, rows // 2, s), (0, 1, 3, 2))


def body(sky, seen, keep, tile_owner, tile_channel, tile_base, pairs, gains, duals, consensus, rho):
    channels_here, _, _, directions = gains.shape
    nx, nz = lax.axis_size(XS), lax.axis_size(ZS)
    sub_count = lax.axis_size("sub")
    half_count = channels_here // sub_count
    gain_rows = to_rows(gains)
    table, order, groups = gather_gains(gain_rows, tile_base.reshape(1, -1), pairs.shape[0], nx, nz)
    sums = tile_sums(sky, seen, keep, order, groups, tile_owner[:, 0], tile_channel, tile_base, pairs, table,
                     nx * nz * sub_count, half_count)
    rho_rows = jnp.broadcast_to(rho[:, None], (directions, 2 * HALF))
    result = finish(sums, gain_rows, to_rows(duals), to_rows(consensus), rho_rows,
                                          gram_inverse(channels_here * nx * nz).tolist(), nx, nz)
    return (from_rows(result[:half_count]), from_rows(result[2 * half_count:]),
            from_rows(result[half_count:2 * half_count]))


def solution(mesh):
    groups, subs = mesh.shape["groups"], mesh.shape["sub"]
    torus = Mesh(mesh.devices.reshape(groups, 4, mesh.shape["chan"] // 4, subs), GROUPS_CHAN_SUB)
    return jax.shard_map(
        body,
        mesh=torus,
        in_specs=(
            P(GROUPS_CHAN_SUB, None, None, None),
            P(GROUPS_CHAN_SUB, None, None),
            P(GROUPS_CHAN_SUB, None),
            P(GROUPS_CHAN_SUB, None),
            P(GROUPS_CHAN_SUB),
            P(GROUPS_CHAN_SUB),
            P(),
            P(GROUPS_CHAN, None, None, None),
            P(GROUPS_CHAN_SUB, None, None, None),
            P("groups", None, None, None),
            P(),
        ),
        out_specs=(
            P(GROUPS_CHAN_SUB, None, None, None),
            P("groups", None, None, None),
            P(GROUPS_CHAN_SUB, None, None, None),
        ),
        check_vma=False,
    )
```
